32 devices in a mesh: dp: 4 (over y, z), tp: 8 (over x, core).
Axes of the slice: x: 4, y: 2, z: 2, core: 2. Of those that a mesh axis runs over, the one named last changes fastest.
The devices are a block of a 4x4x8 slice.
Arguments:
- x_in: bfloat16 [32, 256, 3072], P('dp'), parts along dimension 0
- gain_attn: float32 [1, 3072], replicated
- w_qkv: bfloat16 [1, 3072, 3, 32, 96], P(None, None, None, 'tp')
- w_out: bfloat16 [1, 32, 96, 3072], P(None, 'tp')
- gain_mlp: float32 [1, 3072], replicated
- w_up: bfloat16 [1, 3072, 12288], P(None, None, 'tp')
- w_down: bfloat16 [1, 12288, 3072], P(None, 'tp')
- dy_out: bfloat16 [32, 256, 3072], P('dp'), parts along dimension 0
Outputs:
- output 1: bfloat16 [32, 256, 3072], P('dp'), parts along dimension 0
- output 2: bfloat16 [32, 256, 3072], P('dp'), parts along dimension 0
- output 3: float32 [4, 3072], P('dp'), parts along dimension 0
- output 4: bfloat16 [4, 3072, 3, 32, 96], P('dp', None, None, 'tp'), parts along dimension 0
- output 5: bfloat16 [4, 32, 96, 3072], P('dp', 'tp'), parts along dimension 0
- output 6: float32 [4, 3072], P('dp'), parts along dimension 0
- output 7: bfloat16 [4, 3072, 12288], P('dp', None, 'tp'), parts along dimension 0
- output 8: bfloat16 [4, 12288, 3072], P('dp', 'tp'), parts along dimension 0
There are 4 independent parts. The reference program is written for one: setup_inputs(seed, part) draws one part's arguments, and reference() takes and returns one part's arrays. A program takes and returns all parts, laid end to end along the dimension named above; an argument that names none is the same for every part.
All inputs are finite; a program needn't handle non-finite values.
Results may differ from the reference program's by a relative error of at most 0.0187187.
Values are sent between devices in bfloat16 or wider.
A program may use at most 768 MiB of HBM per device.

```python
import jax
import jax.numpy as jnp
from jax import lax

NUM_SEQS = 8
SEQ_LEN = 256
MODEL_DIM = 3072
NUM_HEADS = 32
FFN_DIM = 12288
NUM_LAYERS = 1
HEAD_DIM = MODEL_DIM // NUM_HEADS
LN_EPS = 1e-5


def setup_inputs(seed: int = 0, part: int = 0) -> dict:
    root_key = jax.random.key(seed)
    part_key = jax.random.fold_in(root_key, part)
    key_base, key_noise, key_cot = jax.random.split(part_key, 3)
    weight_keys = jax.random.split(root_key, 6)
    shape_act = (NUM_SEQS, SEQ_LEN, MODEL_DIM)
    seq_base = jax.random.normal(key_base, (NUM_SEQS, 1, MODEL_DIM), jnp.float32)
    tok_noise = jax.random.normal(key_noise, shape_act, jnp.float32)
    x_in = (0.7 * seq_base + tok_noise).astype(jnp.bfloat16)
    gain_attn = jax.random.uniform(weight_keys[0], (NUM_LAYERS, MODEL_DIM), jnp.float32, 0.5, 1.5)
    w_qkv = (jax.random.normal(weight_keys[1], (NUM_LAYERS, MODEL_DIM, 3, NUM_HEADS, HEAD_DIM), jnp.float32) * MODEL_DIM ** -0.5).astype(jnp.bfloat16)
    w_out = (jax.random.normal(weight_keys[2], (NUM_LAYERS, NUM_HEADS, HEAD_DIM, MODEL_DIM), jnp.float32) * MODEL_DIM ** -0.5).astype(jnp.bfloat16)
    gain_mlp = jax.random.uniform(weight_keys[3], (NUM_LAYERS, MODEL_DIM), jnp.float32, 0.5, 1.5)
    w_up = (jax.random.normal(weight_keys[4], (NUM_LAYERS, MODEL_DIM, FFN_DIM), jnp.float32) * MODEL_DIM ** -0.5).astype(jnp.bfloat16)
    w_down = (jax.random.normal(weight_keys[5], (NUM_LAYERS, FFN_DIM, MODEL_DIM), jnp.float32) * FFN_DIM ** -0.5).astype(jnp.bfloat16)
    dy_out = jax.random.normal(key_cot, shape_act, jnp.float32).astype(jnp.bfloat16)
    return {'x_in': x_in, 'gain_attn': gain_attn, 'w_qkv': w_qkv, 'w_out': w_out, 'gain_mlp': gain_mlp, 'w_up': w_up, 'w_down': w_down, 'dy_out': dy_out}


def layer_norm(resid_f32, gain_vec):
    mean_val = jnp.mean(resid_f32, axis=-1, keepdims=True)
    centered = resid_f32 - mean_val
    variance = jnp.mean(centered * centered, axis=-1, keepdims=True)
    return centered * lax.rsqrt(variance + LN_EPS) * gain_vec


def block_forward(x_cur, layer_params):
    gain_attn, w_qkv, w_out, gain_mlp, w_up, w_down = layer_params
    resid_in = x_cur.astype(jnp.float32)
    normed_a = layer_norm(resid_in, gain_attn).astype(jnp.bfloat16)
    qkv_act = jnp.einsum('bsd,dcne->bscne', normed_a.astype(jnp.float32), w_qkv.astype(jnp.float32)).astype(jnp.bfloat16)
    queries = qkv_act[:, :, 0].astype(jnp.float32)
    keys_act = qkv_act[:, :, 1].astype(jnp.float32)
    values = qkv_act[:, :, 2].astype(jnp.float32)
    scores = jnp.einsum('bqne,bkne->bnqk', queries, keys_act) * (HEAD_DIM ** -0.5)
    causal = jnp.arange(SEQ_LEN)[:, None] >= jnp.arange(SEQ_LEN)[None, :]
    attn_probs = jax.nn.softmax(jnp.where(causal, scores, -1e30), axis=-1).astype(jnp.bfloat16)
    attn_out = jnp.einsum('bnqk,bkne->bqne', attn_probs.astype(jnp.float32), values).astype(jnp.bfloat16)
    attn_proj = jnp.einsum('bqne,nef->bqf', attn_out.astype(jnp.float32), w_out.astype(jnp.float32))
    x_mid = (resid_in + attn_proj).astype(jnp.bfloat16)
    resid_mid = x_mid.astype(jnp.float32)
    normed_m = layer_norm(resid_mid, gain_mlp).astype(jnp.bfloat16)
    pre_act = jnp.einsum('bsd,df->bsf', normed_m.astype(jnp.float32), w_up.astype(jnp.float32))
    hidden = jax.nn.gelu(pre_act).astype(jnp.bfloat16)
    mlp_proj = jnp.einsum('bsf,fd->bsd', hidden.astype(jnp.float32), w_down.astype(jnp.float32))
    return (resid_mid + mlp_proj).astype(jnp.bfloat16)


def stack_forward(x_in, gain_attn, w_qkv, w_out, gain_mlp, w_up, w_down):
    block_remat = jax.checkpoint(block_forward)

    def scan_step(x_cur, layer_params):
        return block_remat(x_cur, layer_params), None

    return lax.scan(scan_step, x_in, (gain_attn, w_qkv, w_out, gain_mlp, w_up, w_down))[0]


def reference(x_in, gain_attn, w_qkv, w_out, gain_mlp, w_up, w_down, dy_out):
    y_out, pullback = jax.vjp(stack_forward, x_in, gain_attn, w_qkv, w_out, gain_mlp, w_up, w_down)
    dx_in, dgain_attn, dw_qkv, dw_out, dgain_mlp, dw_up, dw_down = pullback(dy_out)
    return (y_out, dx_in, dgain_attn, dw_qkv, dw_out, dgain_mlp, dw_up, dw_down)
```

```python
import jax
import jax.numpy as jnp
from jax import lax
from jax.sharding import Mesh
from jax.sharding import PartitionSpec as P

LN_EPS = 1e-5
CORES = 2
NSUB = 2
BF = jnp.bfloat16
F32 = jnp.float32


def dot(spec, a, b):
    return jnp.einsum(spec, a, b, preferred_element_type=F32)


def ln_parts(z):
    mu = jnp.mean(z, axis=-1, keepdims=True)
    c = z - mu
    var = jnp.mean(c * c, axis=-1, keepdims=True)
    r = lax.rsqrt(var + LN_EPS)
    return c * r, r


def ln_bwd(z, gain, d):
    xhat, r = ln_parts(z)
    dgain = jnp.sum(d * xhat, axis=0)
    h = d * gain
    m1 = jnp.mean(h, axis=-1, keepdims=True)
    m2 = jnp.mean(h * xhat, axis=-1, keepdims=True)
    return r * (h - m1 - xhat * m2), dgain


def probs(q, k, scale):
    n = q.shape[1]
    s = dot('bqne,bkne->bnqk', q, k) * scale
    causal = jnp.arange(n)[:, None] >= jnp.arange(n)[None, :]
    return jax.nn.softmax(jnp.where(causal, s, -1e30), axis=-1)


def solution(mesh):
    chips = mesh.shape['tp'] // CORES
    mesh3 = Mesh(mesh.devices.reshape(mesh.shape['dp'], chips, CORES), ('dp', 'chip', 'core'))
    TP = ('chip', 'core')

    def swap(v):
        return lax.ppermute(v, 'core', [(0, 1), (1, 0)])

    def step(x_in, gain_attn, w_qkv, w_out, gain_mlp, w_up, w_down, dy_out):
        ga, gm = gain_attn[0], gain_mlp[0]
        wqkv, wo, wu, wd = w_qkv[0], w_out[0], w_up[0], w_down[0]
        nseq, slen, dm = x_in.shape
        scale = wqkv.shape[-1] ** -0.5
        core = lax.axis_index('core')
        chip = lax.axis_index('chip')
        half = nseq // CORES
        cs = half // NSUB
        rows = cs * slen // chips

        def cut(v, mine, k):
            first = core if mine else 1 - core
            return lax.dynamic_slice_in_dim(v, first * half + cs * k, cs, axis=0)

        def shard(v):
            return lax.dynamic_slice_in_dim(v.reshape(cs * slen, dm), chip * rows, rows, axis=0)

        def rs(part_mine, part_other):
            got = swap(part_other.astype(BF))
            s = (part_mine + got.astype(F32)).astype(BF)
            return lax.psum_scatter(s.reshape(cs * slen, dm), 'chip', scatter_dimension=0, tiled=True)

        def ag(v):
            mine = lax.all_gather(v, 'chip', axis=0, tiled=True)
            return mine, swap(mine)

        A, QKV, O = {}, {}, {}
        xm, nm, nmg = [], [], {}
        for k in range(NSUB):
            part = {}
            for mine in (False, True):
                xc = cut(x_in, mine, k)
                xh, _ = ln_parts(xc.astype(F32))
                a = (xh * ga).astype(BF)
                qkv = dot('bsd,dcne->bscne', a, wqkv).astype(BF)
                p = probs(qkv[:, :, 0], qkv[:, :, 1], scale).astype(BF)
                o = dot('bnqk,bkne->bqne', p, qkv[:, :, 2]).astype(BF)
                part[mine] = dot('bqne,nef->bqf', o, wo)
                A[mine, k], QKV[mine, k], O[mine, k] = a, qkv, o
            r = rs(part[True], part[False])
            xs = (shard(cut(x_in, True, k)).astype(F32) + r.astype(F32)).astype(BF)
            xm.append(xs)
            xh, _ = ln_parts(xs.astype(F32))
            nmg[True, k], nmg[False, k] = ag((xh * gm).astype(BF))
        H, DP = {}, {}
        gmid, gms, ys, dgm = {}, [], [], 0.
        for k in range(NSUB):
            part, part_y = {}, {}
            for mine in (False, True):
                b = nmg[mine, k]
                pre = dot('td,df->tf', b, wu)
                act, pull = jax.vjp(jax.nn.gelu, pre)
                h = act.astype(BF)
                dyc = cut(dy_out, mine, k).reshape(cs * slen, dm)
                dh = dot('td,fd->tf', dyc, wd).astype(BF)
                dp = pull(dh.astype(F32))[0].astype(BF)
                part[mine] = dot('tf,df->td', dp, wu)
                part_y[mine] = dot('tf,fd->td', h, wd)
                H[mine, k], DP[mine, k] = h, dp
            r = rs(part[True], part[False])
            dr, dg = ln_bwd(xm[k].astype(F32), gm, r.astype(F32))
            dgm = dgm + dg
            gs = (shard(cut(dy_out, True, k)).astype(F32) + dr).astype(BF)
            gms.append(gs)
            gmid[True, k], gmid[False, k] = ag(gs)
            ry = rs(part_y[True], part_y[False])
            ys.append((xm[k].astype(F32) + ry.astype(F32)).astype(BF))
        DQKV = {}
        dxs, dga = [], 0.
        for k in range(NSUB):
            part = {}
            for mine in (False, True):
                g = gmid[mine, k].reshape(cs, slen, dm)
                qkv = QKV[mine, k]
                q, kk, v = qkv[:, :, 0], qkv[:, :, 1], qkv[:, :, 2]
                do = dot('bqf,nef->bqne', g, wo).astype(BF)
                pf = probs(q, kk, scale)
                pb = pf.astype(BF)
                dv = dot('bnqk,bqne->bkne', pb, do).astype(BF)
                dpr = dot('bqne,bkne->bnqk', do, v).astype(BF).astype(F32)
                ds = pf * (dpr - jnp.sum(dpr * pf, axis=-1, keepdims=True))
                ds = (ds * scale).astype(BF)
                dq = dot('bnqk,bkne->bqne', ds, kk).astype(BF)
                dk = dot('bnqk,bqne->bkne', ds, q).astype(BF)
                dqkv = jnp.stack([dq, dk, dv], axis=2)
                DQKV[mine, k] = dqkv
                part[mine] = dot('bscne,dcne->bsd', dqkv, wqkv)
            r = rs(part[True], part[False])
            dr, dg = ln_bwd(shard(cut(x_in, True, k)).astype(F32), ga, r.astype(F32))
            dga = dga + dg
            dxs.append((gms[k].astype(F32) + dr).astype(BF))

        order = [(m, k) for k in range(NSUB) for m in (False, True)]

        def cat(d):
            return jnp.concatenate([d[o] for o in order], axis=0)

        dys = jnp.concatenate([cut(dy_out, m, k) for m, k in order], axis=0).reshape(nseq * slen, dm)
        dw_down = dot('tf,td->fd', cat(H), dys).astype(BF)
        dw_up = dot('td,tf->df', cat(nmg), cat(DP)).astype(BF)
        g_all = cat(gmid).reshape(nseq, slen, dm)
        dw_out = dot('bqne,bqf->nef', cat(O), g_all).astype(BF)
        dw_qkv = dot('bsd,bscne->dcne', cat(A), cat(DQKV)).astype(BF)

        def full(parts):
            mine = jnp.concatenate([lax.all_gather(v, 'chip', axis=0, tiled=True) for v in parts], axis=0)
            return lax.all_gather(mine, 'core', axis=0, tiled=True).reshape(nseq, slen, dm)

        y = full(ys)
        dx = full(dxs)
        dgains = lax.psum(jnp.stack([dgm, dga]), TP)
        return (y, dx, dgains[1:2], dw_qkv[None], dw_out[None], dgains[0:1], dw_up[None], dw_down[None])

    act = P('dp', None, None)
    in_specs = (act, P(None, None), P(None, None, None, TP, None), P(None, TP, None, None), P(None, None), P(None, None, TP), P(None, TP, None), act)
    out_specs = (act, act, P('dp', None), P('dp', None, None, TP, None), P('dp', TP, None, None), P('dp', None), P('dp', None, TP), P('dp', TP, None))
    return jax.shard_map(step, mesh=mesh3, in_specs=in_specs, out_specs=out_specs, check_vma=False)
```

```python
import functools

import jax
import jax.numpy as jnp
from jax import lax
from jax.experimental import pallas as pl
from jax.experimental.pallas import tpu as pltpu
from jax.sharding import PartitionSpec as P

LN_EPS = 1e-5
CORES = 2
CHIPS = 4
BF = jnp.bfloat16
F32 = jnp.float32
MESH = pl.DeviceIdType.MESH
VMEM_BYTES = 67043328
GELU_C = 0.7978845608028654
GELU_K = 0.044715
SLOTS = 3

ORDER = (
    ('d1', 4), ('f4', 22), ('b3', 8), ('c3', 9), ('f1', 6), ('c4', 17), ('a4', 15), ('F1', 0), ('MY', 7),
    ('e3', 12), ('d4', 18), ('a3', 7), ('d3', 10), ('MU', 6), ('e1', 5), ('c1', 2), ('b1', 1), ('a1', 0),
    ('B2', 14), ('MD', 6), ('e4', 20), ('f3', 13), ('b4', 15),
)


def dg(a, b, ca, cb):
    return lax.dot_general(a, b, (((ca,), (cb,)), ((), ())), preferred_element_type=F32)


def ln_parts(z):
    mu = jnp.mean(z, axis=-1, keepdims=True)
    c = z - mu
    var = jnp.mean(c * c, axis=-1, keepdims=True)
    r = lax.rsqrt(var + LN_EPS)
    return c * r, r


def ln_bwd(z, gain, d):
    xhat, r = ln_parts(z)
    h = d * gain
    m1 = jnp.mean(h, axis=-1, keepdims=True)
    m2 = jnp.mean(h * xhat, axis=-1, keepdims=True)
    return r * (h - m1 - xhat * m2), jnp.sum(d * xhat, axis=0, keepdims=True)


def gelu_both(z):
    z2 = z * z
    t = jnp.tanh(GELU_C * (z + GELU_K * (z2 * z)))
    cdf = 0.5 * (1.0 + t)
    d = cdf + z * (0.5 * (1.0 - t * t)) * (GELU_C * (1.0 + (3.0 * GELU_K) * z2))
    return z * cdf, d


def tile_of(n, want):
    t = min(n, want)
    while n % t:
        t //= 2
    return t


def body(heads, x, dy, wqkv_h, wo_h, wu_h, wd_h, ga, gm,
         nm_o, g_o, dx_o, a_o, o_o, qkv_o, h_o, dp_o, dq_o, py_o, xm_o, dgain_o,
         wqkv, wo, wu, wd, S, RD, R1, R2, xb, ab, nb, dyb, gb, qb, qb2, dqb, dqt, ob, obt, hb_, dpb, pyb,
         xs, xm, gs, own, dgb, lsem, ssem, rsem):
    nseq, slen, dm = x.shape
    half = slen // CORES
    blk = half // CHIPS
    hb = blk // 2
    he = wo.shape[0]
    e = he // heads
    ff = wu.shape[1]
    scale = e ** -0.5
    tp = lax.axis_index('tp')
    chip = tp // CORES
    core = tp % CORES
    sib = chip * CORES + (1 - core)
    rchip = (chip + 1) % CHIPS
    lchip = (chip + CHIPS - 1) % CHIPS
    ochip = (chip + 2) % CHIPS
    right = rchip * CORES + core
    left = lchip * CORES + core

    def off(ch, co):
        return pl.multiple_of(co * half + ch * blk, blk)

    myoff = off(chip, core)

    def lc(src, dst, k):
        return pltpu.make_async_copy(src, dst, lsem.at[k])

    w1 = (lc(wqkv_h, wqkv, 0), lc(wo_h, wo, 1))
    w2 = (lc(wu_h, wu, 2), lc(wd_h, wd, 3))

    def ld_x(c):
        return lc(x.at[c], xb, 4)

    def ld_dy(c):
        return lc(dy.at[c], dyb, 5)

    def ld_nm(c):
        return lc(nm_o.at[c], nb, 6)

    def ld_g(c):
        return lc(g_o.at[c], gb, 7)

    def ld_q(c):
        return lc(qkv_o.at[c], qb2, 8)

    def st_a(c):
        return lc(ab, a_o.at[c], 9)

    def st_q(c):
        return lc(qb, qkv_o.at[c], 10)

    def st_o(c):
        return lc(ob, o_o.at[c], 11)

    def st_h(c):
        return lc(hb_, h_o.at[c], 12)

    def st_dp(c):
        return lc(dpb, dp_o.at[c], 13)

    def st_py(c):
        return lc(pyb, py_o.at[c], 14)

    def st_dq(c):
        return lc(dqb, dq_o.at[c], 15)

    xs_ld = lc(x.at[:, pl.ds(myoff, blk), :], xs, 16)
    dys_ld = lc(dy.at[:, pl.ds(myoff, blk), :], gs, 17)
    out_ref = {1: nm_o, 3: g_o, 4: dx_o}
    fset = {1: 0, 3: 1, 4: 0}

    def st_own(fl, c):
        return lc(own.at[fset[fl], c % 2], out_ref[fl].at[c, pl.ds(myoff, blk)], 19 + (fl // 2) * nseq + c)

    def rc(kind, fl, c, src, dst, dev):
        f = fl // 2
        return pltpu.make_async_remote_copy(
            src_ref=src, dst_ref=dst, send_sem=ssem.at[f, kind, c], recv_sem=rsem.at[f, kind, c],
            device_id={'tp': dev}, device_id_type=MESH)

    def c_pair(fl, c):
        f = fset[fl]
        return rc(0, fl, c, S.at[f, SLOTS], RD.at[f, c % SLOTS], sib)

    def rows(f, s, ch, second):
        return S.at[f, s, pl.ds(pl.multiple_of(ch * blk + second * hb, hb), hb)]

    def c_relay(fl, c, d):
        f, s = fset[fl], c % SLOTS
        return rc(1 + d, fl, c, rows(f, s, ochip, d), R1.at[f, s, d, 0], left if d else right)

    def c_direct(fl, c, d):
        f, s = fset[fl], c % SLOTS
        return rc(3 + d, fl, c, rows(f, s, lchip if d else rchip, 1 - d), R1.at[f, s, d, 1], left if d else right)

    def c_second(fl, c, d):
        f, s = fset[fl], c % SLOTS
        return rc(5 + d, fl, c, rows(f, s, lchip if d else rchip, d), R2.at[f, s, d], left if d else right)

    def c_own(fl, c, d):
        dev = (right, left, sib)[d]
        return rc(7 + d, fl, c, own.at[fset[fl], c % 2], out_ref[fl].at[c, pl.ds(myoff, blk)], dev)

    def c_fwd(fl, c, d):
        o = pl.multiple_of(off(rchip if d else lchip, core) + d * hb, hb)
        r = out_ref[fl].at[c, pl.ds(o, hb)]
        return rc(10 + d, fl, c, r, r, left if d else right)

    def c_cross(fl, c, d):
        o = off((lchip, rchip, ochip)[d], core)
        r = out_ref[fl].at[c, pl.ds(o, blk)]
        return rc(12 + d, fl, c, r, r, sib)

    def store_part(f, c, col, n, val):
        v = val.astype(BF)
        s = c % SLOTS
        i0 = s * (1 - core) + SLOTS * core
        i1 = s * core + SLOTS * (1 - core)
        S[f, i0, :, pl.ds(col, n)] = v[:half]
        S[f, i1, :, pl.ds(col, n)] = v[half:]

    def stage_a(fl, c):
        f, s = fset[fl], c % SLOTS
        c_pair(fl, c).wait_recv()
        c_pair(fl, c).wait_send()

        for st in {1: (st_a, st_q, st_o), 3: (st_h, st_dp), 4: (st_dq,)}[fl]:
            st(c).wait()

        def add(t, _):
            r = pl.ds(pl.multiple_of(t * hb, hb), hb)
            S[f, s, r] = (S[f, s, r].astype(F32) + RD[f, s, r].astype(F32)).astype(BF)
            return 0

        lax.fori_loop(0, half // hb, add, 0)
        for d in (0, 1):
            c_relay(fl, c, d).start()
        for d in (0, 1):
            c_direct(fl, c, d).start()

    def stage_b(fl, c):
        f, s = fset[fl], c % SLOTS
        for d in (0, 1):
            c_relay(fl, c, d).wait_recv()
        for d in (0, 1):
            o = pl.ds(pl.multiple_of((lchip if d else rchip) * blk + d * hb, hb), hb)
            S[f, s, o] = (S[f, s, o].astype(F32) + R1[f, s, d, 0].astype(F32)).astype(BF)
            c_second(fl, c, d).start()

    def stage_c(fl, c):
        f, s = fset[fl], c % SLOTS
        for d in (0, 1):
            c_direct(fl, c, d).wait_recv()
            c_second(fl, c, d).wait_recv()

        for k in (0, 1):
            q = pl.ds(k * hb, hb)
            o = pl.ds(pl.multiple_of(chip * blk + k * hb, hb), hb)
            tot = S[f, s, o].astype(F32) + R1[f, s, 1 - k, 1].astype(F32) + R2[f, s, k].astype(F32)
            if fl == 1:
                z = (xs[c, q].astype(F32) + tot).astype(BF)
                xm[c, q] = z
                xh, _ = ln_parts(z.astype(F32))
                own[f, c % 2, q] = (xh * gm[...]).astype(BF)
            elif fl == 3:
                dr, dgn = ln_bwd(xm[c, q].astype(F32), gm[...], tot)
                v = (gs[c, q].astype(F32) + dr).astype(BF)
                gs[c, q] = v
                own[f, c % 2, q] = v
                dgb[1:2] += dgn
            else:
                dr, dgn = ln_bwd(xs[c, q].astype(F32), ga[...], tot)
                own[f, c % 2, q] = (gs[c, q].astype(F32) + dr).astype(BF)
                dgb[0:1] += dgn
        for d in (0, 1, 2):
            c_own(fl, c, d).start()
        st_own(fl, c).start()
        for d in (0, 1):
            c_relay(fl, c, d).wait_send()
            c_direct(fl, c, d).wait_send()
            c_second(fl, c, d).wait_send()

    def stage_d(fl, c):
        for d in (1, 0):
            c_own(fl, c, 1 - d).wait_recv()
            c_fwd(fl, c, 1 - d).start()
        for d in (0, 1):
            c_cross(fl, c, d).start()
        for d in (0, 1, 2):
            c_own(fl, c, d).wait_send()
        st_own(fl, c).wait()

    def stage_e(fl, c):
        for d in (0, 1):
            c_fwd(fl, c, d).wait_recv()
        c_cross(fl, c, 2).start()

    def stage_f(fl, c):
        c_own(fl, c, 2).wait_recv()
        for d in (0, 1, 2):
            c_cross(fl, c, d).wait_recv()
        for d in (0, 1):
            c_fwd(fl, c, d).wait_send()
        for d in (0, 1, 2):
            c_cross(fl, c, d).wait_send()
        if fl == 1:
            ld_nm(c).start()
        if fl == 3:
            ld_g(c).start()

    def probs_t(q_ref, hd):
        qt = q_ref[pl.ds(pl.multiple_of(hd * e, e), e)]
        kt = q_ref[pl.ds(pl.multiple_of(he + hd * e, e), e)]
        vt = q_ref[pl.ds(pl.multiple_of(2 * he + hd * e, e), e)]
        s = dg(kt, qt, 0, 0) * scale
        keep = lax.broadcasted_iota(jnp.int32, (slen, slen), 0) <= lax.broadcasted_iota(jnp.int32, (slen, slen), 1)
        s = jnp.where(keep, s, -1e30)
        ex = jnp.exp(s - jnp.max(s, axis=0, keepdims=True))
        return qt, kt, vt, ex / jnp.sum(ex, axis=0, keepdims=True)

    def stage_F1(c):
        @pl.when(c == 0)
        def _():
            for w in w1:
                w.wait()
            xs_ld.wait()

        ld_x(c).wait()

        def ln(t, _):
            r = pl.ds(pl.multiple_of(t * hb, hb), hb)
            xh, _r = ln_parts(xb[r].astype(F32))
            ab[r] = (xh * ga[...]).astype(BF)
            return 0

        lax.fori_loop(0, slen // hb, ln, 0)
        st_a(c).start()

        @pl.when(c + 1 < nseq)
        def _():
            ld_x(c + 1).start()

        qt = tile_of(3 * he, 3 * he // 2)

        def qkv(t, _):
            r = pl.ds(pl.multiple_of(t * qt, qt), qt)
            qb[r] = dg(wqkv[r], ab[...], 1, 1).astype(BF)
            return 0

        lax.fori_loop(0, 3 * he // qt, qkv, 0)
        st_q(c).start()

        def head(hd, _):
            _q, _k, vt, p = probs_t(qb, hd)
            obt[pl.ds(pl.multiple_of(hd * e, e), e)] = dg(vt, p.astype(BF), 1, 0).astype(BF)
            return 0

        lax.fori_loop(0, heads, head, 0)
        tr = tile_of(he, 128)
        for t in range(he // tr):
            ob[:, t * tr:(t + 1) * tr] = obt[t * tr:(t + 1) * tr].T
        st_o(c).start()
        n = tile_of(dm, 1024)

        def proj(t, _):
            col = pl.multiple_of(t * n, n)
            store_part(0, c, col, n, dg(ob[...], wo[:, pl.ds(col, n)], 1, 0))
            return 0

        lax.fori_loop(0, dm // n, proj, 0)
        c_pair(1, c).start()

    def stage_MU(c):
        @pl.when(c == 0)
        def _():
            for w in w2:
                w.wait()
            dys_ld.wait()

        ld_nm(c).wait()
        ld_dy(c).wait()
        n = tile_of(ff, 512)

        def up(t, _):
            col = pl.ds(pl.multiple_of(t * n, n), n)
            pre = dg(nb[...], wu[:, col], 1, 0)
            dh = dg(dyb[...], wd[col], 1, 1)
            act, der = gelu_both(pre)
            hb_[:, col] = act.astype(BF)
            dpb[:, col] = (dh.astype(BF).astype(F32) * der).astype(BF)
            return 0

        lax.fori_loop(0, ff // n, up, 0)
        st_h(c).start()
        st_dp(c).start()

        @pl.when(c + 1 < nseq)
        def _():
            ld_dy(c + 1).start()

    m = tile_of(dm, 512)

    def stage_MD(c):
        def down(t, _):
            col = pl.multiple_of(t * m, m)
            store_part(1, c, col, m, dg(dpb[...], wu[pl.ds(col, m)], 1, 1))
            return 0

        lax.fori_loop(0, dm // m, down, 0)
        c_pair(3, c).start()

    def stage_MY(c):
        @pl.when(c > 0)
        def _():
            st_py(c - 1).wait()

        def outp(t, _):
            col = pl.multiple_of(t * m, m)
            pyb[:, pl.ds(col, m)] = dg(hb_[...], wd[:, pl.ds(col, m)], 1, 0).astype(BF)
            return 0

        lax.fori_loop(0, dm // m, outp, 0)
        st_py(c).start()

    def stage_B2(c):
        ld_q(c).start()
        ld_g(c).wait()
        obt[...] = dg(wo[...], gb[...], 1, 1).astype(BF)
        ld_q(c).wait()

        def head(hd, _):
            qt, kt, vt, p = probs_t(qb2, hd)
            do = obt[pl.ds(pl.multiple_of(hd * e, e), e)]
            dqt[pl.ds(pl.multiple_of(2 * he + hd * e, e), e)] = dg(do, p.astype(BF), 1, 1).astype(BF)
            dpr = dg(vt, do, 0, 0).astype(BF).astype(F32)
            ds = p * (dpr - jnp.sum(dpr * p, axis=0, keepdims=True))
            ds = (ds * scale).astype(BF)
            dqt[pl.ds(pl.multiple_of(hd * e, e), e)] = dg(kt, ds, 1, 0).astype(BF)
            dqt[pl.ds(pl.multiple_of(he + hd * e, e), e)] = dg(qt, ds, 1, 1).astype(BF)
            return 0

        lax.fori_loop(0, heads, head, 0)
        tr = tile_of(3 * he, 128)
        for t in range(3 * he // tr):
            dqb[:, t * tr:(t + 1) * tr] = dqt[t * tr:(t + 1) * tr].T
        st_dq(c).start()
        n = tile_of(dm, 512)

        def proj(t, _):
            col = pl.multiple_of(t * n, n)
            store_part(0, c, col, n, dg(dqb[...], wqkv[:, pl.ds(col, n)], 1, 0))
            return 0

        lax.fori_loop(0, dm // n, proj, 0)
        c_pair(4, c).start()

    barrier = pltpu.get_barrier_semaphore()
    for dev in (sib, left, right):
        pl.semaphore_signal(barrier, inc=1, device_id={'tp': dev}, device_id_type=MESH)
    ld_x(0).start()
    for w in w1:
        w.start()
    xs_ld.start()
    for w in w2:
        w.start()
    dys_ld.start()
    ld_dy(0).start()
    dgb[...] = jnp.zeros_like(dgb)
    pl.semaphore_wait(barrier, 3)

    run = {'F1': stage_F1, 'MU': stage_MU, 'MD': stage_MD, 'MY': stage_MY, 'B2': stage_B2}
    hops = {'a': stage_a, 'b': stage_b, 'c': stage_c, 'd': stage_d, 'e': stage_e, 'f': stage_f}
    order = ORDER

    def step(i, _):
        for name, lag in order:
            c = i - lag

            @pl.when((c >= 0) & (c < nseq))
            def _():
                if name in run:
                    run[name](c)
                else:
                    hops[name[0]](int(name[1]), c)
        return 0

    lax.fori_loop(0, nseq + max(l for _, l in order), step, 0)

    last = nseq - 1
    st_py(last).wait()
    xo = lc(xm, xm_o, 18)
    xo.start()
    dgain_o[...] = dgb[...]
    xo.wait()


def mega(x, dy, wqkv, wo, wu, wd, ga, gm, heads):
    nseq, slen, dm = x.shape
    he, ff = wo.shape[0], wu.shape[1]
    half = slen // CORES
    blk = half // CHIPS
    hb = blk // 2
    act = jax.ShapeDtypeStruct((nseq, slen, dm), BF)

    def arr(n, dt=BF):
        return jax.ShapeDtypeStruct((nseq, n, slen) if dt is None else (nseq, slen, n), BF)

    outs = (act, act, act, act, arr(he), jax.ShapeDtypeStruct((nseq, 3 * he, slen), BF), arr(ff), arr(ff), arr(3 * he), act,
            jax.ShapeDtypeStruct((nseq, blk, dm), BF), jax.ShapeDtypeStruct((2, dm), F32))
    hbm = pl.BlockSpec(memory_space=pl.ANY)
    vm = pl.BlockSpec(memory_space=pltpu.VMEM)
    V = pltpu.VMEM
    scratch = [
        V(wqkv.shape, BF), V(wo.shape, BF), V(wu.shape, BF), V(wd.shape, BF),
        V((2, SLOTS + 1, half, dm), BF), V((2, SLOTS, half, dm), BF),
        V((2, SLOTS, 2, 2, hb, dm), BF), V((2, SLOTS, 2, hb, dm), BF),
        V((slen, dm), BF), V((slen, dm), BF), V((slen, dm), BF), V((slen, dm), BF), V((slen, dm), BF),
        V((3 * he, slen), BF), V((3 * he, slen), BF), V((slen, 3 * he), BF), V((3 * he, slen), BF),
        V((slen, he), BF), V((he, slen), BF), V((slen, ff), BF), V((slen, ff), BF), V((slen, dm), BF),
        V((nseq, blk, dm), BF), V((nseq, blk, dm), BF), V((nseq, blk, dm), BF), V((2, 2, blk, dm), BF), V((2, dm), F32),
        pltpu.SemaphoreType.DMA((19 + 3 * nseq,)), pltpu.SemaphoreType.DMA((3, 15, nseq)), pltpu.SemaphoreType.DMA((3, 15, nseq)),
    ]
    flops = 2 * nseq * slen * dm * (4 * he * 2 + ff * 4)
    return pl.pallas_call(
        functools.partial(body, heads),
        name='mega',
        out_shape=outs,
        in_specs=[hbm] * 6 + [vm] * 2,
        out_specs=(hbm,) * 11 + (vm,),
        scratch_shapes=scratch,
        compiler_params=pltpu.CompilerParams(collective_id=0, has_side_effects=True, vmem_limit_bytes=VMEM_BYTES),
        cost_estimate=pl.CostEstimate(flops=flops, bytes_accessed=12 * nseq * slen * dm * 2, transcendentals=0),
    )(x, dy, wqkv, wo, wu, wd, ga, gm)


def solution(mesh):
    tpn = mesh.shape['tp']

    def hop(v, chips_by, cores_by):
        perm = []
        for t in range(tpn):
            ch, co = t // CORES, t % CORES
            perm.append((t, ((ch + chips_by) % CHIPS) * CORES + (co + cores_by) % CORES))
        return lax.ppermute(v, 'tp', perm)

    def reduce_and_gather(py, xm, chip, core):
        nseq, slen, dm = py.shape
        half = slen // CORES
        blk = half // CHIPS
        hb = blk // 2
        rchip, lchip, ochip = (chip + 1) % CHIPS, (chip + CHIPS - 1) % CHIPS, (chip + 2) % CHIPS

        def half_of(co):
            return lax.dynamic_slice_in_dim(py, co * half, half, axis=1)

        got = hop(half_of(1 - core), 0, 1)
        s = (half_of(core).astype(F32) + got.astype(F32)).astype(BF)

        def rows(ch, k):
            return lax.dynamic_slice_in_dim(s, ch * blk + k * hb, hb, axis=1)

        rel_l = hop(rows(ochip, 0), 1, 0)
        rel_r = hop(rows(ochip, 1), -1, 0)
        dir_l = hop(rows(rchip, 1), 1, 0)
        dir_r = hop(rows(lchip, 0), -1, 0)
        sec_l = hop((rows(rchip, 0).astype(F32) + rel_l.astype(F32)).astype(BF), 1, 0)
        sec_r = hop((rows(lchip, 1).astype(F32) + rel_r.astype(F32)).astype(BF), -1, 0)
        tot0 = rows(chip, 0).astype(F32) + dir_r.astype(F32) + sec_l.astype(F32)
        tot1 = rows(chip, 1).astype(F32) + dir_l.astype(F32) + sec_r.astype(F32)
        y = (xm.astype(F32) + jnp.concatenate([tot0, tot1], axis=1)).astype(BF)
        y_l, y_r = hop(y, 1, 0), hop(y, -1, 0)
        y_o = jnp.concatenate([hop(y_l[:, :hb], 1, 0), hop(y_r[:, hb:], -1, 0)], axis=1)
        out = jnp.zeros((nseq, half, dm), BF)
        for ch, v in ((chip, y), (lchip, y_l), (rchip, y_r), (ochip, y_o)):
            out = lax.dynamic_update_slice_in_dim(out, v, ch * blk, axis=1)
        other = hop(out, 0, 1)
        return jnp.where(core == 0, jnp.concatenate([out, other], axis=1), jnp.concatenate([other, out], axis=1))

    def step(x_in, gain_attn, w_qkv, w_out, gain_mlp, w_up, w_down, dy_out):
        nseq, slen, dm = x_in.shape
        heads, e = w_qkv.shape[3:]
        he = heads * e
        tp = lax.axis_index('tp')
        wqkv = jnp.transpose(w_qkv[0], (1, 2, 3, 0)).reshape(3 * he, dm)
        wo = w_out[0].reshape(he, dm)
        nm, g, dx, a, o, _qkv, h, dp, dq, py, xm, dgain = mega(
            x_in, dy_out, wqkv, wo, w_up[0], w_down[0], gain_attn, gain_mlp, heads)
        tok = nseq * slen

        def wg(p, q):
            return lax.dot_general(p.reshape(tok, -1), q.reshape(tok, -1), (((0,), (0,)), ((), ())),
                                   preferred_element_type=F32).astype(BF)

        y = reduce_and_gather(py, xm, tp // CORES, tp % CORES)
        dw_down = wg(h, dy_out)
        dw_up = wg(nm, dp)
        dw_out = wg(o, g)
        dw_qkv = wg(dq, a)
        dw_qkv = jnp.transpose(dw_qkv.reshape(3, heads, e, dm), (3, 0, 1, 2))
        dgain = lax.psum(dgain, 'tp')
        return (y, dx, dgain[0:1], dw_qkv[None], dw_out.reshape(1, heads, e, dm), dgain[1:2], dw_up[None], dw_down[None])

    act = P('dp', None, None)
    in_specs = (act, P(None, None), P(None, None, None, 'tp', None), P(None, 'tp', None, None), P(None, None),
                P(None, None, 'tp'), P(None, 'tp', None), act)
    out_specs = (act, act, P('dp', None), P('dp', None, None, 'tp', None), P('dp', 'tp', None, None), P('dp', None),
                 P('dp', None, 'tp'), P('dp', 'tp', None))
    return jax.shard_map(step, mesh=mesh, in_specs=in_specs, out_specs=out_specs, check_vma=False)
```

```python
import functools
import math

import jax
import jax.numpy as jnp
from jax import lax
from jax.experimental import pallas as pl
from jax.experimental.pallas import tpu as pltpu
from jax.sharding import PartitionSpec as P

LN_EPS = 1e-5
CORES = 2
CHIPS = 4
BF = jnp.bfloat16
F32 = jnp.float32
MESH = pl.DeviceIdType.MESH
VMEM_BYTES = 67043328
GELU_C = 0.7978845608028654
GELU_K = 0.044715
SLOTS = 3

ORDER = (
    ('e5', 27), ('f1', 6), ('c3', 9), ('c1', 3), ('b5', 23), ('b1', 2), ('b3', 8), ('a3', 7), ('f3', 14),
    ('e3', 13), ('d3', 10), ('MU', 6), ('a1', 1), ('c5', 24), ('a5', 22), ('d4', 19), ('c4', 17), ('YL', 21),
    ('d5', 25), ('f5', 28), ('e4', 22), ('MD', 6), ('b4', 16), ('d1', 4), ('e1', 5), ('F1', 0), ('YS', 21),
    ('a4', 15), ('WG', 22), ('MY', 6), ('f4', 23), ('B2', 14),
)


def dg(a, b, ca, cb):
    return lax.dot_general(a, b, (((ca,), (cb,)), ((), ())), preferred_element_type=F32)


def ln_parts(z):
    mu = jnp.mean(z, axis=-1, keepdims=True)
    c = z - mu
    var = jnp.mean(c * c, axis=-1, keepdims=True)
    r = lax.rsqrt(var + LN_EPS)
    return c * r, r


def ln_bwd(z, gain, d):
    xhat, r = ln_parts(z)
    h = d * gain
    m1 = jnp.mean(h, axis=-1, keepdims=True)
    m2 = jnp.mean(h * xhat, axis=-1, keepdims=True)
    return r * (h - m1 - xhat * m2), jnp.sum(d * xhat, axis=0, keepdims=True)


def gelu_both(z):
    z2 = z * z
    t = jnp.tanh(GELU_C * (z + GELU_K * (z2 * z)))
    cdf = 0.5 * (1.0 + t)
    d = cdf + z * (0.5 * (1.0 - t * t)) * (GELU_C * (1.0 + (3.0 * GELU_K) * z2))
    return z * cdf, d


def tile_of(n, want):
    t = min(n, want)
    while n % t:
        t //= 2
    return t


def body(heads, x, dy, dyf, wqkv_h, wo_h, wu_h, wd_h, ga, gm,
         y_o, dx_o, dwq_o, dwo_o, dwu_o, dwd_o, nm_o, g_o, a_o, o_o, qkv_o, h_o, dp_o, dq_o, py_o, dgain_o,
         wqkv, wo, wu, wd, S, RD, R1, R2, xb, ab, nb, dyb, gb, qb, qb2, dqb, dqt, ob, obt, hb_, dpb, pyb,
         xs, xm, gs, own, dgb, dgs, lsem, wsem, dsem, ssem, rsem):
    nseq, slen, dm = x.shape
    tok = nseq * slen
    half = slen // CORES
    blk = half // CHIPS
    hb = blk // 2
    he = wo.shape[0]
    e = he // heads
    ff = wu.shape[1]
    scale = e ** -0.5
    tpn = CHIPS * CORES
    tp = lax.axis_index('tp')
    chip = tp // CORES
    core = tp % CORES
    sib = chip * CORES + (1 - core)
    rchip = (chip + 1) % CHIPS
    lchip = (chip + CHIPS - 1) % CHIPS
    ochip = (chip + 2) % CHIPS
    right = rchip * CORES + core
    left = lchip * CORES + core

    def seq(c):
        return pl.ds(pl.multiple_of(c * slen, slen), slen)

    def off(ch, co):
        return pl.multiple_of(co * half + ch * blk, blk)

    myoff = off(chip, core)

    def lc(src, dst, k):
        return pltpu.make_async_copy(src, dst, lsem.at[k])

    w1 = (lc(wqkv_h, wqkv, 0), lc(wo_h, wo, 1))
    w2 = (lc(wu_h, wu, 2), lc(wd_h, wd, 3))

    def ld_x(c):
        return lc(x.at[c], xb, 4)

    def ld_dy(c):
        return lc(dy.at[c], dyb, 5)

    def ld_nm(c):
        return lc(nm_o.at[seq(c)], nb, 6)

    def ld_g(c):
        return lc(g_o.at[seq(c)], gb, 7)

    def ld_q(c):
        return lc(qkv_o.at[c], qb2, 8)

    def st_a(c):
        return lc(ab, a_o.at[seq(c)], 9)

    def st_q(c):
        return lc(qb, qkv_o.at[c], 10)

    def st_o(c):
        return lc(ob, o_o.at[seq(c)], 11)

    def st_h(c):
        return lc(hb_, h_o.at[seq(c)], 12)

    def st_dp(c):
        return lc(dpb, dp_o.at[seq(c)], 13)

    def st_py(c):
        return lc(pyb, py_o.at[seq(c)], 14)

    def st_dq(c):
        return lc(dqb, dq_o.at[seq(c)], 15)

    xs_ld = lc(x.at[:, pl.ds(myoff, blk), :], xs, 16)
    dys_ld = lc(dy.at[:, pl.ds(myoff, blk), :], gs, 17)
    out_ref = {1: nm_o, 3: g_o, 4: dx_o, 5: y_o}
    fset = {1: 0, 3: 1, 4: 0, 5: 1}
    semset = {1: 0, 3: 1, 4: 2, 5: 3}

    def out_rows(fl, c, o, n):
        return out_ref[fl].at[pl.ds(pl.multiple_of(c * slen + o, n), n)]

    def st_own(fl, c):
        return lc(own.at[fset[fl], c % 2], out_rows(fl, c, myoff, blk), 21 + semset[fl] * nseq + c)

    def rc(kind, fl, c, src, dst, dev):
        f = semset[fl]
        return pltpu.make_async_remote_copy(
            src_ref=src, dst_ref=dst, send_sem=ssem.at[f, kind, c], recv_sem=rsem.at[f, kind, c],
            device_id={'tp': dev}, device_id_type=MESH)

    def c_pair(fl, c):
        f = fset[fl]
        return rc(0, fl, c, S.at[f, SLOTS], RD.at[f, c % SLOTS], sib)

    def rows(f, s, ch, second):
        return S.at[f, s, pl.ds(pl.multiple_of(ch * blk + second * hb, hb), hb)]

    def c_relay(fl, c, d):
        f, s = fset[fl], c % SLOTS
        return rc(1 + d, fl, c, rows(f, s, ochip, d), R1.at[f, s, d, 0], left if d else right)

    def c_direct(fl, c, d):
        f, s = fset[fl], c % SLOTS
        return rc(3 + d, fl, c, rows(f, s, lchip if d else rchip, 1 - d), R1.at[f, s, d, 1], left if d else right)

    def c_second(fl, c, d):
        f, s = fset[fl], c % SLOTS
        return rc(5 + d, fl, c, rows(f, s, lchip if d else rchip, d), R2.at[f, s, d], left if d else right)

    def c_own(fl, c, d):
        dev = (right, left, sib)[d]
        return rc(7 + d, fl, c, own.at[fset[fl], c % 2], out_rows(fl, c, myoff, blk), dev)

    def c_fwd(fl, c, d):
        r = out_rows(fl, c, off(rchip if d else lchip, core) + d * hb, hb)
        return rc(10 + d, fl, c, r, r, left if d else right)

    def c_cross(fl, c, d):
        r = out_rows(fl, c, off((lchip, rchip, ochip)[d], core), blk)
        return rc(12 + d, fl, c, r, r, sib)

    def c_gain(k):
        return pltpu.make_async_remote_copy(
            src_ref=dgb, dst_ref=dgs.at[tp], send_sem=dsem.at[0, k], recv_sem=dsem.at[1, k],
            device_id={'tp': (tp + k) % tpn}, device_id_type=MESH)

    def store_part(f, c, col, n, val):
        v = val.astype(BF)
        s = c % SLOTS
        i0 = s * (1 - core) + SLOTS * core
        i1 = s * core + SLOTS * (1 - core)
        S[f, i0, :, pl.ds(col, n)] = v[:half]
        S[f, i1, :, pl.ds(col, n)] = v[half:]

    def stage_a(fl, c):
        f, s = fset[fl], c % SLOTS
        c_pair(fl, c).wait_recv()
        c_pair(fl, c).wait_send()

        for st in {1: (st_a, st_q, st_o), 3: (st_h, st_dp), 4: (st_dq,), 5: ()}[fl]:
            st(c).wait()

        def add(t, _):
            r = pl.ds(pl.multiple_of(t * hb, hb), hb)
            S[f, s, r] = (S[f, s, r].astype(F32) + RD[f, s, r].astype(F32)).astype(BF)
            return 0

        lax.fori_loop(0, half // hb, add, 0)
        for d in (0, 1):
            c_relay(fl, c, d).start()
        for d in (0, 1):
            c_direct(fl, c, d).start()

    def stage_b(fl, c):
        f, s = fset[fl], c % SLOTS
        for d in (0, 1):
            c_relay(fl, c, d).wait_recv()
        for d in (0, 1):
            o = pl.ds(pl.multiple_of((lchip if d else rchip) * blk + d * hb, hb), hb)
            S[f, s, o] = (S[f, s, o].astype(F32) + R1[f, s, d, 0].astype(F32)).astype(BF)
            c_second(fl, c, d).start()

    def stage_c(fl, c):
        f, s = fset[fl], c % SLOTS
        for d in (0, 1):
            c_direct(fl, c, d).wait_recv()
            c_second(fl, c, d).wait_recv()

        for k in (0, 1):
            q = pl.ds(k * hb, hb)
            o = pl.ds(pl.multiple_of(chip * blk + k * hb, hb), hb)
            tot = S[f, s, o].astype(F32) + R1[f, s, 1 - k, 1].astype(F32) + R2[f, s, k].astype(F32)
            if fl == 1:
                z = (xs[c, q].astype(F32) + tot).astype(BF)
                xm[c, q] = z
                xh, _ = ln_parts(z.astype(F32))
                own[f, c % 2, q] = (xh * gm[...]).astype(BF)
            elif fl == 3:
                dr, dgn = ln_bwd(xm[c, q].astype(F32), gm[...], tot)
                v = (gs[c, q].astype(F32) + dr).astype(BF)
                gs[c, q] = v
                own[f, c % 2, q] = v
                dgb[1:2] += dgn
            elif fl == 5:
                own[f, c % 2, q] = (xm[c, q].astype(F32) + tot).astype(BF)
            else:
                dr, dgn = ln_bwd(xs[c, q].astype(F32), ga[...], tot)
                own[f, c % 2, q] = (gs[c, q].astype(F32) + dr).astype(BF)
                dgb[0:1] += dgn
        for d in (0, 1, 2):
            c_own(fl, c, d).start()
        st_own(fl, c).start()
        for d in (0, 1):
            c_relay(fl, c, d).wait_send()
            c_direct(fl, c, d).wait_send()
            c_second(fl, c, d).wait_send()
        if fl == 4:
            @pl.when(c == nseq - 1)
            def _():
                dgs[tp] = dgb[...]
                for k in range(1, tpn):
                    c_gain(k).start()

    def stage_d(fl, c):
        for d in (1, 0):
            c_own(fl, c, 1 - d).wait_recv()
            c_fwd(fl, c, 1 - d).start()
        for d in (0, 1):
            c_cross(fl, c, d).start()
        for d in (0, 1, 2):
            c_own(fl, c, d).wait_send()
        st_own(fl, c).wait()

    def stage_e(fl, c):
        for d in (0, 1):
            c_fwd(fl, c, d).wait_recv()
        c_cross(fl, c, 2).start()

    def stage_f(fl, c):
        c_own(fl, c, 2).wait_recv()
        for d in (0, 1, 2):
            c_cross(fl, c, d).wait_recv()
        for d in (0, 1):
            c_fwd(fl, c, d).wait_send()
        for d in (0, 1, 2):
            c_cross(fl, c, d).wait_send()
        if fl == 1:
            ld_nm(c).start()
        if fl == 3:
            ld_g(c).start()

    def probs_t(q_ref, hd):
        qt = q_ref[pl.ds(pl.multiple_of(hd * e, e), e)]
        kt = q_ref[pl.ds(pl.multiple_of(he + hd * e, e), e)]
        vt = q_ref[pl.ds(pl.multiple_of(2 * he + hd * e, e), e)]
        s = dg(kt, qt, 0, 0) * scale
        keep = lax.broadcasted_iota(jnp.int32, (slen, slen), 0) <= lax.broadcasted_iota(jnp.int32, (slen, slen), 1)
        s = jnp.where(keep, s, -1e30)
        ex = jnp.exp(s - jnp.max(s, axis=0, keepdims=True))
        return qt, kt, vt, ex / jnp.sum(ex, axis=0, keepdims=True)

    def stage_F1(c):
        @pl.when(c == 0)
        def _():
            for w in w1:
                w.wait()
            xs_ld.wait()

        ld_x(c).wait()

        def ln(t, _):
            r = pl.ds(pl.multiple_of(t * hb, hb), hb)
            xh, _r = ln_parts(xb[r].astype(F32))
            ab[r] = (xh * ga[...]).astype(BF)
            return 0

        lax.fori_loop(0, slen // hb, ln, 0)
        st_a(c).start()

        @pl.when(c + 1 < nseq)
        def _():
            ld_x(c + 1).start()

        qt = tile_of(3 * he, 3 * he // 2)

        def qkv(t, _):
            r = pl.ds(pl.multiple_of(t * qt, qt), qt)
            qb[r] = dg(wqkv[r], ab[...], 1, 1).astype(BF)
            return 0

        lax.fori_loop(0, 3 * he // qt, qkv, 0)
        st_q(c).start()

        def head(hd, _):
            _q, _k, vt, p = probs_t(qb, hd)
            obt[pl.ds(pl.multiple_of(hd * e, e), e)] = dg(vt, p.astype(BF), 1, 0).astype(BF)
            return 0

        lax.fori_loop(0, heads, head, 0)
        tr = tile_of(he, 128)
        for t in range(he // tr):
            ob[:, t * tr:(t + 1) * tr] = obt[t * tr:(t + 1) * tr].T
        st_o(c).start()
        n = tile_of(dm, 1024)

        def proj(t, _):
            col = pl.multiple_of(t * n, n)
            store_part(0, c, col, n, dg(ob[...], wo[:, pl.ds(col, n)], 1, 0))
            return 0

        lax.fori_loop(0, dm // n, proj, 0)
        c_pair(1, c).start()

    def stage_MU(c):
        @pl.when(c == 0)
        def _():
            for w in w2:
                w.wait()
            dys_ld.wait()

        ld_nm(c).wait()
        ld_dy(c).wait()
        n = tile_of(ff, 512)

        def up(t, _):
            col = pl.ds(pl.multiple_of(t * n, n), n)
            pre = dg(nb[...], wu[:, col], 1, 0)
            dh = dg(dyb[...], wd[col], 1, 1)
            act, der = gelu_both(pre)
            hb_[:, col] = act.astype(BF)
            dpb[:, col] = (dh.astype(BF).astype(F32) * der).astype(BF)
            return 0

        lax.fori_loop(0, ff // n, up, 0)
        st_h(c).start()
        st_dp(c).start()

        @pl.when(c + 1 < nseq)
        def _():
            ld_dy(c + 1).start()

    m = tile_of(dm, 512)

    def stage_MD(c):
        def down(t, _):
            col = pl.multiple_of(t * m, m)
            store_part(1, c, col, m, dg(dpb[...], wu[pl.ds(col, m)], 1, 1))
            return 0

        lax.fori_loop(0, dm // m, down, 0)
        c_pair(3, c).start()

    def stage_MY(c):
        @pl.when(c > 0)
        def _():
            st_py(c - 1).wait()

        def outp(t, _):
            col = pl.multiple_of(t * m, m)
            pyb[:, pl.ds(col, m)] = dg(hb_[...], wd[:, pl.ds(col, m)], 1, 0).astype(BF)
            return 0

        lax.fori_loop(0, dm // m, outp, 0)
        st_py(c).start()

    def stage_B2(c):
        @pl.when(c == nseq - 1)
        def _():
            start_a(0)
            for k in (0, 1):
                b_load(0, k).start()

        ld_q(c).start()
        ld_g(c).wait()
        obt[...] = dg(wo[...], gb[...], 1, 1).astype(BF)
        ld_q(c).wait()

        def head(hd, _):
            qt, kt, vt, p = probs_t(qb2, hd)
            do = obt[pl.ds(pl.multiple_of(hd * e, e), e)]
            dqt[pl.ds(pl.multiple_of(2 * he + hd * e, e), e)] = dg(do, p.astype(BF), 1, 1).astype(BF)
            dpr = dg(vt, do, 0, 0).astype(BF).astype(F32)
            ds = p * (dpr - jnp.sum(dpr * p, axis=0, keepdims=True))
            ds = (ds * scale).astype(BF)
            dqt[pl.ds(pl.multiple_of(hd * e, e), e)] = dg(kt, ds, 1, 0).astype(BF)
            dqt[pl.ds(pl.multiple_of(he + hd * e, e), e)] = dg(qt, ds, 1, 1).astype(BF)
            return 0

        lax.fori_loop(0, heads, head, 0)
        tr = tile_of(3 * he, 128)
        for t in range(3 * he // tr):
            dqb[:, t * tr:(t + 1) * tr] = dqt[t * tr:(t + 1) * tr].T
        st_dq(c).start()
        n = tile_of(dm, 512)

        def proj(t, _):
            col = pl.multiple_of(t * n, n)
            store_part(0, c, col, n, dg(dqb[...], wqkv[:, pl.ds(col, n)], 1, 0))
            return 0

        lax.fori_loop(0, dm // n, proj, 0)
        c_pair(4, c).start()

    def y_loads(c):
        s = c % SLOTS

        def part(co):
            return py_o.at[pl.ds(pl.multiple_of(c * slen + co * half, half), half)]

        return lc(part(1 - core), S.at[1, SLOTS], 19), lc(part(core), S.at[1, s], 20)

    def stage_YL(c):
        @pl.when(c == nseq - 1)
        def _():
            st_py(c).wait()

        for cp in y_loads(c):
            cp.start()

    def stage_YS(c):
        for cp in y_loads(c):
            cp.wait()
        c_pair(5, c).start()

    kh = tok // 2
    gemms = []
    for lhs, rhs, res in ((nm_o, dp_o, dwu_o), (h_o, dyf, dwd_o), (dq_o, a_o, dwq_o), (o_o, g_o, dwo_o)):
        for cb in range(rhs.shape[1] // ff):
            gemms.append((lhs, rhs, res, lhs.shape[1] // he, cb * ff))
    first = [sum(g[3] for g in gemms[:p]) for p in range(len(gemms) + 1)]
    tiles = first[-1]

    def a_buf(b, k):
        return wd.at[pl.ds(0, kh), pl.ds(pl.multiple_of((2 * b + k) * he, he), he)]

    def b_buf(p, k):
        return wqkv.at[pl.ds(0, kh), pl.ds(k * ff, ff)] if p % 2 else wu.at[pl.ds(k * kh, kh)]

    def o_buf(b):
        return wu.at[pl.ds(pl.multiple_of(tok + b * he, math.gcd(tok, he)), he)]

    def a_load(p, w, k):
        col = pl.multiple_of((w - first[p]) * he, he)
        return pltpu.make_async_copy(gemms[p][0].at[pl.ds(k * kh, kh), pl.ds(col, he)], a_buf(w % 2, k), wsem.at[k, w % 2])

    def b_load(p, k):
        return pltpu.make_async_copy(gemms[p][1].at[pl.ds(k * kh, kh), pl.ds(gemms[p][4], ff)], b_buf(p, k), wsem.at[2 + k, p % 2])

    def o_store(p, w):
        row = pl.multiple_of((w - first[p]) * he, he)
        return pltpu.make_async_copy(o_buf(w % 2), gemms[p][2].at[pl.ds(row, he), pl.ds(gemms[p][4], ff)], wsem.at[4, w % 2])

    def in_gemm(p, w):
        return (w >= first[p]) & (w < first[p + 1])

    def start_a(w):
        for p in range(len(gemms)):
            @pl.when(in_gemm(p, w))
            def _():
                for k in (0, 1):
                    a_load(p, w, k).start()

    def tile(w):
        for k in (0, 1):
            a_load(0, w % 2, k).wait()
        start_a(w + 1)
        for p in range(len(gemms)):
            @pl.when(w == first[p])
            def _():
                for k in (0, 1):
                    b_load(p, k).wait()
                if p + 1 < len(gemms):
                    for k in (0, 1):
                        b_load(p + 1, k).start()

        @pl.when(w >= 2)
        def _():
            o_store(0, w % 2).wait()

        n = tile_of(ff, 512)
        for odd in (0, 1):
            sel = functools.reduce(lambda u, v: u | v, [in_gemm(p, w) for p in range(len(gemms)) if p % 2 == odd])

            @pl.when(sel)
            def _():
                for j in range(ff // n):
                    acc = None
                    for k in (0, 1):
                        t = dg(a_buf(w % 2, k)[...], b_buf(odd, k)[:, pl.ds(j * n, n)], 0, 0)
                        acc = t if acc is None else acc + t
                    o_buf(w % 2)[:, pl.ds(j * n, n)] = acc.astype(BF)

        for p in range(len(gemms)):
            @pl.when(in_gemm(p, w))
            def _():
                o_store(p, w).start()

    def stage_WG(c):
        per = tiles // nseq

        def one(j, _):
            tile(c * per + j)
            return 0

        lax.fori_loop(0, per, one, 0)

    barrier = pltpu.get_barrier_semaphore()
    for k in range(1, tpn):
        pl.semaphore_signal(barrier, inc=1, device_id={'tp': (tp + k) % tpn}, device_id_type=MESH)
    ld_x(0).start()
    for w in w1:
        w.start()
    xs_ld.start()
    for w in w2:
        w.start()
    dys_ld.start()
    ld_dy(0).start()
    dgb[...] = jnp.zeros_like(dgb)
    pl.semaphore_wait(barrier, tpn - 1)

    run = {'F1': stage_F1, 'MU': stage_MU, 'MD': stage_MD, 'MY': stage_MY, 'B2': stage_B2,
           'YL': stage_YL, 'YS': stage_YS, 'WG': stage_WG}
    hops = {'a': stage_a, 'b': stage_b, 'c': stage_c, 'd': stage_d, 'e': stage_e, 'f': stage_f}
    order = ORDER

    def step(i, _):
        for name, lag in order:
            c = i - lag

            @pl.when((c >= 0) & (c < nseq))
            def _():
                if name in run:
                    run[name](c)
                else:
                    hops[name[0]](int(name[1]), c)
        return 0

    lax.fori_loop(0, nseq + max(l for _, l in order), step, 0)

    for b in (0, 1):
        o_store(0, b).wait()
    for k in range(1, tpn):
        c_gain(k).wait_recv()
    tot = dgs[0]
    for t in range(1, tpn):
        tot = tot + dgs[t]
    dgain_o[...] = tot
    for k in range(1, tpn):
        c_gain(k).wait_send()


def mega(x, dy, wqkv, wo, wu, wd, ga, gm, heads):
    nseq, slen, dm = x.shape
    he, ff = wo.shape[0], wu.shape[1]
    half = slen // CORES
    blk = half // CHIPS
    hb = blk // 2
    tok = nseq * slen

    def arr(*shape):
        return jax.ShapeDtypeStruct(shape, BF)

    act = arr(tok, dm)
    outs = (act, act, arr(3 * he, dm), arr(he, dm), arr(dm, ff), arr(ff, dm), act, act, act, arr(tok, he),
            arr(nseq, 3 * he, slen), arr(tok, ff), arr(tok, ff), arr(tok, 3 * he), act, jax.ShapeDtypeStruct((2, dm), F32))
    hbm = pl.BlockSpec(memory_space=pl.ANY)
    vm = pl.BlockSpec(memory_space=pltpu.VMEM)
    V = pltpu.VMEM
    scratch = [
        V(wqkv.shape, BF), V(wo.shape, BF), V(wu.shape, BF), V(wd.shape, BF),
        V((2, SLOTS + 1, half, dm), BF), V((2, SLOTS, half, dm), BF),
        V((2, SLOTS, 2, 2, hb, dm), BF), V((2, SLOTS, 2, hb, dm), BF),
        V((slen, dm), BF), V((slen, dm), BF), V((slen, dm), BF), V((slen, dm), BF), V((slen, dm), BF),
        V((3 * he, slen), BF), V((3 * he, slen), BF), V((slen, 3 * he), BF), V((3 * he, slen), BF),
        V((slen, he), BF), V((he, slen), BF), V((slen, ff), BF), V((slen, ff), BF), V((slen, dm), BF),
        V((nseq, blk, dm), BF), V((nseq, blk, dm), BF), V((nseq, blk, dm), BF), V((2, 2, blk, dm), BF), V((2, dm), F32),
        V((CHIPS * CORES, 2, dm), F32),
        pltpu.SemaphoreType.DMA((21 + 4 * nseq,)), pltpu.SemaphoreType.DMA((5, 2)), pltpu.SemaphoreType.DMA((2, CHIPS * CORES)),
        pltpu.SemaphoreType.DMA((4, 15, nseq)), pltpu.SemaphoreType.DMA((4, 15, nseq)),
    ]
    flops = 2 * nseq * slen * dm * (4 * he * 2 + ff * 4)
    return pl.pallas_call(
        functools.partial(body, heads),
        name='mega',
        out_shape=outs,
        in_specs=[hbm] * 7 + [vm] * 2,
        out_specs=(hbm,) * 15 + (vm,),
        scratch_shapes=scratch,
        compiler_params=pltpu.CompilerParams(collective_id=0, has_side_effects=True, vmem_limit_bytes=VMEM_BYTES),
        cost_estimate=pl.CostEstimate(flops=flops, bytes_accessed=12 * nseq * slen * dm * 2, transcendentals=0),
    )(x, dy, dy.reshape(tok, dm), wqkv, wo, wu, wd, ga, gm)


def solution(mesh):
    assert mesh.shape['tp'] == CHIPS * CORES

    def step(x_in, gain_attn, w_qkv, w_out, gain_mlp, w_up, w_down, dy_out):
        heads, e = w_qkv.shape[3:]
        dm = x_in.shape[2]
        he = heads * e
        wqkv = jnp.transpose(w_qkv[0], (1, 2, 3, 0)).reshape(3 * he, dm)
        wo = w_out[0].reshape(he, dm)
        out = mega(x_in, dy_out, wqkv, wo, w_up[0], w_down[0], gain_attn, gain_mlp, heads)
        y, dx, dwq, dwo, dwu, dwd = out[:6]
        dgain = out[-1]
        dwq = jnp.transpose(dwq.reshape(3, heads, e, dm), (3, 0, 1, 2))
        return (y.reshape(x_in.shape), dx.reshape(x_in.shape), dgain[0:1], dwq[None], dwo.reshape(1, heads, e, dm),
                dgain[1:2], dwu[None], dwd[None])

    act = P('dp', None, None)
    in_specs = (act, P(None, None), P(None, None, None, 'tp', None), P(None, 'tp', None, None), P(None, None),
                P(None, None, 'tp'), P(None, 'tp', None), act)
    out_specs = (act, act, P('dp', None), P('dp', None, None, 'tp', None), P('dp', 'tp', None, None), P('dp', None),
                 P('dp', None, 'tp'), P('dp', 'tp', None))
    return jax.shard_map(step, mesh=mesh, in_specs=in_specs, out_specs=out_specs, check_vma=False)
```

```python
import functools
import math

import jax
import jax.numpy as jnp
from jax import lax
from jax.experimental import pallas as pl
from jax.experimental.pallas import tpu as pltpu
from jax.sharding import PartitionSpec as P

LN_EPS = 1e-5
CORES = 2
CHIPS = 4
BF = jnp.bfloat16
F32 = jnp.float32
MESH = pl.DeviceIdType.MESH
VMEM_BYTES = 67043328
GELU_C = 0.7978845608028654
GELU_K = 0.044715
SLOTS = 3
PAIRS = 2

ORDER = (
    ('a3', 8), ('a5', 21), ('MU', 7), ('d3', 11), ('c4', 17), ('f4', 21), ('B2', 15), ('b4', 16), ('b1', 2),
    ('d5', 24), ('a4', 15), ('e1', 6), ('a1', 1), ('YL', 20), ('MD', 7), ('d1', 4), ('f3', 14), ('c3', 9),
    ('d4', 18), ('WG', 22), ('c5', 22), ('f1', 6), ('e5', 25), ('F1', 0), ('c1', 2), ('MY', 7), ('b5', 21),
    ('b3', 8), ('e4', 19), ('f5', 29), ('YS', 20), ('e3', 13),
)


def dg(a, b, ca, cb):
    return lax.dot_general(a, b, (((ca,), (cb,)), ((), ())), preferred_element_type=F32)


def ln_parts(z):
    mu = jnp.mean(z, axis=-1, keepdims=True)
    c = z - mu
    var = jnp.mean(c * c, axis=-1, keepdims=True)
    r = lax.rsqrt(var + LN_EPS)
    return c * r, r


def ln_bwd(z, gain, d):
    xhat, r = ln_parts(z)
    h = d * gain
    m1 = jnp.mean(h, axis=-1, keepdims=True)
    m2 = jnp.mean(h * xhat, axis=-1, keepdims=True)
    return r * (h - m1 - xhat * m2), jnp.sum(d * xhat, axis=0, keepdims=True)


def gelu_both(z):
    z2 = z * z
    t = jnp.tanh(GELU_C * (z + GELU_K * (z2 * z)))
    cdf = 0.5 * (1.0 + t)
    d = cdf + z * (0.5 * (1.0 - t * t)) * (GELU_C * (1.0 + (3.0 * GELU_K) * z2))
    return z * cdf, d


def tile_of(n, want):
    t = min(n, want)
    while n % t:
        t //= 2
    return t


def body(heads, x, dy, dyf, wqkv_h, wo_h, wu_h, wd_h, ga, gm,
         y_o, dx_o, dwq_o, dwo_o, dwu_o, dwd_o, nm_o, g_o, a_o, o_o, qkv_o, h_o, dp_o, dq_o, py_o, dgain_o,
         wqkv, wo, wu, wd, S, RD, R1, R2, xb, ab, nb, dyb, gb, qb, qb2, dqb, dqt, ob, obt, hb_, dpb, pyb,
         xs, xm, gs, own, dgb, dgs, lsem, wsem, dsem, ysem, ssem1, rsem1, ssem, rsem):
    nseq, slen, dm = x.shape
    tok = nseq * slen
    half = slen // CORES
    blk = half // CHIPS
    hb = blk // 2
    he = wo.shape[0]
    e = he // heads
    ff = wu.shape[1]
    scale = e ** -0.5
    tpn = CHIPS * CORES
    tp = lax.axis_index('tp')
    chip = tp // CORES
    core = tp % CORES
    sib = chip * CORES + (1 - core)
    rchip = (chip + 1) % CHIPS
    lchip = (chip + CHIPS - 1) % CHIPS
    ochip = (chip + 2) % CHIPS
    right = rchip * CORES + core
    left = lchip * CORES + core

    def seq(c):
        return pl.ds(pl.multiple_of(c * slen, slen), slen)

    def off(ch, co):
        return pl.multiple_of(co * half + ch * blk, blk)

    myoff = off(chip, core)

    def lc(src, dst, k):
        return pltpu.make_async_copy(src, dst, lsem.at[k])

    w1 = (lc(wqkv_h, wqkv, 0), lc(wo_h, wo, 1))
    w2 = (lc(wu_h, wu, 2), lc(wd_h, wd, 3))

    def ld_x(c):
        return lc(x.at[c], xb, 4)

    def ld_dy(c):
        return lc(dy.at[c], dyb, 5)

    def ld_nm(c):
        return lc(nm_o.at[seq(c)], nb, 6)

    def ld_g(c):
        return lc(g_o.at[seq(c)], gb, 7)

    def ld_q(c):
        return lc(qkv_o.at[c], qb2, 8)

    def st_a(c):
        return lc(ab, a_o.at[seq(c)], 9)

    def st_q(c):
        return lc(qb, qkv_o.at[c], 10)

    def st_o(c):
        return lc(ob, o_o.at[seq(c)], 11)

    def st_h(c):
        return lc(hb_, h_o.at[seq(c)], 12)

    def st_dp(c):
        return lc(dpb, dp_o.at[seq(c)], 13)

    def st_py(c):
        return lc(pyb, py_o.at[seq(c)], 14)

    def st_dq(c):
        return lc(dqb, dq_o.at[seq(c)], 15)

    xs_ld = lc(x.at[:, pl.ds(myoff, blk), :], xs, 16)
    dys_ld = lc(dy.at[:, pl.ds(myoff, blk), :], gs, 17)
    out_ref = {1: nm_o, 3: g_o, 4: dx_o, 5: y_o}
    fset = {1: 0, 3: 1, 4: 0, 5: 1}

    def out_rows(fl, c, o, n):
        return out_ref[fl].at[pl.ds(pl.multiple_of(c * slen + o, n), n)]

    def st_own(fl, c):
        return lc(own.at[fset[fl], c % 2], out_rows(fl, c, myoff, blk), 19 + fset[fl] * 2 + c % 2)

    def rc(kind, fl, c, src, dst, dev):
        f = fset[fl]
        if kind < 5:
            send, recv = ssem1.at[f, kind * SLOTS + c], rsem1.at[f, kind * SLOTS + c]
        else:
            send, recv = (m.at[f, (kind - 5) * nseq + c] for m in (ssem, rsem))
        return pltpu.make_async_remote_copy(
            src_ref=src, dst_ref=dst, send_sem=send, recv_sem=recv,
            device_id={'tp': dev}, device_id_type=MESH)

    def c_pair(fl, c):
        f = fset[fl]
        return rc(0, fl, c % PAIRS, S.at[f, SLOTS], RD.at[f, c % PAIRS], sib)

    def c_first(fl, c, d):
        f, s = fset[fl], c % SLOTS
        src = S.at[f, s, pl.ds(blk + hb if d else hb, blk)]
        return rc(1 + d, fl, c % SLOTS, src, R1.at[f, s, d], left if d else right)

    def c_second(fl, c, d):
        f, s = fset[fl], c % SLOTS
        src = S.at[f, s, pl.ds(2 * blk + hb if d else 0, hb)]
        return rc(3 + d, fl, c % SLOTS, src, R2.at[f, s, d], left if d else right)

    def c_own(fl, c, d):
        dev = (right, left, sib)[d]
        return rc(5 + d, fl, c, own.at[fset[fl], c % 2], out_rows(fl, c, myoff, blk), dev)

    def c_fwd(fl, c, d):
        r = out_rows(fl, c, off(rchip if d else lchip, core) + d * hb, hb)
        return rc(8 + d, fl, c, r, r, left if d else right)

    def c_cross(fl, c, d):
        r = out_rows(fl, c, off((lchip, rchip, ochip)[d], core), blk)
        return rc(10 + d, fl, c, r, r, sib)

    def c_gain(k):
        return pltpu.make_async_remote_copy(
            src_ref=dgb, dst_ref=dgs.at[tp], send_sem=dsem.at[0, k], recv_sem=dsem.at[1, k],
            device_id={'tp': (tp + k) % tpn}, device_id_type=MESH)

    def store_part(f, c, col, n, val):
        v = val.astype(BF)
        s = c % SLOTS
        i0 = s * (1 - core) + SLOTS * core
        i1 = s * core + SLOTS * (1 - core)
        for b in range(CHIPS):
            r = pl.ds(pl.multiple_of(((b + CHIPS - 1 - chip) % CHIPS) * blk, blk), blk)
            S[f, i0, r, pl.ds(col, n)] = v[b * blk:(b + 1) * blk]
            S[f, i1, r, pl.ds(col, n)] = v[half + b * blk:half + (b + 1) * blk]

    def stage_a(fl, c):
        f, s = fset[fl], c % SLOTS
        c_pair(fl, c).wait_recv()
        c_pair(fl, c).wait_send()
        for st in {1: (st_a, st_q, st_o), 3: (st_h, st_dp), 4: (st_dq,), 5: ()}[fl]:
            st(c).wait()

        def add(t, _):
            r = pl.ds(pl.multiple_of(t * hb, hb), hb)
            S[f, s, r] = (S[f, s, r].astype(F32) + RD[f, c % PAIRS, r].astype(F32)).astype(BF)
            return 0

        lax.fori_loop(0, half // hb, add, 0, unroll=2)
        for d in (0, 1):
            c_first(fl, c, d).start()

    def stage_b(fl, c):
        f, s = fset[fl], c % SLOTS
        for d in (0, 1):
            c_first(fl, c, d).wait_recv()
        for d in (0, 1):
            o = pl.ds(2 * blk + hb if d else 0, hb)
            S[f, s, o] = (S[f, s, o].astype(F32) + R1[f, s, d, pl.ds(0 if d else hb, hb)].astype(F32)).astype(BF)
            c_second(fl, c, d).start()

    def stage_c(fl, c):
        f, s = fset[fl], c % SLOTS
        for d in (0, 1):
            c_second(fl, c, d).wait_recv()

        for k in (0, 1):
            q = pl.ds(k * hb, hb)
            o = pl.ds(3 * blk + k * hb, hb)
            tot = S[f, s, o].astype(F32) + R1[f, s, 1 - k, pl.ds(0 if k else hb, hb)].astype(F32) + R2[f, s, k].astype(F32)
            if fl == 1:
                z = (xs[c, q].astype(F32) + tot).astype(BF)
                xm[c, q] = z
                xh, _ = ln_parts(z.astype(F32))
                own[f, c % 2, q] = (xh * gm[...]).astype(BF)
            elif fl == 3:
                dr, dgn = ln_bwd(xm[c, q].astype(F32), gm[...], tot)
                v = (gs[c, q].astype(F32) + dr).astype(BF)
                gs[c, q] = v
                own[f, c % 2, q] = v
                dgb[1:2] += dgn
            elif fl == 5:
                own[f, c % 2, q] = (xm[c, q].astype(F32) + tot).astype(BF)
            else:
                dr, dgn = ln_bwd(xs[c, q].astype(F32), ga[...], tot)
                own[f, c % 2, q] = (gs[c, q].astype(F32) + dr).astype(BF)
                dgb[0:1] += dgn
        for d in (0, 1, 2):
            c_own(fl, c, d).start()
        st_own(fl, c).start()
        for d in (0, 1):
            c_first(fl, c, d).wait_send()
            c_second(fl, c, d).wait_send()
        if fl == 4:
            @pl.when(c == nseq - 1)
            def _():
                dgs[tp] = dgb[...]
                for k in range(1, tpn):
                    c_gain(k).start()

    def stage_d(fl, c):
        for d in (1, 0):
            c_own(fl, c, 1 - d).wait_recv()
            c_fwd(fl, c, 1 - d).start()
        for d in (0, 1):
            c_cross(fl, c, d).start()
        for d in (0, 1, 2):
            c_own(fl, c, d).wait_send()
        st_own(fl, c).wait()

    def stage_e(fl, c):
        for d in (0, 1):
            c_fwd(fl, c, d).wait_recv()
        c_cross(fl, c, 2).start()

    def stage_f(fl, c):
        c_own(fl, c, 2).wait_recv()
        for d in (0, 1, 2):
            c_cross(fl, c, d).wait_recv()
        for d in (0, 1):
            c_fwd(fl, c, d).wait_send()
        for d in (0, 1, 2):
            c_cross(fl, c, d).wait_send()
        if fl == 1:
            ld_nm(c).start()
        if fl == 3:
            ld_g(c).start()

    def probs_t(q_ref, hd):
        qt = q_ref[pl.ds(pl.multiple_of(hd * e, e), e)]
        kt = q_ref[pl.ds(pl.multiple_of(he + hd * e, e), e)]
        vt = q_ref[pl.ds(pl.multiple_of(2 * he + hd * e, e), e)]
        s = dg(kt, qt, 0, 0) * scale
        keep = lax.broadcasted_iota(jnp.int32, (slen, slen), 0) <= lax.broadcasted_iota(jnp.int32, (slen, slen), 1)
        s = jnp.where(keep, s, -1e30)
        ex = jnp.exp(s - jnp.max(s, axis=0, keepdims=True))
        return qt, kt, vt, ex / jnp.sum(ex, axis=0, keepdims=True)

    def stage_F1(c):
        ld_x(c).wait()

        def ln(t, _):
            r = pl.ds(pl.multiple_of(t * hb, hb), hb)
            xh, _r = ln_parts(xb[r].astype(F32))
            ab[r] = (xh * ga[...]).astype(BF)
            return 0

        lax.fori_loop(0, slen // hb, ln, 0, unroll=4)
        st_a(c).start()

        @pl.when(c == 0)
        def _():
            for w in w1:
                w.wait()
            xs_ld.wait()

        @pl.when(c + 1 < nseq)
        def _():
            ld_x(c + 1).start()

        qt = tile_of(3 * he, 3 * he // 2)

        def qkv(t, _):
            r = pl.ds(pl.multiple_of(t * qt, qt), qt)
            qb[r] = dg(wqkv[r], ab[...], 1, 1).astype(BF)
            return 0

        lax.fori_loop(0, 3 * he // qt, qkv, 0)
        st_q(c).start()

        def head(hd, _):
            _q, _k, vt, p = probs_t(qb, hd)
            obt[pl.ds(pl.multiple_of(hd * e, e), e)] = dg(vt, p.astype(BF), 1, 0).astype(BF)
            return 0

        lax.fori_loop(0, heads, head, 0)
        tr = tile_of(he, 128)
        for t in range(he // tr):
            ob[:, t * tr:(t + 1) * tr] = obt[t * tr:(t + 1) * tr].T
        st_o(c).start()
        n = tile_of(dm, 1024)

        def proj(t, _):
            col = pl.multiple_of(t * n, n)
            store_part(0, c, col, n, dg(ob[...], wo[:, pl.ds(col, n)], 1, 0))
            return 0

        lax.fori_loop(0, dm // n, proj, 0)
        c_pair(1, c).start()

    def stage_MU(c):
        @pl.when(c == 0)
        def _():
            for w in w2:
                w.wait()
            dys_ld.wait()

        ld_nm(c).wait()
        ld_dy(c).wait()
        n = tile_of(ff, 512)

        def up(t, _):
            col = pl.ds(pl.multiple_of(t * n, n), n)
            pre = dg(nb[...], wu[:, col], 1, 0)
            dh = dg(dyb[...], wd[col], 1, 1)
            act, der = gelu_both(pre)
            hb_[:, col] = act.astype(BF)
            dpb[:, col] = (dh.astype(BF).astype(F32) * der).astype(BF)
            return 0

        lax.fori_loop(0, ff // n, up, 0)
        st_h(c).start()
        st_dp(c).start()

        @pl.when(c + 1 < nseq)
        def _():
            ld_dy(c + 1).start()

    m = tile_of(dm, 512)

    def stage_MD(c):
        def down(t, _):
            col = pl.multiple_of(t * m, m)
            store_part(1, c, col, m, dg(dpb[...], wu[pl.ds(col, m)], 1, 1))
            return 0

        lax.fori_loop(0, dm // m, down, 0)
        c_pair(3, c).start()

    def stage_MY(c):
        @pl.when(c > 0)
        def _():
            st_py(c - 1).wait()

        def outp(t, _):
            col = pl.multiple_of(t * m, m)
            pyb[:, pl.ds(col, m)] = dg(hb_[...], wd[:, pl.ds(col, m)], 1, 0).astype(BF)
            return 0

        lax.fori_loop(0, dm // m, outp, 0)
        st_py(c).start()

    def stage_B2(c):
        @pl.when(c == nseq - 1)
        def _():
            start_a(0)
            for k in (0, 1):
                b_load(0, k).start()

        ld_q(c).start()
        ld_g(c).wait()
        obt[...] = dg(wo[...], gb[...], 1, 1).astype(BF)
        ld_q(c).wait()

        def head(hd, _):
            qt, kt, vt, p = probs_t(qb2, hd)
            do = obt[pl.ds(pl.multiple_of(hd * e, e), e)]
            dqt[pl.ds(pl.multiple_of(2 * he + hd * e, e), e)] = dg(do, p.astype(BF), 1, 1).astype(BF)
            dpr = dg(vt, do, 0, 0).astype(BF).astype(F32)
            ds = p * (dpr - jnp.sum(dpr * p, axis=0, keepdims=True))
            ds = (ds * scale).astype(BF)
            dqt[pl.ds(pl.multiple_of(hd * e, e), e)] = dg(kt, ds, 1, 0).astype(BF)
            dqt[pl.ds(pl.multiple_of(he + hd * e, e), e)] = dg(qt, ds, 1, 1).astype(BF)
            return 0

        lax.fori_loop(0, heads, head, 0)
        tr = tile_of(3 * he, 128)
        for t in range(3 * he // tr):
            dqb[:, t * tr:(t + 1) * tr] = dqt[t * tr:(t + 1) * tr].T
        st_dq(c).start()
        n = tile_of(dm, 512)

        def proj(t, _):
            col = pl.multiple_of(t * n, n)
            store_part(0, c, col, n, dg(dqb[...], wqkv[:, pl.ds(col, n)], 1, 0))
            return 0

        lax.fori_loop(0, dm // n, proj, 0)
        c_pair(4, c).start()

    def y_loads(c):
        s = c % SLOTS

        cps = []
        for b in range(CHIPS):
            ch = (chip + 1 + b) % CHIPS
            for k, (co, t) in enumerate(((1 - core, SLOTS), (core, s))):
                src = py_o.at[pl.ds(pl.multiple_of(c * slen + co * half + ch * blk, blk), blk)]
                cps.append(pltpu.make_async_copy(src, S.at[1, t, pl.ds(b * blk, blk)], ysem.at[k, b]))
        return cps

    def stage_YL(c):
        @pl.when(c == nseq - 1)
        def _():
            st_py(c).wait()

        for cp in y_loads(c):
            cp.start()

    def stage_YS(c):
        for cp in y_loads(c):
            cp.wait()
        c_pair(5, c).start()

    kh = tok // 2
    gemms = []
    for lhs, rhs, res in ((nm_o, dp_o, dwu_o), (h_o, dyf, dwd_o), (dq_o, a_o, dwq_o), (o_o, g_o, dwo_o)):
        for cb in range(rhs.shape[1] // ff):
            gemms.append((lhs, rhs, res, lhs.shape[1] // he, cb * ff))
    first = [sum(g[3] for g in gemms[:p]) for p in range(len(gemms) + 1)]
    tiles = first[-1]

    def a_buf(b, k):
        return wd.at[pl.ds(0, kh), pl.ds(pl.multiple_of((2 * b + k) * he, he), he)]

    def b_buf(p, k):
        return wqkv.at[pl.ds(0, kh), pl.ds(k * ff, ff)] if p % 2 else wu.at[pl.ds(k * kh, kh)]

    def o_buf(b):
        return wu.at[pl.ds(pl.multiple_of(tok + b * he, math.gcd(tok, he)), he)]

    def a_load(p, w, k):
        col = pl.multiple_of((w - first[p]) * he, he)
        return pltpu.make_async_copy(gemms[p][0].at[pl.ds(k * kh, kh), pl.ds(col, he)], a_buf(w % 2, k), wsem.at[k, w % 2])

    def b_load(p, k):
        return pltpu.make_async_copy(gemms[p][1].at[pl.ds(k * kh, kh), pl.ds(gemms[p][4], ff)], b_buf(p, k), wsem.at[2 + k, p % 2])

    def o_store(p, w):
        row = pl.multiple_of((w - first[p]) * he, he)
        return pltpu.make_async_copy(o_buf(w % 2), gemms[p][2].at[pl.ds(row, he), pl.ds(gemms[p][4], ff)], wsem.at[4, w % 2])

    def in_gemm(p, w):
        return (w >= first[p]) & (w < first[p + 1])

    def start_a(w):
        for p in range(len(gemms)):
            @pl.when(in_gemm(p, w))
            def _():
                for k in (0, 1):
                    a_load(p, w, k).start()

    def tile(w):
        for k in (0, 1):
            a_load(0, w % 2, k).wait()
        start_a(w + 1)
        for p in range(len(gemms)):
            @pl.when(w == first[p])
            def _():
                for k in (0, 1):
                    b_load(p, k).wait()
                if p + 1 < len(gemms):
                    for k in (0, 1):
                        b_load(p + 1, k).start()

        @pl.when(w >= 2)
        def _():
            o_store(0, w % 2).wait()

        n = tile_of(ff, 512)
        for odd in (0, 1):
            sel = functools.reduce(lambda u, v: u | v, [in_gemm(p, w) for p in range(len(gemms)) if p % 2 == odd])

            @pl.when(sel)
            def _():
                for j in range(ff // n):
                    acc = None
                    for k in (0, 1):
                        t = dg(a_buf(w % 2, k)[...], b_buf(odd, k)[:, pl.ds(j * n, n)], 0, 0)
                        acc = t if acc is None else acc + t
                    o_buf(w % 2)[:, pl.ds(j * n, n)] = acc.astype(BF)

        for p in range(len(gemms)):
            @pl.when(in_gemm(p, w))
            def _():
                o_store(p, w).start()

    def stage_WG(c):
        per = tiles // nseq

        def one(j, _):
            tile(c * per + j)
            return 0

        lax.fori_loop(0, per, one, 0)

    barrier = pltpu.get_barrier_semaphore()
    for k in range(1, tpn):
        pl.semaphore_signal(barrier, inc=1, device_id={'tp': (tp + k) % tpn}, device_id_type=MESH)
    ld_x(0).start()
    for w in w1:
        w.start()
    xs_ld.start()
    for w in w2:
        w.start()
    dys_ld.start()
    ld_dy(0).start()
    dgb[...] = jnp.zeros_like(dgb)
    pl.semaphore_wait(barrier, tpn - 1)

    run = {'F1': stage_F1, 'MU': stage_MU, 'MD': stage_MD, 'MY': stage_MY, 'B2': stage_B2,
           'YL': stage_YL, 'YS': stage_YS, 'WG': stage_WG}
    hops = {'a': stage_a, 'b': stage_b, 'c': stage_c, 'd': stage_d, 'e': stage_e, 'f': stage_f}
    order = ORDER

    def step(i, _):
        for name, lag in order:
            c = i - lag

            @pl.when((c >= 0) & (c < nseq))
            def _():
                if name in run:
                    run[name](c)
                else:
                    hops[name[0]](int(name[1]), c)
        return 0

    lax.fori_loop(0, nseq + max(l for _, l in order), step, 0)

    for b in (0, 1):
        o_store(0, b).wait()
    for k in range(1, tpn):
        c_gain(k).wait_recv()
    tot = dgs[0]
    for t in range(1, tpn):
        tot = tot + dgs[t]
    dgain_o[...] = tot
    for k in range(1, tpn):
        c_gain(k).wait_send()


def mega(x, dy, wqkv, wo, wu, wd, ga, gm, heads):
    nseq, slen, dm = x.shape
    he, ff = wo.shape[0], wu.shape[1]
    half = slen // CORES
    blk = half // CHIPS
    hb = blk // 2
    tok = nseq * slen

    def arr(*shape):
        return jax.ShapeDtypeStruct(shape, BF)

    act = arr(tok, dm)
    outs = (act, act, arr(3 * he, dm), arr(he, dm), arr(dm, ff), arr(ff, dm), act, act, act, arr(tok, he),
            arr(nseq, 3 * he, slen), arr(tok, ff), arr(tok, ff), arr(tok, 3 * he), act, jax.ShapeDtypeStruct((2, dm), F32))
    hbm = pl.BlockSpec(memory_space=pl.ANY)
    vm = pl.BlockSpec(memory_space=pltpu.VMEM)
    V = pltpu.VMEM
    scratch = [
        V(wqkv.shape, BF), V(wo.shape, BF), V(wu.shape, BF), V(wd.shape, BF),
        V((2, SLOTS + 1, half, dm), BF), V((2, PAIRS, half, dm), BF),
        V((2, SLOTS, 2, blk, dm), BF), V((2, SLOTS, 2, hb, dm), BF),
        V((slen, dm), BF), V((slen, dm), BF), V((slen, dm), BF), V((slen, dm), BF), V((slen, dm), BF),
        V((3 * he, slen), BF), V((3 * he, slen), BF), V((slen, 3 * he), BF), V((3 * he, slen), BF),
        V((slen, he), BF), V((he, slen), BF), V((slen, ff), BF), V((slen, ff), BF), V((slen, dm), BF),
        V((nseq, blk, dm), BF), V((nseq, blk, dm), BF), V((nseq, blk, dm), BF), V((2, 2, blk, dm), BF), V((2, dm), F32),
        V((CHIPS * CORES, 2, dm), F32),
        pltpu.SemaphoreType.DMA((23,)), pltpu.SemaphoreType.DMA((5, 2)), pltpu.SemaphoreType.DMA((2, CHIPS * CORES)),
        pltpu.SemaphoreType.DMA((2, CHIPS)),
        pltpu.SemaphoreType.DMA((2, 5 * SLOTS)), pltpu.SemaphoreType.DMA((2, 5 * SLOTS)),
        pltpu.SemaphoreType.DMA((2, 8 * nseq)), pltpu.SemaphoreType.DMA((2, 8 * nseq)),
    ]
    flops = 2 * nseq * slen * dm * (4 * he * 2 + ff * 4)
    return pl.pallas_call(
        functools.partial(body, heads),
        name='mega',
        out_shape=outs,
        in_specs=[hbm] * 7 + [vm] * 2,
        out_specs=(hbm,) * 15 + (vm,),
        scratch_shapes=scratch,
        compiler_params=pltpu.CompilerParams(collective_id=0, has_side_effects=True, vmem_limit_bytes=VMEM_BYTES),
        cost_estimate=pl.CostEstimate(flops=flops, bytes_accessed=12 * nseq * slen * dm * 2, transcendentals=0),
    )(x, dy, dy.reshape(tok, dm), wqkv, wo, wu, wd, ga, gm)


def solution(mesh):
    assert mesh.shape['tp'] == CHIPS * CORES

    def step(x_in, gain_attn, w_qkv, w_out, gain_mlp, w_up, w_down, dy_out):
        heads, e = w_qkv.shape[3:]
        dm = x_in.shape[2]
        he = heads * e
        wqkv = jnp.transpose(w_qkv[0], (1, 2, 3, 0)).reshape(3 * he, dm)
        wo = w_out[0].reshape(he, dm)
        out = mega(x_in, dy_out, wqkv, wo, w_up[0], w_down[0], gain_attn, gain_mlp, heads)
        y, dx, dwq, dwo, dwu, dwd = out[:6]
        dgain = out[-1]
        dwq = jnp.transpose(dwq.reshape(3, heads, e, dm), (3, 0, 1, 2))
        return (y.reshape(x_in.shape), dx.reshape(x_in.shape), dgain[0:1], dwq[None], dwo.reshape(1, heads, e, dm),
                dgain[1:2], dwu[None], dwd[None])

    act = P('dp', None, None)
    in_specs = (act, P(None, None), P(None, None, None, 'tp', None), P(None, 'tp', None, None), P(None, None),
                P(None, None, 'tp'), P(None, 'tp', None), act)
    out_specs = (act, act, P('dp', None), P('dp', None, None, 'tp', None), P('dp', 'tp', None, None), P('dp', None),
                 P('dp', None, 'tp'), P('dp', 'tp', None))
    return jax.shard_map(step, mesh=mesh, in_specs=in_specs, out_specs=out_specs, check_vma=False)
```

```python
import functools
import math

import jax
import jax.numpy as jnp
from jax import lax
from jax.experimental import pallas as pl
from jax.experimental.pallas import tpu as pltpu
from jax.sharding import PartitionSpec as P


LN_EPS = 1e-5
CORES = 2
CHIPS = 4
BF = jnp.bfloat16
F32 = jnp.float32
MESH = pl.DeviceIdType.MESH
VMEM_BYTES = 67043328
GELU_C = 0.7978845608028654
GELU_K = 0.044715
SLOTS = 3
PAIRS = 2

ORDER = (
    ('b4', 14), ('d3', 10), ('f3', 12), ('c4', 15), ('F1', 0), ('c1', 2), ('MU', 6), ('e1', 5), ('b1', 1),
    ('a4', 13), ('a1', 0), ('YL', 18), ('MD', 6), ('f1', 5), ('WG', 20), ('e3', 11), ('YS', 18), ('c3', 8),
    ('c5', 20), ('b5', 19), ('MY', 6), ('e4', 18), ('f4', 19), ('a5', 18), ('b3', 7), ('a3', 6), ('d4', 16),
    ('d1', 3), ('B2', 12),
)


def dg(a, b, ca, cb):
    return lax.dot_general(a, b, (((ca,), (cb,)), ((), ())), preferred_element_type=F32)


def ln_parts(z):
    mu = jnp.mean(z, axis=-1, keepdims=True)
    c = z - mu
    var = jnp.mean(c * c, axis=-1, keepdims=True)
    r = lax.rsqrt(var + LN_EPS)
    return c * r, r


def ln_bwd(z, gain, d):
    xhat, r = ln_parts(z)
    h = d * gain
    m1 = jnp.mean(h, axis=-1, keepdims=True)
    m2 = jnp.mean(h * xhat, axis=-1, keepdims=True)
    return r * (h - m1 - xhat * m2), jnp.sum(d * xhat, axis=0, keepdims=True)


def gelu_both(z):
    z2 = z * z
    t = jnp.tanh(GELU_C * (z + GELU_K * (z2 * z)))
    cdf = 0.5 * (1.0 + t)
    d = cdf + z * (0.5 * (1.0 - t * t)) * (GELU_C * (1.0 + (3.0 * GELU_K) * z2))
    return z * cdf, d


def tile_of(n, want):
    t = min(n, want)
    while n % t:
        t //= 2
    return t


def body(heads, x, dy, dyf, wqkv_h, wo_h, wu_h, wd_h, ga, gm,
         ys_o, dx_o, dwq_o, dwo_o, dwu_o, dwd_o, nm_o, g_o, a_o, o_o, qkv_o, h_o, dp_o, dq_o, py_o, dgain_o,
         wqkv, wo, wu, wd, S, RD, R1, R2, xb, ab, nb, dyb, gb, qb, qb2, dqb, dqt, ob, obt, hb_, dpb, pyb,
         xs, xm, gs, own, dgb, dgs, lsem, wsem, dsem, ysem, ssem1, rsem1, ssem, rsem):
    nseq, slen, dm = x.shape
    tok = nseq * slen
    half = slen // CORES
    blk = half // CHIPS
    hb = blk // 2
    he = wo.shape[0]
    e = he // heads
    ff = wu.shape[1]
    scale = e ** -0.5
    tpn = CHIPS * CORES
    tp = lax.axis_index('tp')
    chip = tp // CORES
    core = tp % CORES
    sib = chip * CORES + (1 - core)
    rchip = (chip + 1) % CHIPS
    lchip = (chip + CHIPS - 1) % CHIPS
    ochip = (chip + 2) % CHIPS
    right = rchip * CORES + core
    left = lchip * CORES + core

    def seq(c):
        return pl.ds(pl.multiple_of(c * slen, slen), slen)

    def off(ch, co):
        return pl.multiple_of(co * half + ch * blk, blk)

    myoff = off(chip, core)

    def lc(src, dst, k):
        return pltpu.make_async_copy(src, dst, lsem.at[k])

    w1 = (lc(wqkv_h, wqkv, 0), lc(wo_h, wo, 1))
    w2 = (lc(wu_h, wu, 2), lc(wd_h, wd, 3))

    def ld_x(c):
        return lc(x.at[c], xb, 4)

    def ld_dy(c):
        return lc(dy.at[c], dyb, 5)

    def ld_nm(c):
        return lc(nm_o.at[seq(c)], nb, 6)

    def ld_g(c):
        return lc(g_o.at[seq(c)], gb, 7)

    def ld_q(c):
        return lc(qkv_o.at[c], qb2, 8)

    def st_a(c):
        return lc(ab, a_o.at[seq(c)], 9)

    def st_q(c):
        return lc(qb, qkv_o.at[c], 10)

    def st_o(c):
        return lc(ob, o_o.at[seq(c)], 11)

    def st_h(c):
        return lc(hb_, h_o.at[seq(c)], 12)

    def st_dp(c):
        return lc(dpb, dp_o.at[seq(c)], 13)

    def st_py(c):
        return lc(pyb, py_o.at[seq(c)], 14)

    def st_dq(c):
        return lc(dqb, dq_o.at[seq(c)], 15)

    xs_ld = lc(x.at[:, pl.ds(myoff, blk), :], xs, 16)
    dys_ld = lc(dy.at[:, pl.ds(myoff, blk), :], gs, 17)
    out_ref = {1: nm_o, 3: g_o, 4: dx_o}
    fset = {1: 0, 3: 1, 4: 0, 5: 1}

    def out_rows(fl, c, o, n):
        return out_ref[fl].at[pl.ds(pl.multiple_of(c * slen + o, n), n)]

    def st_own(fl, c):
        return lc(own.at[fset[fl], c % 2], out_rows(fl, c, myoff, blk), 19 + fset[fl] * 2 + c % 2)

    def rc(kind, fl, c, src, dst, dev):
        f = fset[fl]
        if kind < 5:
            send, recv = ssem1.at[f, kind * SLOTS + c], rsem1.at[f, kind * SLOTS + c]
        else:
            send, recv = (m.at[f, (kind - 5) * nseq + c] for m in (ssem, rsem))
        return pltpu.make_async_remote_copy(
            src_ref=src, dst_ref=dst, send_sem=send, recv_sem=recv,
            device_id={'tp': dev}, device_id_type=MESH)

    def c_pair(fl, c):
        f = fset[fl]
        return rc(0, fl, c % PAIRS, S.at[f, SLOTS], RD.at[f, c % PAIRS], sib)

    def c_first(fl, c, d):
        f, s = fset[fl], c % SLOTS
        src = S.at[f, s, pl.ds(blk + hb if d else hb, blk)]
        return rc(1 + d, fl, c % SLOTS, src, R1.at[f, s, d], left if d else right)

    def c_second(fl, c, d):
        f, s = fset[fl], c % SLOTS
        src = S.at[f, s, pl.ds(2 * blk + hb if d else 0, hb)]
        return rc(3 + d, fl, c % SLOTS, src, R2.at[f, s, d], left if d else right)

    def c_own(fl, c, d):
        dev = (right, left, sib)[d]
        return rc(5 + d, fl, c, own.at[fset[fl], c % 2], out_rows(fl, c, myoff, blk), dev)

    def c_fwd(fl, c, d):
        r = out_rows(fl, c, off(rchip if d else lchip, core) + d * hb, hb)
        return rc(8 + d, fl, c, r, r, left if d else right)

    def c_cross(fl, c, d):
        r = out_rows(fl, c, off((lchip, rchip, ochip)[d], core), blk)
        return rc(10 + d, fl, c, r, r, sib)

    def c_gain(k):
        return pltpu.make_async_remote_copy(
            src_ref=dgb, dst_ref=dgs.at[tp], send_sem=dsem.at[0, k], recv_sem=dsem.at[1, k],
            device_id={'tp': (tp + k) % tpn}, device_id_type=MESH)

    def store_part(f, c, col, n, val):
        v = val.astype(BF)
        s = c % SLOTS
        i0 = s * (1 - core) + SLOTS * core
        i1 = s * core + SLOTS * (1 - core)
        for b in range(CHIPS):
            r = pl.ds(pl.multiple_of(((b + CHIPS - 1 - chip) % CHIPS) * blk, blk), blk)
            S[f, i0, r, pl.ds(col, n)] = v[b * blk:(b + 1) * blk]
            S[f, i1, r, pl.ds(col, n)] = v[half + b * blk:half + (b + 1) * blk]

    def stage_a(fl, c):
        f, s = fset[fl], c % SLOTS
        c_pair(fl, c).wait_recv()
        c_pair(fl, c).wait_send()
        for st in {1: (st_a, st_q, st_o), 3: (st_h, st_dp), 4: (st_dq,), 5: ()}[fl]:
            st(c).wait()

        def add(t, _):
            r = pl.ds(pl.multiple_of(t * hb, hb), hb)
            S[f, s, r] = (S[f, s, r].astype(F32) + RD[f, c % PAIRS, r].astype(F32)).astype(BF)
            return 0

        lax.fori_loop(0, half // hb, add, 0, unroll=2)
        for d in (0, 1):
            c_first(fl, c, d).start()

    def stage_b(fl, c):
        f, s = fset[fl], c % SLOTS
        for d in (0, 1):
            c_first(fl, c, d).wait_recv()
        for d in (0, 1):
            o = pl.ds(2 * blk + hb if d else 0, hb)
            S[f, s, o] = (S[f, s, o].astype(F32) + R1[f, s, d, pl.ds(0 if d else hb, hb)].astype(F32)).astype(BF)
            c_second(fl, c, d).start()

    def stage_c(fl, c):
        f, s = fset[fl], c % SLOTS
        for d in (0, 1):
            c_second(fl, c, d).wait_recv()

        for k in (0, 1):
            q = pl.ds(k * hb, hb)
            o = pl.ds(3 * blk + k * hb, hb)
            tot = S[f, s, o].astype(F32) + R1[f, s, 1 - k, pl.ds(0 if k else hb, hb)].astype(F32) + R2[f, s, k].astype(F32)
            if fl == 1:
                z = (xs[c, q].astype(F32) + tot).astype(BF)
                xm[c, q] = z
                xh, _ = ln_parts(z.astype(F32))
                own[f, c % 2, q] = (xh * gm[...]).astype(BF)
            elif fl == 3:
                dr, dgn = ln_bwd(xm[c, q].astype(F32), gm[...], tot)
                v = (gs[c, q].astype(F32) + dr).astype(BF)
                gs[c, q] = v
                own[f, c % 2, q] = v
                dgb[1:2] += dgn
            elif fl == 5:
                xm[c, q] = (xm[c, q].astype(F32) + tot).astype(BF)
            else:
                dr, dgn = ln_bwd(xs[c, q].astype(F32), ga[...], tot)
                own[f, c % 2, q] = (gs[c, q].astype(F32) + dr).astype(BF)
                dgb[0:1] += dgn
        if fl != 5:
            for d in (0, 1, 2):
                c_own(fl, c, d).start()
            st_own(fl, c).start()
        for d in (0, 1):
            c_first(fl, c, d).wait_send()
            c_second(fl, c, d).wait_send()
        if fl == 4:
            @pl.when(c == nseq - 1)
            def _():
                dgs[tp] = dgb[...]
                for k in range(1, tpn):
                    c_gain(k).start()

    def stage_d(fl, c):
        for d in (1, 0):
            c_own(fl, c, 1 - d).wait_recv()
            c_fwd(fl, c, 1 - d).start()
        for d in (0, 1):
            c_cross(fl, c, d).start()
        for d in (0, 1, 2):
            c_own(fl, c, d).wait_send()
        st_own(fl, c).wait()

    def stage_e(fl, c):
        for d in (0, 1):
            c_fwd(fl, c, d).wait_recv()
        c_cross(fl, c, 2).start()

    def stage_f(fl, c):
        c_own(fl, c, 2).wait_recv()
        for d in (0, 1, 2):
            c_cross(fl, c, d).wait_recv()
        for d in (0, 1):
            c_fwd(fl, c, d).wait_send()
        for d in (0, 1, 2):
            c_cross(fl, c, d).wait_send()
        if fl == 1:
            ld_nm(c).start()
        if fl == 3:
            ld_g(c).start()

    def probs_t(q_ref, hd):
        qt = q_ref[pl.ds(pl.multiple_of(hd * e, e), e)]
        kt = q_ref[pl.ds(pl.multiple_of(he + hd * e, e), e)]
        vt = q_ref[pl.ds(pl.multiple_of(2 * he + hd * e, e), e)]
        s = dg(kt, qt, 0, 0) * scale
        keep = lax.broadcasted_iota(jnp.int32, (slen, slen), 0) <= lax.broadcasted_iota(jnp.int32, (slen, slen), 1)
        s = jnp.where(keep, s, -1e30)
        ex = jnp.exp(s - jnp.max(s, axis=0, keepdims=True))
        return qt, kt, vt, ex / jnp.sum(ex, axis=0, keepdims=True)

    def stage_F1(c):
        ld_x(c).wait()

        def ln(t, _):
            r = pl.ds(pl.multiple_of(t * hb, hb), hb)
            xh, _ = ln_parts(xb[r].astype(F32))
            ab[r] = (xh * ga[...]).astype(BF)
            return 0

        lax.fori_loop(0, slen // hb, ln, 0, unroll=4)
        st_a(c).start()

        @pl.when(c == 0)
        def _():
            for w in w1:
                w.wait()
            xs_ld.wait()

        @pl.when(c + 1 < nseq)
        def _():
            ld_x(c + 1).start()

        qt = tile_of(3 * he, 3 * he // 2)

        def qkv(t, _):
            r = pl.ds(pl.multiple_of(t * qt, qt), qt)
            qb[r] = dg(wqkv[r], ab[...], 1, 1).astype(BF)
            return 0

        lax.fori_loop(0, 3 * he // qt, qkv, 0)
        st_q(c).start()

        def head(hd, _):
            _, _, vt, p = probs_t(qb, hd)
            obt[pl.ds(pl.multiple_of(hd * e, e), e)] = dg(vt, p.astype(BF), 1, 0).astype(BF)
            return 0

        lax.fori_loop(0, heads, head, 0)
        tr = tile_of(he, 128)
        for t in range(he // tr):
            ob[:, t * tr:(t + 1) * tr] = obt[t * tr:(t + 1) * tr].T
        st_o(c).start()
        n = tile_of(dm, 1024)

        def proj(t, _):
            col = pl.multiple_of(t * n, n)
            store_part(0, c, col, n, dg(ob[...], wo[:, pl.ds(col, n)], 1, 0))
            return 0

        lax.fori_loop(0, dm // n, proj, 0)
        c_pair(1, c).start()

    def stage_MU(c):
        @pl.when(c == 0)
        def _():
            for w in w2:
                w.wait()
            dys_ld.wait()

        ld_nm(c).wait()
        ld_dy(c).wait()
        n = tile_of(ff, 512)

        def up(t, _):
            col = pl.ds(pl.multiple_of(t * n, n), n)
            pre = dg(nb[...], wu[:, col], 1, 0)
            dh = dg(dyb[...], wd[col], 1, 1)
            act, der = gelu_both(pre)
            hb_[:, col] = act.astype(BF)
            dpb[:, col] = (dh.astype(BF).astype(F32) * der).astype(BF)
            return 0

        lax.fori_loop(0, ff // n, up, 0)
        st_h(c).start()
        st_dp(c).start()

        @pl.when(c + 1 < nseq)
        def _():
            ld_dy(c + 1).start()

    m = tile_of(dm, 512)

    def stage_MD(c):
        def down(t, _):
            col = pl.multiple_of(t * m, m)
            store_part(1, c, col, m, dg(dpb[...], wu[pl.ds(col, m)], 1, 1))
            return 0

        lax.fori_loop(0, dm // m, down, 0)
        c_pair(3, c).start()

    def stage_MY(c):
        @pl.when(c > 0)
        def _():
            st_py(c - 1).wait()

        def outp(t, _):
            col = pl.multiple_of(t * m, m)
            pyb[:, pl.ds(col, m)] = dg(hb_[...], wd[:, pl.ds(col, m)], 1, 0).astype(BF)
            return 0

        lax.fori_loop(0, dm // m, outp, 0)
        st_py(c).start()

    def stage_B2(c):
        @pl.when(c == nseq - 1)
        def _():
            start_a(0)
            for k in (0, 1):
                b_load(0, k).start()

        ld_q(c).start()
        ld_g(c).wait()
        obt[...] = dg(wo[...], gb[...], 1, 1).astype(BF)
        ld_q(c).wait()

        def head(hd, _):
            qt, kt, vt, p = probs_t(qb2, hd)
            do = obt[pl.ds(pl.multiple_of(hd * e, e), e)]
            dqt[pl.ds(pl.multiple_of(2 * he + hd * e, e), e)] = dg(do, p.astype(BF), 1, 1).astype(BF)
            dpr = dg(vt, do, 0, 0).astype(BF).astype(F32)
            ds = p * (dpr - jnp.sum(dpr * p, axis=0, keepdims=True))
            ds = (ds * scale).astype(BF)
            dqt[pl.ds(pl.multiple_of(hd * e, e), e)] = dg(kt, ds, 1, 0).astype(BF)
            dqt[pl.ds(pl.multiple_of(he + hd * e, e), e)] = dg(qt, ds, 1, 1).astype(BF)
            return 0

        lax.fori_loop(0, heads, head, 0)
        tr = tile_of(3 * he, 128)
        for t in range(3 * he // tr):
            dqb[:, t * tr:(t + 1) * tr] = dqt[t * tr:(t + 1) * tr].T
        st_dq(c).start()
        n = tile_of(dm, 512)

        def proj(t, _):
            col = pl.multiple_of(t * n, n)
            store_part(0, c, col, n, dg(dqb[...], wqkv[:, pl.ds(col, n)], 1, 0))
            return 0

        lax.fori_loop(0, dm // n, proj, 0)
        c_pair(4, c).start()

    def y_loads(c):
        s = c % SLOTS

        cps = []
        for b in range(CHIPS):
            ch = (chip + 1 + b) % CHIPS
            for k, (co, t) in enumerate(((1 - core, SLOTS), (core, s))):
                src = py_o.at[pl.ds(pl.multiple_of(c * slen + co * half + ch * blk, blk), blk)]
                cps.append(pltpu.make_async_copy(src, S.at[1, t, pl.ds(b * blk, blk)], ysem.at[k, b]))
        return cps

    def stage_YL(c):
        @pl.when(c == nseq - 1)
        def _():
            st_py(c).wait()

        for cp in y_loads(c):
            cp.start()

    def stage_YS(c):
        for cp in y_loads(c):
            cp.wait()
        c_pair(5, c).start()

    kh = tok // 2
    gemms = []
    for lhs, rhs, res in ((nm_o, dp_o, dwu_o), (h_o, dyf, dwd_o), (dq_o, a_o, dwq_o), (o_o, g_o, dwo_o)):
        for cb in range(rhs.shape[1] // ff):
            gemms.append((lhs, rhs, res, lhs.shape[1] // he, cb * ff))
    first = [sum(g[3] for g in gemms[:p]) for p in range(len(gemms) + 1)]
    tiles = first[-1]

    def a_buf(b, k):
        return wd.at[pl.ds(0, kh), pl.ds(pl.multiple_of((2 * b + k) * he, he), he)]

    def b_buf(p, k):
        return wqkv.at[pl.ds(0, kh), pl.ds(k * ff, ff)] if p % 2 else wu.at[pl.ds(k * kh, kh)]

    def o_buf(b):
        return wu.at[pl.ds(pl.multiple_of(tok + b * he, math.gcd(tok, he)), he)]

    def a_load(p, w, k):
        col = pl.multiple_of((w - first[p]) * he, he)
        return pltpu.make_async_copy(gemms[p][0].at[pl.ds(k * kh, kh), pl.ds(col, he)], a_buf(w % 2, k), wsem.at[k, w % 2])

    def b_load(p, k):
        return pltpu.make_async_copy(gemms[p][1].at[pl.ds(k * kh, kh), pl.ds(gemms[p][4], ff)], b_buf(p, k), wsem.at[2 + k, p % 2])

    def o_store(p, w):
        row = pl.multiple_of((w - first[p]) * he, he)
        return pltpu.make_async_copy(o_buf(w % 2), gemms[p][2].at[pl.ds(row, he), pl.ds(gemms[p][4], ff)], wsem.at[4, w % 2])

    def in_gemm(p, w):
        return (w >= first[p]) & (w < first[p + 1])

    def start_a(w):
        for p in range(len(gemms)):
            @pl.when(in_gemm(p, w))
            def _():
                for k in (0, 1):
                    a_load(p, w, k).start()

    def tile(w):
        for k in (0, 1):
            a_load(0, w % 2, k).wait()
        start_a(w + 1)
        for p in range(len(gemms)):
            @pl.when(w == first[p])
            def _():
                for k in (0, 1):
                    b_load(p, k).wait()
                if p + 1 < len(gemms):
                    for k in (0, 1):
                        b_load(p + 1, k).start()

        @pl.when(w >= 2)
        def _():
            o_store(0, w % 2).wait()

        n = tile_of(ff, 512)
        for odd in (0, 1):
            sel = functools.reduce(lambda u, v: u | v, [in_gemm(p, w) for p in range(len(gemms)) if p % 2 == odd])

            @pl.when(sel)
            def _():
                for j in range(ff // n):
                    acc = None
                    for k in (0, 1):
                        t = dg(a_buf(w % 2, k)[...], b_buf(odd, k)[:, pl.ds(j * n, n)], 0, 0)
                        acc = t if acc is None else acc + t
                    o_buf(w % 2)[:, pl.ds(j * n, n)] = acc.astype(BF)

        for p in range(len(gemms)):
            @pl.when(in_gemm(p, w))
            def _():
                o_store(p, w).start()

    def stage_WG(c):
        per = tiles // nseq

        def one(j, _):
            tile(c * per + j)
            return 0

        lax.fori_loop(0, per, one, 0)

    barrier = pltpu.get_barrier_semaphore()
    for k in range(1, tpn):
        pl.semaphore_signal(barrier, inc=1, device_id={'tp': (tp + k) % tpn}, device_id_type=MESH)
    ld_x(0).start()
    for w in w1:
        w.start()
    xs_ld.start()
    for w in w2:
        w.start()
    dys_ld.start()
    ld_dy(0).start()
    dgb[...] = jnp.zeros_like(dgb)
    pl.semaphore_wait(barrier, tpn - 1)

    run = {'F1': stage_F1, 'MU': stage_MU, 'MD': stage_MD, 'MY': stage_MY, 'B2': stage_B2,
           'YL': stage_YL, 'YS': stage_YS, 'WG': stage_WG}
    hops = {'a': stage_a, 'b': stage_b, 'c': stage_c, 'd': stage_d, 'e': stage_e, 'f': stage_f}
    order = ORDER

    def step(i, _):
        for name, lag in order:
            c = i - lag

            @pl.when((c >= 0) & (c < nseq))
            def _():
                if name in run:
                    run[name](c)
                else:
                    hops[name[0]](int(name[1]), c)
        return 0

    lax.fori_loop(0, nseq + max(l for _, l in order), step, 0)

    ys = lc(xm, ys_o, 18)
    ys.start()
    for b in (0, 1):
        o_store(0, b).wait()
    for k in range(1, tpn):
        c_gain(k).wait_recv()
    tot = dgs[0]
    for t in range(1, tpn):
        tot = tot + dgs[t]
    dgain_o[...] = tot
    for k in range(1, tpn):
        c_gain(k).wait_send()
    ys.wait()


def mega(x, dy, wqkv, wo, wu, wd, ga, gm, heads):
    nseq, slen, dm = x.shape
    he, ff = wo.shape[0], wu.shape[1]
    half = slen // CORES
    blk = half // CHIPS
    hb = blk // 2
    tok = nseq * slen

    def arr(*shape):
        return jax.ShapeDtypeStruct(shape, BF)

    act = arr(tok, dm)
    outs = (arr(nseq, blk, dm), act, arr(3 * he, dm), arr(he, dm), arr(dm, ff), arr(ff, dm), act, act, act, arr(tok, he),
            arr(nseq, 3 * he, slen), arr(tok, ff), arr(tok, ff), arr(tok, 3 * he), act, jax.ShapeDtypeStruct((2, dm), F32))
    hbm = pl.BlockSpec(memory_space=pl.ANY)
    vm = pl.BlockSpec(memory_space=pltpu.VMEM)
    V = pltpu.VMEM
    scratch = [
        V(wqkv.shape, BF), V(wo.shape, BF), V(wu.shape, BF), V(wd.shape, BF),
        V((2, SLOTS + 1, half, dm), BF), V((2, PAIRS, half, dm), BF),
        V((2, SLOTS, 2, blk, dm), BF), V((2, SLOTS, 2, hb, dm), BF),
        V((slen, dm), BF), V((slen, dm), BF), V((slen, dm), BF), V((slen, dm), BF), V((slen, dm), BF),
        V((3 * he, slen), BF), V((3 * he, slen), BF), V((slen, 3 * he), BF), V((3 * he, slen), BF),
        V((slen, he), BF), V((he, slen), BF), V((slen, ff), BF), V((slen, ff), BF), V((slen, dm), BF),
        V((nseq, blk, dm), BF), V((nseq, blk, dm), BF), V((nseq, blk, dm), BF), V((2, 2, blk, dm), BF), V((2, dm), F32),
        V((CHIPS * CORES, 2, dm), F32),
        pltpu.SemaphoreType.DMA((23,)), pltpu.SemaphoreType.DMA((5, 2)), pltpu.SemaphoreType.DMA((2, CHIPS * CORES)),
        pltpu.SemaphoreType.DMA((2, CHIPS)),
        pltpu.SemaphoreType.DMA((2, 5 * SLOTS)), pltpu.SemaphoreType.DMA((2, 5 * SLOTS)),
        pltpu.SemaphoreType.DMA((2, 8 * nseq)), pltpu.SemaphoreType.DMA((2, 8 * nseq)),
    ]
    flops = 2 * nseq * slen * dm * (4 * he * 2 + ff * 4)
    return pl.pallas_call(
        functools.partial(body, heads),
        name='mega',
        out_shape=outs,
        in_specs=[hbm] * 7 + [vm] * 2,
        out_specs=(hbm,) * 15 + (vm,),
        scratch_shapes=scratch,
        compiler_params=pltpu.CompilerParams(collective_id=0, has_side_effects=True, vmem_limit_bytes=VMEM_BYTES),
        cost_estimate=pl.CostEstimate(flops=flops, bytes_accessed=12 * nseq * slen * dm * 2, transcendentals=0),
    )(x, dy, dy.reshape(tok, dm), wqkv, wo, wu, wd, ga, gm)


def copied(v):
    rows = tile_of(v.shape[0], 256 * 1536 // v.shape[1] * 2)

    def move(src, dst):
        dst[...] = src[...]

    spec = pl.BlockSpec((rows, v.shape[1]), lambda i: (i, 0))
    return pl.pallas_call(
        move, grid=(v.shape[0] // rows,), in_specs=[spec], out_specs=spec,
        out_shape=jax.ShapeDtypeStruct(v.shape, v.dtype),
        cost_estimate=pl.CostEstimate(flops=v.size * 500, bytes_accessed=4 * v.size, transcendentals=0))(v)


def solution(mesh):
    tpn = mesh.shape['tp']
    assert tpn == CHIPS * CORES

    def hop(v, chips_by, cores_by):
        perm = []
        for t in range(tpn):
            ch, co = t // CORES, t % CORES
            perm.append((t, ((ch + chips_by) % CHIPS) * CORES + (co + cores_by) % CORES))
        return lax.ppermute(v, 'tp', perm)

    def gather(v, chip, core):
        nseq, blk, dm = v.shape
        hb = blk // 2
        half = blk * CHIPS
        v_l, v_r = hop(v, 1, 0), hop(v, -1, 0)
        v_x = hop(v, 0, 1)
        o0, o1 = hop(v_l[:, :hb], 1, 0), hop(v_r[:, hb:], -1, 0)
        v_lx, v_rx = hop(v_l, 0, 1), hop(v_r, 0, 1)
        o0x, o1x = hop(o0, 0, 1), hop(o1, 0, 1)
        l, r, o = (chip + CHIPS - 1) % CHIPS, (chip + 1) % CHIPS, (chip + 2) % CHIPS
        out = jnp.zeros((nseq, half * CORES, dm), v.dtype)
        for co, pieces in ((core, (v, v_l, v_r, o0, o1)), (1 - core, (v_x, v_lx, v_rx, o0x, o1x))):
            for p, at in zip(pieces, (chip * blk, l * blk, r * blk, o * blk, o * blk + hb)):
                out = lax.dynamic_update_slice_in_dim(out, p, co * half + at, axis=1)
        return out

    def step(x_in, gain_attn, w_qkv, w_out, gain_mlp, w_up, w_down, dy_out):
        heads, e = w_qkv.shape[3:]
        dm = x_in.shape[2]
        he = heads * e
        wqkv = jnp.transpose(w_qkv[0], (1, 2, 3, 0)).reshape(3 * he, dm)
        wo = w_out[0].reshape(he, dm)
        out = mega(x_in, dy_out, wqkv, wo, w_up[0], w_down[0], gain_attn, gain_mlp, heads)
        ys, dx, dwq, dwo, dwu, dwd = out[:6]
        dgain = out[-1]
        tp = lax.axis_index('tp')
        dwu, dwd, dx, dwq, dwo = (copied(v) for v in (
            dwu, dwd, dx, dwq, dwo))
        y = gather(ys, tp // CORES, tp % CORES)
        dwq = jnp.transpose(dwq.reshape(3, heads, e, dm), (3, 0, 1, 2))
        return (y, dx.reshape(x_in.shape), dgain[0:1], dwq[None], dwo.reshape(1, heads, e, dm),
                dgain[1:2], dwu[None], dwd[None])

    act = P('dp', None, None)
    in_specs = (act, P(None, None), P(None, None, None, 'tp', None), P(None, 'tp', None, None), P(None, None),
                P(None, None, 'tp'), P(None, 'tp', None), act)
    out_specs = (act, act, P('dp', None), P('dp', None, None, 'tp', None), P('dp', 'tp', None, None), P('dp', None),
                 P('dp', None, 'tp'), P('dp', 'tp', None))
    step = jax.shard_map(step, mesh=mesh, in_specs=in_specs, out_specs=out_specs, check_vma=False)
    return step
```

```python
import functools
import math

import jax
import jax.numpy as jnp
from jax import lax
from jax.experimental import pallas as pl
from jax.experimental.pallas import tpu as pltpu
from jax.sharding import PartitionSpec as P


LN_EPS = 1e-5
CORES = 2
CHIPS = 4
BF = jnp.bfloat16
F32 = jnp.float32
MESH = pl.DeviceIdType.MESH
VMEM_BYTES = 67043328
GELU_C = 0.7978845608028654
GELU_K = 0.044715
SLOTS = 3
PAIRS = 2
TILES = 2

ORDER = (
    ('e3', 15), ('MU', 8), ('b1', 3), ('d3', 12), ('WP', 10), ('a1', 2), ('B2', 16), ('F1', 1), ('f1', 7),
    ('f3', 15), ('e1', 6), ('d1', 5), ('MD', 8), ('YS', 19), ('WG', 17), ('c3', 10), ('c5', 21), ('b5', 20),
    ('c1', 3), ('a5', 19), ('YL', 18), ('d4', 20), ('e4', 22), ('MY', 8), ('f4', 23), ('c4', 18), ('b3', 9),
    ('b4', 17), ('a3', 8), ('a4', 16),
)


def dg(a, b, ca, cb):
    return lax.dot_general(a, b, (((ca,), (cb,)), ((), ())), preferred_element_type=F32)


def ln_parts(z):
    mu = jnp.mean(z, axis=-1, keepdims=True)
    c = z - mu
    var = jnp.mean(c * c, axis=-1, keepdims=True)
    r = lax.rsqrt(var + LN_EPS)
    return c * r, r


def ln_bwd(z, gain, d):
    xhat, r = ln_parts(z)
    h = d * gain
    m1 = jnp.mean(h, axis=-1, keepdims=True)
    m2 = jnp.mean(h * xhat, axis=-1, keepdims=True)
    return r * (h - m1 - xhat * m2), jnp.sum(d * xhat, axis=0, keepdims=True)


def gelu_both(z):
    z2 = z * z
    t = jnp.tanh(GELU_C * (z + GELU_K * (z2 * z)))
    cdf = 0.5 * (1.0 + t)
    d = cdf + z * (0.5 * (1.0 - t * t)) * (GELU_C * (1.0 + (3.0 * GELU_K) * z2))
    return z * cdf, d


def tile_of(n, want):
    t = min(n, want)
    while n % t:
        t //= 2
    return t


def body(heads, x, dy, dyf, wqkv_h, wo_h, wu_h, wd_h, ga, gm,
         ys_o, dx_o, dwq_o, dwo_o, dwu_o, dwd_o, nm_o, g_o, a_o, o_o, qkv_o, h_o, dp_o, dq_o, py_o, dgain_o,
         wqkv, wo, wu, wd, S, RD, R1, R2, xb, ab, nb, dyb, gb, qb, qb2, dqb, dqt, ob, obt, hb_, dpb, pyb,
         xs, xm, gs, own, dgb, dgs, lsem, wsem, dsem, ysem, ssem1, rsem1, ssem, rsem):
    nseq, slen, dm = x.shape
    tok = nseq * slen
    half = slen // CORES
    blk = half // CHIPS
    hb = blk // 2
    he = wo.shape[0]
    e = he // heads
    ff = wu.shape[1]
    scale = e ** -0.5
    tpn = CHIPS * CORES
    tp = lax.axis_index('tp')
    chip = tp // CORES
    core = tp % CORES
    sib = chip * CORES + (1 - core)
    rchip = (chip + 1) % CHIPS
    lchip = (chip + CHIPS - 1) % CHIPS
    ochip = (chip + 2) % CHIPS
    right = rchip * CORES + core
    left = lchip * CORES + core

    def seq(c):
        return pl.ds(pl.multiple_of(c * slen, slen), slen)

    def off(ch, co):
        return pl.multiple_of(co * half + ch * blk, blk)

    myoff = off(chip, core)

    def lc(src, dst, k):
        return pltpu.make_async_copy(src, dst, lsem.at[k])

    w1 = (lc(wqkv_h, wqkv, 0), lc(wo_h, wo, 1))
    w2 = (lc(wu_h, wu, 2), lc(wd_h, wd, 3))

    def ld_x(c):
        return lc(x.at[c], xb, 4)

    def ld_dy(c):
        return lc(dy.at[c], dyb, 5)

    def ld_nm(c):
        return lc(nm_o.at[seq(c)], nb, 6)

    def ld_g(c):
        return lc(g_o.at[seq(c)], gb, 7)

    def ld_q(c):
        return lc(qkv_o.at[c], qb2, 8)

    def st_a(c):
        return lc(ab, a_o.at[seq(c)], 9)

    def st_q(c):
        return lc(qb, qkv_o.at[c], 10)

    def st_o(c):
        return lc(ob, o_o.at[seq(c)], 11)

    def st_h(c):
        return lc(hb_, h_o.at[seq(c)], 12)

    def st_dp(c):
        return lc(dpb, dp_o.at[seq(c)], 13)

    def st_py(c):
        return lc(pyb, py_o.at[seq(c)], 14)

    def st_dq(c):
        return lc(dqb, dq_o.at[seq(c)], 15)

    xs_ld = lc(x.at[:, pl.ds(myoff, blk), :], xs, 16)
    dys_ld = lc(dy.at[:, pl.ds(myoff, blk), :], gs, 17)
    out_ref = {1: nm_o, 3: g_o, 4: dx_o}
    fset = {1: 0, 3: 1, 4: 0, 5: 1}

    def out_rows(fl, c, o, n):
        return out_ref[fl].at[pl.ds(pl.multiple_of(c * slen + o, n), n)]

    def st_own(fl, c):
        return lc(own.at[fset[fl], c % 2], out_rows(fl, c, myoff, blk), 19 + fset[fl] * 2 + c % 2)

    def rc(kind, fl, c, src, dst, dev):
        f = fset[fl]
        if kind < 5:
            send, recv = ssem1.at[f, kind * SLOTS + c], rsem1.at[f, kind * SLOTS + c]
        else:
            send, recv = (m.at[f, (kind - 5) * nseq + c] for m in (ssem, rsem))
        return pltpu.make_async_remote_copy(
            src_ref=src, dst_ref=dst, send_sem=send, recv_sem=recv,
            device_id={'tp': dev}, device_id_type=MESH)

    def c_pair(fl, c):
        f = fset[fl]
        return rc(0, fl, c % PAIRS, S.at[f, SLOTS], RD.at[f, c % PAIRS], sib)

    def c_first(fl, c, d):
        f, s = fset[fl], c % SLOTS
        src = S.at[f, s, pl.ds(blk + hb if d else hb, blk)]
        return rc(1 + d, fl, c % SLOTS, src, R1.at[f, s, d], left if d else right)

    def c_second(fl, c, d):
        f, s = fset[fl], c % SLOTS
        src = S.at[f, s, pl.ds(2 * blk + hb if d else 0, hb)]
        return rc(3 + d, fl, c % SLOTS, src, R2.at[f, s, d], left if d else right)

    def c_own(fl, c, d):
        dev = (right, left, sib)[d]
        return rc(5 + d, fl, c, own.at[fset[fl], c % 2], out_rows(fl, c, myoff, blk), dev)

    def c_fwd(fl, c, d):
        r = out_rows(fl, c, off(rchip if d else lchip, core) + d * hb, hb)
        return rc(8 + d, fl, c, r, r, left if d else right)

    def c_cross(fl, c, d):
        r = out_rows(fl, c, off((lchip, rchip, ochip)[d], core), blk)
        return rc(10 + d, fl, c, r, r, sib)

    def c_gain(k):
        return pltpu.make_async_remote_copy(
            src_ref=dgb, dst_ref=dgs.at[tp], send_sem=dsem.at[0, k], recv_sem=dsem.at[1, k],
            device_id={'tp': (tp + k) % tpn}, device_id_type=MESH)

    def store_part(f, c, col, n, val):
        v = val.astype(BF)
        s = c % SLOTS
        i0 = s * (1 - core) + SLOTS * core
        i1 = s * core + SLOTS * (1 - core)
        for b in range(CHIPS):
            r = pl.ds(pl.multiple_of(((b + CHIPS - 1 - chip) % CHIPS) * blk, blk), blk)
            S[f, i0, r, pl.ds(col, n)] = v[b * blk:(b + 1) * blk]
            S[f, i1, r, pl.ds(col, n)] = v[half + b * blk:half + (b + 1) * blk]

    def stage_a(fl, c):
        f, s = fset[fl], c % SLOTS
        c_pair(fl, c).wait_recv()
        c_pair(fl, c).wait_send()
        for st in {1: (st_a, st_q, st_o), 3: (st_h, st_dp), 4: (st_dq,), 5: ()}[fl]:
            st(c).wait()

        def add(t, _):
            r = pl.ds(pl.multiple_of(t * hb, hb), hb)
            S[f, s, r] = (S[f, s, r].astype(F32) + RD[f, c % PAIRS, r].astype(F32)).astype(BF)
            return 0

        lax.fori_loop(0, half // hb, add, 0, unroll=2)
        for d in (0, 1):
            c_first(fl, c, d).start()

    def stage_b(fl, c):
        f, s = fset[fl], c % SLOTS
        for d in (0, 1):
            c_first(fl, c, d).wait_recv()
        for d in (0, 1):
            o = pl.ds(2 * blk + hb if d else 0, hb)
            S[f, s, o] = (S[f, s, o].astype(F32) + R1[f, s, d, pl.ds(0 if d else hb, hb)].astype(F32)).astype(BF)
            c_second(fl, c, d).start()

    def stage_c(fl, c):
        f, s = fset[fl], c % SLOTS
        for d in (0, 1):
            c_second(fl, c, d).wait_recv()

        for k in (0, 1):
            q = pl.ds(k * hb, hb)
            o = pl.ds(3 * blk + k * hb, hb)
            tot = S[f, s, o].astype(F32) + R1[f, s, 1 - k, pl.ds(0 if k else hb, hb)].astype(F32) + R2[f, s, k].astype(F32)
            if fl == 1:
                z = (xs[c, q].astype(F32) + tot).astype(BF)
                xm[c, q] = z
                xh, _ = ln_parts(z.astype(F32))
                own[f, c % 2, q] = (xh * gm[...]).astype(BF)
            elif fl == 3:
                dr, dgn = ln_bwd(xm[c, q].astype(F32), gm[...], tot)
                v = (gs[c, q].astype(F32) + dr).astype(BF)
                gs[c, q] = v
                own[f, c % 2, q] = v
                dgb[1:2] += dgn
            elif fl == 5:
                xm[c, q] = (xm[c, q].astype(F32) + tot).astype(BF)
            else:
                dr, dgn = ln_bwd(xs[c, q].astype(F32), ga[...], tot)
                own[f, c % 2, q] = (gs[c, q].astype(F32) + dr).astype(BF)
                dgb[0:1] += dgn
        if fl != 5:
            for d in (0, 1, 2):
                c_own(fl, c, d).start()
            st_own(fl, c).start()
        for d in (0, 1):
            c_first(fl, c, d).wait_send()
            c_second(fl, c, d).wait_send()
        if fl == 4:
            @pl.when(c == nseq - 1)
            def _():
                dgs[tp] = dgb[...]
                for k in range(1, tpn):
                    c_gain(k).start()

    def stage_d(fl, c):
        for d in (1, 0):
            c_own(fl, c, 1 - d).wait_recv()
            c_fwd(fl, c, 1 - d).start()
        for d in (0, 1):
            c_cross(fl, c, d).start()
        for d in (0, 1, 2):
            c_own(fl, c, d).wait_send()
        st_own(fl, c).wait()

    def stage_e(fl, c):
        for d in (0, 1):
            c_fwd(fl, c, d).wait_recv()
        c_cross(fl, c, 2).start()

    def stage_f(fl, c):
        c_own(fl, c, 2).wait_recv()
        for d in (0, 1, 2):
            c_cross(fl, c, d).wait_recv()
        for d in (0, 1):
            c_fwd(fl, c, d).wait_send()
        for d in (0, 1, 2):
            c_cross(fl, c, d).wait_send()
        if fl == 1:
            ld_nm(c).start()
        if fl == 3:
            ld_g(c).start()

    def probs_t(q_ref, hd):
        qt = q_ref[pl.ds(pl.multiple_of(hd * e, e), e)]
        kt = q_ref[pl.ds(pl.multiple_of(he + hd * e, e), e)]
        vt = q_ref[pl.ds(pl.multiple_of(2 * he + hd * e, e), e)]
        s = dg(kt, qt, 0, 0) * scale
        keep = lax.broadcasted_iota(jnp.int32, (slen, slen), 0) <= lax.broadcasted_iota(jnp.int32, (slen, slen), 1)
        s = jnp.where(keep, s, -1e30)
        ex = jnp.exp(s - jnp.max(s, axis=0, keepdims=True))
        return qt, kt, vt, ex / jnp.sum(ex, axis=0, keepdims=True)

    def stage_F1(c):
        ld_x(c).wait()

        def ln(t, _):
            r = pl.ds(pl.multiple_of(t * hb, hb), hb)
            xh, _ = ln_parts(xb[r].astype(F32))
            ab[r] = (xh * ga[...]).astype(BF)
            return 0

        lax.fori_loop(0, slen // hb, ln, 0, unroll=4)
        st_a(c).start()

        @pl.when(c == 0)
        def _():
            for w in w1:
                w.wait()
            xs_ld.wait()

        @pl.when(c + 1 < nseq)
        def _():
            ld_x(c + 1).start()

        qt = tile_of(3 * he, 3 * he // 2)

        def qkv(t, _):
            r = pl.ds(pl.multiple_of(t * qt, qt), qt)
            qb[r] = dg(wqkv[r], ab[...], 1, 1).astype(BF)
            return 0

        lax.fori_loop(0, 3 * he // qt, qkv, 0)
        st_q(c).start()

        def head(hd, _):
            _, _, vt, p = probs_t(qb, hd)
            obt[pl.ds(pl.multiple_of(hd * e, e), e)] = dg(vt, p.astype(BF), 1, 0).astype(BF)
            return 0

        lax.fori_loop(0, heads, head, 0)
        tr = tile_of(he, 128)
        for t in range(he // tr):
            ob[:, t * tr:(t + 1) * tr] = obt[t * tr:(t + 1) * tr].T
        st_o(c).start()
        n = tile_of(dm, 1024)

        def proj(t, _):
            col = pl.multiple_of(t * n, n)
            store_part(0, c, col, n, dg(ob[...], wo[:, pl.ds(col, n)], 1, 0))
            return 0

        lax.fori_loop(0, dm // n, proj, 0)
        c_pair(1, c).start()

    def stage_MU(c):
        @pl.when(c == 0)
        def _():
            for w in w2:
                w.wait()
            dys_ld.wait()

        ld_nm(c).wait()
        ld_dy(c).wait()
        n = tile_of(ff, 512)

        def up(t, _):
            col = pl.ds(pl.multiple_of(t * n, n), n)
            pre = dg(nb[...], wu[:, col], 1, 0)
            dh = dg(dyb[...], wd[col], 1, 1)
            act, der = gelu_both(pre)
            hb_[:, col] = act.astype(BF)
            dpb[:, col] = (dh.astype(BF).astype(F32) * der).astype(BF)
            return 0

        lax.fori_loop(0, ff // n, up, 0)
        st_h(c).start()
        st_dp(c).start()

        @pl.when(c + 1 < nseq)
        def _():
            ld_dy(c + 1).start()

    m = tile_of(dm, 512)

    def stage_MD(c):
        def down(t, _):
            col = pl.multiple_of(t * m, m)
            store_part(1, c, col, m, dg(dpb[...], wu[pl.ds(col, m)], 1, 1))
            return 0

        lax.fori_loop(0, dm // m, down, 0)
        c_pair(3, c).start()

    def stage_MY(c):
        @pl.when(c > 0)
        def _():
            st_py(c - 1).wait()

        def outp(t, _):
            col = pl.multiple_of(t * m, m)
            pyb[:, pl.ds(col, m)] = dg(hb_[...], wd[:, pl.ds(col, m)], 1, 0).astype(BF)
            return 0

        lax.fori_loop(0, dm // m, outp, 0)
        st_py(c).start()

    def stage_B2(c):
        ld_q(c).start()
        ld_g(c).wait()
        obt[...] = dg(wo[...], gb[...], 1, 1).astype(BF)
        ld_q(c).wait()

        def head(hd, _):
            qt, kt, vt, p = probs_t(qb2, hd)
            do = obt[pl.ds(pl.multiple_of(hd * e, e), e)]
            dqt[pl.ds(pl.multiple_of(2 * he + hd * e, e), e)] = dg(do, p.astype(BF), 1, 1).astype(BF)
            dpr = dg(vt, do, 0, 0).astype(BF).astype(F32)
            ds = p * (dpr - jnp.sum(dpr * p, axis=0, keepdims=True))
            ds = (ds * scale).astype(BF)
            dqt[pl.ds(pl.multiple_of(hd * e, e), e)] = dg(kt, ds, 1, 0).astype(BF)
            dqt[pl.ds(pl.multiple_of(he + hd * e, e), e)] = dg(qt, ds, 1, 1).astype(BF)
            return 0

        lax.fori_loop(0, heads, head, 0)
        tr = tile_of(3 * he, 128)
        for t in range(3 * he // tr):
            dqb[:, t * tr:(t + 1) * tr] = dqt[t * tr:(t + 1) * tr].T
        st_dq(c).start()
        n = tile_of(dm, 512)

        def proj(t, _):
            col = pl.multiple_of(t * n, n)
            store_part(0, c, col, n, dg(dqb[...], wqkv[:, pl.ds(col, n)], 1, 0))
            return 0

        lax.fori_loop(0, dm // n, proj, 0)
        c_pair(4, c).start()

    def y_loads(c):
        s = c % SLOTS

        cps = []
        for b in range(CHIPS):
            ch = (chip + 1 + b) % CHIPS
            for k, (co, t) in enumerate(((1 - core, SLOTS), (core, s))):
                src = py_o.at[pl.ds(pl.multiple_of(c * slen + co * half + ch * blk, blk), blk)]
                cps.append(pltpu.make_async_copy(src, S.at[1, t, pl.ds(b * blk, blk)], ysem.at[k, b]))
        return cps

    def stage_YL(c):
        @pl.when(c == nseq - 1)
        def _():
            st_py(c).wait()

        for cp in y_loads(c):
            cp.start()

    def stage_YS(c):
        for cp in y_loads(c):
            cp.wait()
        c_pair(5, c).start()

    kh = tok // 2
    gemms = []
    for lhs, rhs, res in ((nm_o, dp_o, dwu_o), (h_o, dyf, dwd_o), (dq_o, a_o, dwq_o), (o_o, g_o, dwo_o)):
        for cb in range(rhs.shape[1] // ff):
            gemms.append((lhs, rhs, res, lhs.shape[1] // he, cb * ff))
    first = [sum(g[3] for g in gemms[:p]) for p in range(len(gemms) + 1)]
    tiles = first[-1]

    def a_buf(b, k):
        return wd.at[pl.ds(0, kh), pl.ds(pl.multiple_of((2 * b + k) * he, he), he)]

    def b_parts(p):
        if p % 2 == 0:
            return [(0, kh, wu.at[pl.ds(0, kh)]), (kh, kh, wu.at[pl.ds(kh, kh)])]
        q = kh // 2
        return [(0, kh, wd.at[pl.ds(0, kh), pl.ds(ff, ff)]), (kh, q, wd.at[pl.ds(kh, q), pl.ds(0, ff)]),
                (kh + q, q, wd.at[pl.ds(kh, q), pl.ds(ff, ff)])]

    def o_buf(b):
        return wu.at[pl.ds(pl.multiple_of(tok + b * he, math.gcd(tok, he)), he)]

    def a_load(p, w, k):
        col = pl.multiple_of((w - first[p]) * he, he)
        return pltpu.make_async_copy(gemms[p][0].at[pl.ds(k * kh, kh), pl.ds(col, he)], a_buf(w % 2, k), wsem.at[k, w % 2])

    def b_loads(p):
        return [pltpu.make_async_copy(gemms[p][1].at[pl.ds(t, n), pl.ds(gemms[p][4], ff)], m, wsem.at[3 + q, p % 2])
                for q, (t, n, m) in enumerate(b_parts(p))]

    def o_store(p, w):
        row = pl.multiple_of((w - first[p]) * he, he)
        return pltpu.make_async_copy(o_buf(w % 2), gemms[p][2].at[pl.ds(row, he), pl.ds(gemms[p][4], ff)], wsem.at[2, w % 2])

    def in_gemm(p, w):
        return (w >= first[p]) & (w < first[p + 1])

    def start_a(w):
        for p in range(len(gemms)):
            @pl.when(in_gemm(p, w))
            def _():
                for k in (0, 1):
                    a_load(p, w, k).start()

    def tile(w):
        for k in (0, 1):
            a_load(0, w % 2, k).wait()
        start_a(w + 1)
        for p in range(len(gemms)):
            @pl.when(w == first[p])
            def _():
                for cp in b_loads(p):
                    cp.wait()
                if p + 1 < len(gemms):
                    for cp in b_loads(p + 1):
                        cp.start()

        @pl.when(w >= 2)
        def _():
            o_store(0, w % 2).wait()

        n = tile_of(ff, 512)
        for odd in (0, 1):
            sel = functools.reduce(lambda u, v: u | v, [in_gemm(p, w) for p in range(len(gemms)) if p % 2 == odd])

            @pl.when(sel)
            def _():
                for j in range(ff // n):
                    acc = None
                    for t0, nt, m in b_parts(odd):
                        lhs = a_buf(w % 2, t0 // kh)[pl.ds(t0 % kh, nt)]
                        t = dg(lhs, m[:, pl.ds(j * n, n)], 0, 0)
                        acc = t if acc is None else acc + t
                    o_buf(w % 2)[:, pl.ds(j * n, n)] = acc.astype(BF)

        for p in range(len(gemms)):
            @pl.when(in_gemm(p, w))
            def _():
                o_store(p, w).start()

    def stage_WG(c):
        def one(j, _):
            tile(c * TILES + j)
            return 0

        lax.fori_loop(0, TILES, one, 0)

    def stage_WP(c):
        @pl.when(c == nseq - 1)
        def _():
            start_a(0)
            for cp in b_loads(0):
                cp.start()

    barrier = pltpu.get_barrier_semaphore()
    for k in range(1, tpn):
        pl.semaphore_signal(barrier, inc=1, device_id={'tp': (tp + k) % tpn}, device_id_type=MESH)
    ld_x(0).start()
    for w in w1:
        w.start()
    xs_ld.start()
    for w in w2:
        w.start()
    dys_ld.start()
    ld_dy(0).start()
    dgb[...] = jnp.zeros_like(dgb)
    pl.semaphore_wait(barrier, tpn - 1)

    run = {'F1': stage_F1, 'MU': stage_MU, 'MD': stage_MD, 'MY': stage_MY, 'B2': stage_B2,
           'YL': stage_YL, 'YS': stage_YS, 'WG': stage_WG, 'WP': stage_WP}
    hops = {'a': stage_a, 'b': stage_b, 'c': stage_c, 'd': stage_d, 'e': stage_e, 'f': stage_f}
    order = ORDER

    def count(name):
        return tiles // TILES if name == 'WG' else nseq

    def step(i, _):
        for name, lag in order:
            c = i - lag

            @pl.when((c >= 0) & (c < count(name)))
            def _():
                if name in run:
                    run[name](c)
                else:
                    hops[name[0]](int(name[1]), c)
        return 0

    lax.fori_loop(0, max(count(n) + l for n, l in order), step, 0)

    ys = lc(xm, ys_o, 18)
    ys.start()
    for b in (0, 1):
        o_store(0, b).wait()
    for k in range(1, tpn):
        c_gain(k).wait_recv()
    tot = dgs[0]
    for t in range(1, tpn):
        tot = tot + dgs[t]
    dgain_o[...] = tot
    for k in range(1, tpn):
        c_gain(k).wait_send()
    ys.wait()


def mega(x, dy, wqkv, wo, wu, wd, ga, gm, heads):
    nseq, slen, dm = x.shape
    he, ff = wo.shape[0], wu.shape[1]
    half = slen // CORES
    blk = half // CHIPS
    hb = blk // 2
    tok = nseq * slen

    def arr(*shape):
        return jax.ShapeDtypeStruct(shape, BF)

    act = arr(tok, dm)
    outs = (arr(nseq, blk, dm), act, arr(3 * he, dm), arr(he, dm), arr(dm, ff), arr(ff, dm), act, act, act, arr(tok, he),
            arr(nseq, 3 * he, slen), arr(tok, ff), arr(tok, ff), arr(tok, 3 * he), act, jax.ShapeDtypeStruct((2, dm), F32))
    hbm = pl.BlockSpec(memory_space=pl.ANY)
    vm = pl.BlockSpec(memory_space=pltpu.VMEM)
    V = pltpu.VMEM
    scratch = [
        V(wqkv.shape, BF), V(wo.shape, BF), V(wu.shape, BF), V(wd.shape, BF),
        V((2, SLOTS + 1, half, dm), BF), V((2, PAIRS, half, dm), BF),
        V((2, SLOTS, 2, blk, dm), BF), V((2, SLOTS, 2, hb, dm), BF),
        V((slen, dm), BF), V((slen, dm), BF), V((slen, dm), BF), V((slen, dm), BF), V((slen, dm), BF),
        V((3 * he, slen), BF), V((3 * he, slen), BF), V((slen, 3 * he), BF), V((3 * he, slen), BF),
        V((slen, he), BF), V((he, slen), BF), V((slen, ff), BF), V((slen, ff), BF), V((slen, dm), BF),
        V((nseq, blk, dm), BF), V((nseq, blk, dm), BF), V((nseq, blk, dm), BF), V((2, 2, blk, dm), BF), V((2, dm), F32),
        V((CHIPS * CORES, 2, dm), F32),
        pltpu.SemaphoreType.DMA((23,)), pltpu.SemaphoreType.DMA((6, 2)), pltpu.SemaphoreType.DMA((2, CHIPS * CORES)),
        pltpu.SemaphoreType.DMA((2, CHIPS)),
        pltpu.SemaphoreType.DMA((2, 5 * SLOTS)), pltpu.SemaphoreType.DMA((2, 5 * SLOTS)),
        pltpu.SemaphoreType.DMA((2, 8 * nseq)), pltpu.SemaphoreType.DMA((2, 8 * nseq)),
    ]
    flops = 2 * nseq * slen * dm * (4 * he * 2 + ff * 4)
    return pl.pallas_call(
        functools.partial(body, heads),
        name='mega',
        out_shape=outs,
        in_specs=[hbm] * 7 + [vm] * 2,
        out_specs=(hbm,) * 15 + (vm,),
        scratch_shapes=scratch,
        compiler_params=pltpu.CompilerParams(collective_id=0, has_side_effects=True, vmem_limit_bytes=VMEM_BYTES),
        cost_estimate=pl.CostEstimate(flops=flops, bytes_accessed=12 * nseq * slen * dm * 2, transcendentals=0),
    )(x, dy, dy.reshape(tok, dm), wqkv, wo, wu, wd, ga, gm)


def copied(arrays):
    n = len(arrays)
    cuts = []
    for a, v in enumerate(arrays):
        rows = tile_of(v.shape[0], 256 * 3072 // v.shape[1])
        cuts += [(a, r, rows) for r in range(0, v.shape[0], rows)]

    def move(*refs):
        src, dst, buf, isem, osem = refs[:n], refs[n:2 * n], refs[2 * n:3 * n], refs[-2], refs[-1]
        into = [pltpu.make_async_copy(src[a].at[pl.ds(r, m)], buf[a].at[pl.ds(r, m)], isem.at[k]) for k, (a, r, m) in enumerate(cuts)]
        out = [pltpu.make_async_copy(buf[a].at[pl.ds(r, m)], dst[a].at[pl.ds(r, m)], osem.at[k]) for k, (a, r, m) in enumerate(cuts)]
        for cp in into:
            cp.start()
        for k in range(len(cuts)):
            into[k].wait()
            out[k].start()
        for cp in out:
            cp.wait()

    hbm = pl.BlockSpec(memory_space=pl.ANY)
    size = sum(v.size for v in arrays)
    return pl.pallas_call(
        move, name='copy_all', in_specs=[hbm] * n, out_specs=(hbm,) * n,
        out_shape=tuple(jax.ShapeDtypeStruct(v.shape, v.dtype) for v in arrays),
        scratch_shapes=[pltpu.VMEM(v.shape, v.dtype) for v in arrays] + [pltpu.SemaphoreType.DMA((len(cuts),))] * 2,
        compiler_params=pltpu.CompilerParams(vmem_limit_bytes=VMEM_BYTES),
        cost_estimate=pl.CostEstimate(flops=size * 500, bytes_accessed=4 * size, transcendentals=0))(*arrays)


def placed(out, pieces, shape, rows_of):
    n = len(pieces)
    given = [] if out is None else [out]

    def put(*refs):
        src, dst = refs[:n], refs[n + len(given)]
        buf, isem, osem = refs[n + len(given) + 1:-2], refs[-2], refs[-1]
        tp = lax.axis_index('tp')
        at = rows_of(tp // CORES, tp % CORES)
        into = [pltpu.make_async_copy(src[k], buf[k], isem.at[k]) for k in range(n)]
        outc = [pltpu.make_async_copy(
            buf[k], dst.at[:, pl.ds(pl.multiple_of(at[k], pieces[k].shape[1]), pieces[k].shape[1])], osem.at[k]) for k in range(n)]
        for cp in into:
            cp.start()
        for k in range(n):
            into[k].wait()
            outc[k].start()
        for cp in outc:
            cp.wait()

    hbm = pl.BlockSpec(memory_space=pl.ANY)
    return pl.pallas_call(
        put, in_specs=[hbm] * (n + len(given)), out_specs=hbm, out_shape=jax.ShapeDtypeStruct(shape, BF),
        scratch_shapes=[pltpu.VMEM(p.shape, p.dtype) for p in pieces] + [pltpu.SemaphoreType.DMA((n,))] * 2,
        input_output_aliases={n: 0} if given else {},
        compiler_params=pltpu.CompilerParams(vmem_limit_bytes=VMEM_BYTES),
        cost_estimate=pl.CostEstimate(flops=sum(p.size for p in pieces) * 500, bytes_accessed=0, transcendentals=0),
    )(*pieces, *given)


def solution(mesh):
    tpn = mesh.shape['tp']
    assert tpn == CHIPS * CORES

    def hop(v, chips_by, cores_by):
        perm = []
        for t in range(tpn):
            ch, co = t // CORES, t % CORES
            perm.append((t, ((ch + chips_by) % CHIPS) * CORES + (co + cores_by) % CORES))
        return lax.ppermute(v, 'tp', perm)

    def gather(v):
        nseq, blk, dm = v.shape
        hb = blk // 2
        half = blk * CHIPS
        v_l, v_r = hop(v, 1, 0), hop(v, -1, 0)
        v_x = hop(v, 0, 1)
        o0, o1 = hop(v_l[:, :hb], 1, 0), hop(v_r[:, hb:], -1, 0)
        v_lx, v_rx = hop(v_l, 0, 1), hop(v_r, 0, 1)
        o0x, o1x = hop(o0, 0, 1), hop(o1, 0, 1)

        def near(chip, core):
            chips = [chip, (chip + CHIPS - 1) % CHIPS, (chip + 1) % CHIPS]
            return [co * half + ch * blk for co in (core, 1 - core) for ch in chips]

        def far(chip, core):
            o = ((chip + 2) % CHIPS) * blk
            return [co * half + o + k for co in (core, 1 - core) for k in (0, hb)]

        out = placed(None, (v, v_l, v_r, v_x, v_lx, v_rx), (nseq, half * CORES, dm), near)
        return placed(out, (o0, o1, o0x, o1x), out.shape, far)

    def step(x_in, gain_attn, w_qkv, w_out, gain_mlp, w_up, w_down, dy_out):
        heads, e = w_qkv.shape[3:]
        dm = x_in.shape[2]
        he = heads * e
        wqkv = jnp.transpose(w_qkv[0], (1, 2, 3, 0)).reshape(3 * he, dm)
        wo = w_out[0].reshape(he, dm)
        out = mega(x_in, dy_out, wqkv, wo, w_up[0], w_down[0], gain_attn, gain_mlp, heads)
        ys, dx, dwq, dwo, dwu, dwd = out[:6]
        dgain = out[-1]
        dx, dwu, dwd, dwq, dwo = copied((dx, dwu, dwd, dwq, dwo))
        y = gather(ys)
        dwq = jnp.transpose(dwq.reshape(3, heads, e, dm), (3, 0, 1, 2))
        return (y, dx.reshape(x_in.shape), dgain[0:1], dwq[None], dwo.reshape(1, heads, e, dm),
                dgain[1:2], dwu[None], dwd[None])

    act = P('dp', None, None)
    in_specs = (act, P(None, None), P(None, None, None, 'tp', None), P(None, 'tp', None, None), P(None, None),
                P(None, None, 'tp'), P(None, 'tp', None), act)
    out_specs = (act, act, P('dp', None), P('dp', None, None, 'tp', None), P('dp', 'tp', None, None), P('dp', None),
                 P('dp', None, 'tp'), P('dp', 'tp', None))
    step = jax.shard_map(step, mesh=mesh, in_specs=in_specs, out_specs=out_specs, check_vma=False)
    return step
```

```python
import functools
import math

import jax
import jax.numpy as jnp
from jax import lax
from jax.experimental import pallas as pl
from jax.experimental.pallas import tpu as pltpu
from jax.sharding import PartitionSpec as P


LN_EPS = 1e-5
CORES = 2
CHIPS = 4
BF = jnp.bfloat16
F32 = jnp.float32
MESH = pl.DeviceIdType.MESH
VMEM_BYTES = 67043328
GELU_C = 0.7978845608028654
GELU_K = 0.044715
SLOTS = 3
PAIRS = 2
TILES = 2

ORDER = (
    ('e3', 15), ('MU', 8), ('b1', 3), ('d3', 12), ('WP', 10), ('a1', 2), ('B2', 16), ('F1', 1), ('f1', 7),
    ('f3', 15), ('e1', 6), ('d1', 5), ('MD', 8), ('YS', 19), ('WG', 17), ('c3', 10), ('c5', 21), ('b5', 20),
    ('c1', 3), ('a5', 19), ('YL', 18), ('d4', 20), ('e4', 22), ('MY', 8), ('f4', 23), ('c4', 18), ('b3', 9),
    ('b4', 17), ('a3', 8), ('a4', 16),
)


def dg(a, b, ca, cb):
    return lax.dot_general(a, b, (((ca,), (cb,)), ((), ())), preferred_element_type=F32)


def ln_parts(z):
    mu = jnp.mean(z, axis=-1, keepdims=True)
    c = z - mu
    var = jnp.mean(c * c, axis=-1, keepdims=True)
    r = lax.rsqrt(var + LN_EPS)
    return c * r, r


def ln_bwd(z, gain, d):
    xhat, r = ln_parts(z)
    h = d * gain
    m1 = jnp.mean(h, axis=-1, keepdims=True)
    m2 = jnp.mean(h * xhat, axis=-1, keepdims=True)
    return r * (h - m1 - xhat * m2), jnp.sum(d * xhat, axis=0, keepdims=True)


def gelu_both(z):
    z2 = z * z
    t = jnp.tanh(GELU_C * (z + GELU_K * (z2 * z)))
    cdf = 0.5 * (1.0 + t)
    d = cdf + z * (0.5 * (1.0 - t * t)) * (GELU_C * (1.0 + (3.0 * GELU_K) * z2))
    return z * cdf, d


def tile_of(n, want):
    t = min(n, want)
    while n % t:
        t //= 2
    return t


def body(heads, x, dy, dyf, wqkv_h, wo_h, wu_h, wd_h, ga, gm,
         ya_o, yb_o, dx_o, dwq_o, dwo_o, dwu_o, dwd_o, nm_o, g_o, a_o, o_o, qkv_o, h_o, dp_o, dq_o, py_o, dgain_o,
         wqkv, wo, wu, wd, S, RD, R1, R2, xb, ab, nb, dyb, gb, qb, qb2, dqb, dqt, ob, obt, hb_, dpb, pyb,
         xs, xm, gs, own, dgb, dgs, lsem, wsem, dsem, ysem, qsem, ssem1, rsem1, ssem, rsem):
    nseq, slen, dm = x.shape
    tok = nseq * slen
    half = slen // CORES
    blk = half // CHIPS
    hb = blk // 2
    he = wo.shape[0]
    e = he // heads
    ff = wu.shape[1]
    scale = e ** -0.5
    tpn = CHIPS * CORES
    tp = lax.axis_index('tp')
    chip = tp // CORES
    core = tp % CORES
    sib = chip * CORES + (1 - core)
    rchip = (chip + 1) % CHIPS
    lchip = (chip + CHIPS - 1) % CHIPS
    ochip = (chip + 2) % CHIPS
    right = rchip * CORES + core
    left = lchip * CORES + core

    def seq(c):
        return pl.ds(pl.multiple_of(c * slen, slen), slen)

    def off(ch, co):
        return pl.multiple_of(co * half + ch * blk, blk)

    myoff = off(chip, core)

    def lc(src, dst, k):
        return pltpu.make_async_copy(src, dst, lsem.at[k])

    qt = tile_of(3 * wo.shape[0], 3 * wo.shape[0] // 2)

    def ld_wqkv(t):
        r = pl.ds(pl.multiple_of(t * qt, qt), qt)
        return pltpu.make_async_copy(wqkv_h.at[r], wqkv.at[r], qsem.at[t])

    ld_wo = lc(wo_h, wo, 1)
    w2 = (lc(wu_h, wu, 2), lc(wd_h, wd, 3))

    def ld_x(c):
        return lc(x.at[c], xb, 4)

    def ld_dy(c):
        return lc(dy.at[c], dyb, 5)

    def ld_nm(c):
        return lc(nm_o.at[seq(c)], nb, 6)

    def ld_g(c):
        return lc(g_o.at[seq(c)], gb, 7)

    def ld_q(c):
        return lc(qkv_o.at[c], qb2, 8)

    def st_a(c):
        return lc(ab, a_o.at[seq(c)], 9)

    def st_q(c):
        return lc(qb, qkv_o.at[c], 10)

    def st_o(c):
        return lc(ob, o_o.at[seq(c)], 11)

    def st_h(c):
        return lc(hb_, h_o.at[seq(c)], 12)

    def st_dp(c):
        return lc(dpb, dp_o.at[seq(c)], 13)

    def st_py(c):
        return lc(pyb, py_o.at[seq(c)], 14)

    def st_dq(c):
        return lc(dqb, dq_o.at[seq(c)], 15)

    xs_ld = lc(x.at[:, pl.ds(myoff, blk), :], xs, 16)
    dys_ld = lc(dy.at[:, pl.ds(myoff, blk), :], gs, 17)
    out_ref = {1: nm_o, 3: g_o, 4: dx_o}
    fset = {1: 0, 3: 1, 4: 0, 5: 1}

    def out_rows(fl, c, o, n):
        return out_ref[fl].at[pl.ds(pl.multiple_of(c * slen + o, n), n)]

    def st_own(fl, c):
        return lc(own.at[fset[fl], c % 2], out_rows(fl, c, myoff, blk), 19 + fset[fl] * 2 + c % 2)

    def rc(kind, fl, c, src, dst, dev):
        f = fset[fl]
        if kind < 5:
            send, recv = ssem1.at[f, kind * SLOTS + c], rsem1.at[f, kind * SLOTS + c]
        else:
            send, recv = (m.at[f, (kind - 5) * nseq + c] for m in (ssem, rsem))
        return pltpu.make_async_remote_copy(
            src_ref=src, dst_ref=dst, send_sem=send, recv_sem=recv,
            device_id={'tp': dev}, device_id_type=MESH)

    def c_pair(fl, c):
        f = fset[fl]
        return rc(0, fl, c % PAIRS, S.at[f, SLOTS], RD.at[f, c % PAIRS], sib)

    def c_first(fl, c, d):
        f, s = fset[fl], c % SLOTS
        src = S.at[f, s, pl.ds(blk + hb if d else hb, blk)]
        return rc(1 + d, fl, c % SLOTS, src, R1.at[f, s, d], left if d else right)

    def c_second(fl, c, d):
        f, s = fset[fl], c % SLOTS
        src = S.at[f, s, pl.ds(2 * blk + hb if d else 0, hb)]
        return rc(3 + d, fl, c % SLOTS, src, R2.at[f, s, d], left if d else right)

    def c_own(fl, c, d):
        dev = (right, left, sib)[d]
        return rc(5 + d, fl, c, own.at[fset[fl], c % 2], out_rows(fl, c, myoff, blk), dev)

    def c_fwd(fl, c, d):
        r = out_rows(fl, c, off(rchip if d else lchip, core) + d * hb, hb)
        return rc(8 + d, fl, c, r, r, left if d else right)

    def c_cross(fl, c, d):
        r = out_rows(fl, c, off((lchip, rchip, ochip)[d], core), blk)
        return rc(10 + d, fl, c, r, r, sib)

    def c_gain(k):
        return pltpu.make_async_remote_copy(
            src_ref=dgb, dst_ref=dgs.at[tp], send_sem=dsem.at[0, k], recv_sem=dsem.at[1, k],
            device_id={'tp': (tp + k) % tpn}, device_id_type=MESH)

    def store_part(f, c, col, n, val):
        v = val.astype(BF)
        s = c % SLOTS
        i0 = s * (1 - core) + SLOTS * core
        i1 = s * core + SLOTS * (1 - core)
        for b in range(CHIPS):
            r = pl.ds(pl.multiple_of(((b + CHIPS - 1 - chip) % CHIPS) * blk, blk), blk)
            S[f, i0, r, pl.ds(col, n)] = v[b * blk:(b + 1) * blk]
            S[f, i1, r, pl.ds(col, n)] = v[half + b * blk:half + (b + 1) * blk]

    def stage_a(fl, c):
        f, s = fset[fl], c % SLOTS
        c_pair(fl, c).wait_recv()
        c_pair(fl, c).wait_send()
        for st in {1: (st_a, st_q, st_o), 3: (st_h, st_dp), 4: (st_dq,), 5: ()}[fl]:
            st(c).wait()

        def add(t, _):
            r = pl.ds(pl.multiple_of(t * hb, hb), hb)
            S[f, s, r] = (S[f, s, r].astype(F32) + RD[f, c % PAIRS, r].astype(F32)).astype(BF)
            return 0

        lax.fori_loop(0, half // hb, add, 0, unroll=2)
        for d in (0, 1):
            c_first(fl, c, d).start()

    def stage_b(fl, c):
        f, s = fset[fl], c % SLOTS
        for d in (0, 1):
            c_first(fl, c, d).wait_recv()
        for d in (0, 1):
            o = pl.ds(2 * blk + hb if d else 0, hb)
            S[f, s, o] = (S[f, s, o].astype(F32) + R1[f, s, d, pl.ds(0 if d else hb, hb)].astype(F32)).astype(BF)
            c_second(fl, c, d).start()

    def stage_c(fl, c):
        f, s = fset[fl], c % SLOTS
        for d in (0, 1):
            c_second(fl, c, d).wait_recv()

        for k in (0, 1):
            q = pl.ds(k * hb, hb)
            o = pl.ds(3 * blk + k * hb, hb)
            tot = S[f, s, o].astype(F32) + R1[f, s, 1 - k, pl.ds(0 if k else hb, hb)].astype(F32) + R2[f, s, k].astype(F32)
            if fl == 1:
                if k == 0:
                    @pl.when(c == 0)
                    def _():
                        xs_ld.wait()

                z = (xs[c, q].astype(F32) + tot).astype(BF)
                xm[c, q] = z
                xh, _ = ln_parts(z.astype(F32))
                own[f, c % 2, q] = (xh * gm[...]).astype(BF)
            elif fl == 3:
                dr, dgn = ln_bwd(xm[c, q].astype(F32), gm[...], tot)
                v = (gs[c, q].astype(F32) + dr).astype(BF)
                gs[c, q] = v
                own[f, c % 2, q] = v
                dgb[1:2] += dgn
            elif fl == 5:
                xm[c, q] = (xm[c, q].astype(F32) + tot).astype(BF)
            else:
                dr, dgn = ln_bwd(xs[c, q].astype(F32), ga[...], tot)
                own[f, c % 2, q] = (gs[c, q].astype(F32) + dr).astype(BF)
                dgb[0:1] += dgn
        if fl != 5:
            for d in (0, 1, 2):
                c_own(fl, c, d).start()
            st_own(fl, c).start()
        for d in (0, 1):
            c_first(fl, c, d).wait_send()
            c_second(fl, c, d).wait_send()
        if fl == 4:
            @pl.when(c == nseq - 1)
            def _():
                dgs[tp] = dgb[...]
                for k in range(1, tpn):
                    c_gain(k).start()

    def stage_d(fl, c):
        for d in (1, 0):
            c_own(fl, c, 1 - d).wait_recv()
            c_fwd(fl, c, 1 - d).start()
        for d in (0, 1):
            c_cross(fl, c, d).start()
        for d in (0, 1, 2):
            c_own(fl, c, d).wait_send()
        st_own(fl, c).wait()

    def stage_e(fl, c):
        for d in (0, 1):
            c_fwd(fl, c, d).wait_recv()
        c_cross(fl, c, 2).start()

    def stage_f(fl, c):
        c_own(fl, c, 2).wait_recv()
        for d in (0, 1, 2):
            c_cross(fl, c, d).wait_recv()
        for d in (0, 1):
            c_fwd(fl, c, d).wait_send()
        for d in (0, 1, 2):
            c_cross(fl, c, d).wait_send()
        if fl == 1:
            ld_nm(c).start()
        if fl == 3:
            ld_g(c).start()

    def probs_t(q_ref, hd):
        qt = q_ref[pl.ds(pl.multiple_of(hd * e, e), e)]
        kt = q_ref[pl.ds(pl.multiple_of(he + hd * e, e), e)]
        vt = q_ref[pl.ds(pl.multiple_of(2 * he + hd * e, e), e)]
        s = dg(kt, qt, 0, 0) * scale
        keep = lax.broadcasted_iota(jnp.int32, (slen, slen), 0) <= lax.broadcasted_iota(jnp.int32, (slen, slen), 1)
        s = jnp.where(keep, s, -1e30)
        ex = jnp.exp(s - jnp.max(s, axis=0, keepdims=True))
        return qt, kt, vt, ex / jnp.sum(ex, axis=0, keepdims=True)

    def norm_rows():
        def ln(t, _):
            r = pl.ds(pl.multiple_of(t * hb, hb), hb)
            xh, _ = ln_parts(xb[r].astype(F32))
            ab[r] = (xh * ga[...]).astype(BF)
            return 0

        lax.fori_loop(0, slen // hb, ln, 0, unroll=4)

    def stage_F1(c):
        @pl.when(c > 0)
        def _():
            ld_x(c).wait()
            norm_rows()

        st_a(c).start()

        @pl.when(c + 1 < nseq)
        def _():
            ld_x(c + 1).start()

        def qkv(t, _):
            @pl.when(c == 0)
            def _():
                ld_wqkv(t).wait()

            r = pl.ds(pl.multiple_of(t * qt, qt), qt)
            qb[r] = dg(wqkv[r], ab[...], 1, 1).astype(BF)
            return 0

        lax.fori_loop(0, 3 * he // qt, qkv, 0)
        st_q(c).start()

        def head(hd, _):
            _, _, vt, p = probs_t(qb, hd)
            obt[pl.ds(pl.multiple_of(hd * e, e), e)] = dg(vt, p.astype(BF), 1, 0).astype(BF)
            return 0

        lax.fori_loop(0, heads, head, 0)
        tr = tile_of(he, 128)
        for t in range(he // tr):
            ob[:, t * tr:(t + 1) * tr] = obt[t * tr:(t + 1) * tr].T
        st_o(c).start()
        n = tile_of(dm, 1024)

        @pl.when(c == 0)
        def _():
            ld_wo.wait()
            for w in w2:
                w.start()
            for w in (xs_ld, dys_ld, ld_dy(0)):
                w.start()

        def proj(t, _):
            col = pl.multiple_of(t * n, n)
            store_part(0, c, col, n, dg(ob[...], wo[:, pl.ds(col, n)], 1, 0))
            return 0

        lax.fori_loop(0, dm // n, proj, 0)
        c_pair(1, c).start()

    def stage_MU(c):
        @pl.when(c == 0)
        def _():
            for w in w2:
                w.wait()
            dys_ld.wait()

        ld_nm(c).wait()
        ld_dy(c).wait()
        n = tile_of(ff, 512)

        def up(t, _):
            col = pl.ds(pl.multiple_of(t * n, n), n)
            pre = dg(nb[...], wu[:, col], 1, 0)
            dh = dg(dyb[...], wd[col], 1, 1)
            act, der = gelu_both(pre)
            hb_[:, col] = act.astype(BF)
            dpb[:, col] = (dh.astype(BF).astype(F32) * der).astype(BF)
            return 0

        lax.fori_loop(0, ff // n, up, 0)
        st_h(c).start()
        st_dp(c).start()

        @pl.when(c + 1 < nseq)
        def _():
            ld_dy(c + 1).start()

    m = tile_of(dm, 512)

    def stage_MD(c):
        def down(t, _):
            col = pl.multiple_of(t * m, m)
            store_part(1, c, col, m, dg(dpb[...], wu[pl.ds(col, m)], 1, 1))
            return 0

        lax.fori_loop(0, dm // m, down, 0)
        c_pair(3, c).start()

    def stage_MY(c):
        @pl.when(c > 0)
        def _():
            st_py(c - 1).wait()

        def outp(t, _):
            col = pl.multiple_of(t * m, m)
            pyb[:, pl.ds(col, m)] = dg(hb_[...], wd[:, pl.ds(col, m)], 1, 0).astype(BF)
            return 0

        lax.fori_loop(0, dm // m, outp, 0)
        st_py(c).start()

    def stage_B2(c):
        ld_q(c).start()
        ld_g(c).wait()
        obt[...] = dg(wo[...], gb[...], 1, 1).astype(BF)
        ld_q(c).wait()

        def head(hd, _):
            qt, kt, vt, p = probs_t(qb2, hd)
            do = obt[pl.ds(pl.multiple_of(hd * e, e), e)]
            dqt[pl.ds(pl.multiple_of(2 * he + hd * e, e), e)] = dg(do, p.astype(BF), 1, 1).astype(BF)
            dpr = dg(vt, do, 0, 0).astype(BF).astype(F32)
            ds = p * (dpr - jnp.sum(dpr * p, axis=0, keepdims=True))
            ds = (ds * scale).astype(BF)
            dqt[pl.ds(pl.multiple_of(hd * e, e), e)] = dg(kt, ds, 1, 0).astype(BF)
            dqt[pl.ds(pl.multiple_of(he + hd * e, e), e)] = dg(qt, ds, 1, 1).astype(BF)
            return 0

        lax.fori_loop(0, heads, head, 0)
        tr = tile_of(3 * he, 128)
        for t in range(3 * he // tr):
            dqb[:, t * tr:(t + 1) * tr] = dqt[t * tr:(t + 1) * tr].T
        st_dq(c).start()
        n = tile_of(dm, 512)

        def proj(t, _):
            col = pl.multiple_of(t * n, n)
            store_part(0, c, col, n, dg(dqb[...], wqkv[:, pl.ds(col, n)], 1, 0))
            return 0

        lax.fori_loop(0, dm // n, proj, 0)
        c_pair(4, c).start()

    def y_loads(c):
        s = c % SLOTS

        cps = []
        for b in range(CHIPS):
            ch = (chip + 1 + b) % CHIPS
            for k, (co, t) in enumerate(((1 - core, SLOTS), (core, s))):
                src = py_o.at[pl.ds(pl.multiple_of(c * slen + co * half + ch * blk, blk), blk)]
                cps.append(pltpu.make_async_copy(src, S.at[1, t, pl.ds(b * blk, blk)], ysem.at[k, b]))
        return cps

    def stage_YL(c):
        @pl.when(c == nseq - 1)
        def _():
            st_py(c).wait()

        for cp in y_loads(c):
            cp.start()

    def stage_YS(c):
        for cp in y_loads(c):
            cp.wait()
        c_pair(5, c).start()

    kh = tok // 2
    gemms = []
    for lhs, rhs, res in ((nm_o, dp_o, dwu_o), (h_o, dyf, dwd_o), (dq_o, a_o, dwq_o), (o_o, g_o, dwo_o)):
        for cb in range(rhs.shape[1] // ff):
            gemms.append((lhs, rhs, res, lhs.shape[1] // he, cb * ff))
    first = [sum(g[3] for g in gemms[:p]) for p in range(len(gemms) + 1)]
    tiles = first[-1]

    def a_buf(b, k):
        return wd.at[pl.ds(0, kh), pl.ds(pl.multiple_of((2 * b + k) * he, he), he)]

    def b_parts(p):
        if p % 2 == 0:
            return [(0, kh, wu.at[pl.ds(0, kh)]), (kh, kh, wu.at[pl.ds(kh, kh)])]
        q = kh // 2
        return [(0, kh, wd.at[pl.ds(0, kh), pl.ds(ff, ff)]), (kh, q, wd.at[pl.ds(kh, q), pl.ds(0, ff)]),
                (kh + q, q, wd.at[pl.ds(kh, q), pl.ds(ff, ff)])]

    def o_buf(b):
        return wu.at[pl.ds(pl.multiple_of(tok + b * he, math.gcd(tok, he)), he)]

    def a_load(p, w, k):
        col = pl.multiple_of((w - first[p]) * he, he)
        return pltpu.make_async_copy(gemms[p][0].at[pl.ds(k * kh, kh), pl.ds(col, he)], a_buf(w % 2, k), wsem.at[k, w % 2])

    def b_loads(p):
        return [pltpu.make_async_copy(gemms[p][1].at[pl.ds(t, n), pl.ds(gemms[p][4], ff)], m, wsem.at[3 + q, p % 2])
                for q, (t, n, m) in enumerate(b_parts(p))]

    def o_store(p, w):
        row = pl.multiple_of((w - first[p]) * he, he)
        return pltpu.make_async_copy(o_buf(w % 2), gemms[p][2].at[pl.ds(row, he), pl.ds(gemms[p][4], ff)], wsem.at[2, w % 2])

    def in_gemm(p, w):
        return (w >= first[p]) & (w < first[p + 1])

    def start_a(w):
        for p in range(len(gemms)):
            @pl.when(in_gemm(p, w))
            def _():
                for k in (0, 1):
                    a_load(p, w, k).start()

    def tile(w):
        for k in (0, 1):
            a_load(0, w % 2, k).wait()
        start_a(w + 1)
        for p in range(len(gemms)):
            @pl.when(w == first[p])
            def _():
                for cp in b_loads(p):
                    cp.wait()
                if p + 1 < len(gemms):
                    for cp in b_loads(p + 1):
                        cp.start()

        @pl.when(w >= 2)
        def _():
            o_store(0, w % 2).wait()

        n = tile_of(ff, 512)
        for odd in (0, 1):
            sel = functools.reduce(lambda u, v: u | v, [in_gemm(p, w) for p in range(len(gemms)) if p % 2 == odd])

            @pl.when(sel)
            def _():
                for j in range(ff // n):
                    acc = None
                    for t0, nt, m in b_parts(odd):
                        lhs = a_buf(w % 2, t0 // kh)[pl.ds(t0 % kh, nt)]
                        t = dg(lhs, m[:, pl.ds(j * n, n)], 0, 0)
                        acc = t if acc is None else acc + t
                    o_buf(w % 2)[:, pl.ds(j * n, n)] = acc.astype(BF)

        for p in range(len(gemms)):
            @pl.when(in_gemm(p, w))
            def _():
                o_store(p, w).start()

    def stage_WG(c):
        def one(j, _):
            tile(c * TILES + j)
            return 0

        lax.fori_loop(0, TILES, one, 0)

    def stage_WP(c):
        @pl.when(c == nseq - 1)
        def _():
            start_a(0)
            for cp in b_loads(0):
                cp.start()

    ld_x(0).start()
    for t in (0, 1):
        ld_wqkv(t).start()
    ld_wo.start()
    barrier = pltpu.get_barrier_semaphore()
    for k in range(1, tpn):
        pl.semaphore_signal(barrier, inc=1, device_id={'tp': (tp + k) % tpn}, device_id_type=MESH)
    dgb[...] = jnp.zeros_like(dgb)
    ld_x(0).wait()
    norm_rows()
    pl.semaphore_wait(barrier, tpn - 1)

    run = {'F1': stage_F1, 'MU': stage_MU, 'MD': stage_MD, 'MY': stage_MY, 'B2': stage_B2,
           'YL': stage_YL, 'YS': stage_YS, 'WG': stage_WG, 'WP': stage_WP}
    hops = {'a': stage_a, 'b': stage_b, 'c': stage_c, 'd': stage_d, 'e': stage_e, 'f': stage_f}
    order = ORDER

    def count(name):
        return tiles // TILES if name == 'WG' else nseq

    def step(i, _):
        for name, lag in order:
            c = i - lag

            @pl.when((c >= 0) & (c < count(name)))
            def _():
                if name in run:
                    run[name](c)
                else:
                    hops[name[0]](int(name[1]), c)
        return 0

    lax.fori_loop(0, max(count(n) + l for n, l in order), step, 0)

    ys = [lc(xm.at[pl.ds(k * nseq // 2, nseq // 2)], r, (0, 18)[k]) for k, r in enumerate((ya_o, yb_o))]
    for cp in ys:
        cp.start()
    for b in (0, 1):
        o_store(0, b).wait()
    for k in range(1, tpn):
        c_gain(k).wait_recv()
    tot = dgs[0]
    for t in range(1, tpn):
        tot = tot + dgs[t]
    dgain_o[...] = tot
    for k in range(1, tpn):
        c_gain(k).wait_send()
    for cp in ys:
        cp.wait()


def mega(x, dy, wqkv, wo, wu, wd, ga, gm, heads):
    nseq, slen, dm = x.shape
    he, ff = wo.shape[0], wu.shape[1]
    half = slen // CORES
    blk = half // CHIPS
    hb = blk // 2
    tok = nseq * slen

    def arr(*shape):
        return jax.ShapeDtypeStruct(shape, BF)

    act = arr(tok, dm)
    outs = (arr(nseq // 2, blk, dm), arr(nseq // 2, blk, dm), act, arr(3 * he, dm), arr(he, dm), arr(dm, ff), arr(ff, dm), act, act, act, arr(tok, he),
            arr(nseq, 3 * he, slen), arr(tok, ff), arr(tok, ff), arr(tok, 3 * he), act, jax.ShapeDtypeStruct((2, dm), F32))
    hbm = pl.BlockSpec(memory_space=pl.ANY)
    vm = pl.BlockSpec(memory_space=pltpu.VMEM)
    V = pltpu.VMEM
    scratch = [
        V(wqkv.shape, BF), V(wo.shape, BF), V(wu.shape, BF), V(wd.shape, BF),
        V((2, SLOTS + 1, half, dm), BF), V((2, PAIRS, half, dm), BF),
        V((2, SLOTS, 2, blk, dm), BF), V((2, SLOTS, 2, hb, dm), BF),
        V((slen, dm), BF), V((slen, dm), BF), V((slen, dm), BF), V((slen, dm), BF), V((slen, dm), BF),
        V((3 * he, slen), BF), V((3 * he, slen), BF), V((slen, 3 * he), BF), V((3 * he, slen), BF),
        V((slen, he), BF), V((he, slen), BF), V((slen, ff), BF), V((slen, ff), BF), V((slen, dm), BF),
        V((nseq, blk, dm), BF), V((nseq, blk, dm), BF), V((nseq, blk, dm), BF), V((2, 2, blk, dm), BF), V((2, dm), F32),
        V((CHIPS * CORES, 2, dm), F32),
        pltpu.SemaphoreType.DMA((23,)), pltpu.SemaphoreType.DMA((6, 2)), pltpu.SemaphoreType.DMA((2, CHIPS * CORES)),
        pltpu.SemaphoreType.DMA((2, CHIPS)), pltpu.SemaphoreType.DMA((2,)),
        pltpu.SemaphoreType.DMA((2, 5 * SLOTS)), pltpu.SemaphoreType.DMA((2, 5 * SLOTS)),
        pltpu.SemaphoreType.DMA((2, 8 * nseq)), pltpu.SemaphoreType.DMA((2, 8 * nseq)),
    ]
    flops = 2 * nseq * slen * dm * (4 * he * 2 + ff * 4)
    return pl.pallas_call(
        functools.partial(body, heads),
        name='mega',
        out_shape=outs,
        in_specs=[hbm] * 7 + [vm] * 2,
        out_specs=(hbm,) * 16 + (vm,),
        scratch_shapes=scratch,
        compiler_params=pltpu.CompilerParams(collective_id=0, has_side_effects=True, vmem_limit_bytes=VMEM_BYTES),
        cost_estimate=pl.CostEstimate(flops=flops, bytes_accessed=12 * nseq * slen * dm * 2, transcendentals=0),
    )(x, dy, dy.reshape(tok, dm), wqkv, wo, wu, wd, ga, gm)


def copied(arrays):
    n = len(arrays)
    cuts = []
    for a, v in enumerate(arrays):
        rows = tile_of(v.shape[0], 256 * 3072 // v.shape[1])
        cuts += [(a, r, rows) for r in range(0, v.shape[0], rows)]

    def move(*refs):
        src, dst, buf, isem, osem = refs[:n], refs[n:2 * n], refs[2 * n:3 * n], refs[-2], refs[-1]
        into = [pltpu.make_async_copy(src[a].at[pl.ds(r, m)], buf[a].at[pl.ds(r, m)], isem.at[k]) for k, (a, r, m) in enumerate(cuts)]
        out = [pltpu.make_async_copy(buf[a].at[pl.ds(r, m)], dst[a].at[pl.ds(r, m)], osem.at[k]) for k, (a, r, m) in enumerate(cuts)]
        for cp in into:
            cp.start()
        for k in range(len(cuts)):
            into[k].wait()
            out[k].start()
        for cp in out:
            cp.wait()

    hbm = pl.BlockSpec(memory_space=pl.ANY)
    size = sum(v.size for v in arrays)
    return pl.pallas_call(
        move, in_specs=[hbm] * n, out_specs=(hbm,) * n,
        out_shape=tuple(jax.ShapeDtypeStruct(v.shape, v.dtype) for v in arrays),
        scratch_shapes=[pltpu.VMEM(v.shape, v.dtype) for v in arrays] + [pltpu.SemaphoreType.DMA((len(cuts),))] * 2,
        compiler_params=pltpu.CompilerParams(vmem_limit_bytes=VMEM_BYTES),
        cost_estimate=pl.CostEstimate(flops=size * 500, bytes_accessed=4 * size, transcendentals=0))(*arrays)


def placed(out, pieces, shape, at_of):
    n = len(pieces)
    given = [] if out is None else [out]

    def put(*refs):
        src, dst = refs[:n], refs[n + len(given)]
        buf, isem, osem = refs[n + len(given) + 1:-2], refs[-2], refs[-1]
        tp = lax.axis_index('tp')
        at = at_of(tp // CORES, tp % CORES)
        into = [pltpu.make_async_copy(src[k], buf[k], isem.at[k]) for k in range(n)]
        outc = [pltpu.make_async_copy(
            buf[k], dst.at[pl.ds(at[k][0], p.shape[0]), pl.ds(pl.multiple_of(at[k][1], p.shape[1]), p.shape[1])], osem.at[k])
            for k, p in enumerate(pieces)]
        for cp in into:
            cp.start()
        for k in range(n):
            into[k].wait()
            outc[k].start()
        for cp in outc:
            cp.wait()

    hbm = pl.BlockSpec(memory_space=pl.ANY)
    return pl.pallas_call(
        put, in_specs=[hbm] * (n + len(given)), out_specs=hbm, out_shape=jax.ShapeDtypeStruct(shape, BF),
        scratch_shapes=[pltpu.VMEM(p.shape, p.dtype) for p in pieces] + [pltpu.SemaphoreType.DMA((n,))] * 2,
        input_output_aliases={n: 0} if given else {},
        compiler_params=pltpu.CompilerParams(vmem_limit_bytes=VMEM_BYTES),
        cost_estimate=pl.CostEstimate(flops=sum(p.size for p in pieces) * 500, bytes_accessed=0, transcendentals=0),
    )(*pieces, *given)


def solution(mesh):
    tpn = mesh.shape['tp']
    assert tpn == CHIPS * CORES

    def hop(v, chips_by, cores_by):
        perm = []
        for t in range(tpn):
            ch, co = t // CORES, t % CORES
            perm.append((t, ((ch + chips_by) % CHIPS) * CORES + (co + cores_by) % CORES))
        return lax.ppermute(v, 'tp', perm)

    def gather(va, vb):
        ns, blk, dm = va.shape
        half = blk * CHIPS
        la, rb = hop(va, 1, 0), hop(vb, -1, 0)
        lb, ra = hop(vb, 1, 0), hop(va, -1, 0)
        oa, ob = hop(la, 1, 0), hop(rb, -1, 0)
        near = [va, vb, la, lb, ra, rb]
        near += [hop(p, 0, 1) for p in near]
        far = [oa, ob, hop(oa, 0, 1), hop(ob, 0, 1)]

        def near_at(chip, core):
            chips = (chip, (chip + CHIPS - 1) % CHIPS, (chip + 1) % CHIPS)
            return [(k * ns, co * half + ch * blk) for co in (core, 1 - core) for ch in chips for k in (0, 1)]

        def far_at(chip, core):
            o = ((chip + 2) % CHIPS) * blk
            return [(k * ns, co * half + o) for co in (core, 1 - core) for k in (0, 1)]

        out = placed(None, near, (2 * ns, half * CORES, dm), near_at)
        return placed(out, far, out.shape, far_at)

    def step(x_in, gain_attn, w_qkv, w_out, gain_mlp, w_up, w_down, dy_out):
        heads, e = w_qkv.shape[3:]
        dm = x_in.shape[2]
        he = heads * e
        wqkv = jnp.transpose(w_qkv[0], (1, 2, 3, 0)).reshape(3 * he, dm)
        wo = w_out[0].reshape(he, dm)
        out = mega(x_in, dy_out, wqkv, wo, w_up[0], w_down[0], gain_attn, gain_mlp, heads)
        ya, yb, dx, dwq, dwo, dwu, dwd = out[:7]
        dgain = out[-1]
        dx, dwu, dwo = copied((dx, dwu, dwo))
        dwd, dwq = copied((dwd, dwq))
        y = gather(ya, yb)
        dwq = jnp.transpose(dwq.reshape(3, heads, e, dm), (3, 0, 1, 2))
        return (y, dx.reshape(x_in.shape), dgain[0:1], dwq[None], dwo.reshape(1, heads, e, dm),
                dgain[1:2], dwu[None], dwd[None])

    act = P('dp', None, None)
    in_specs = (act, P(None, None), P(None, None, None, 'tp', None), P(None, 'tp', None, None), P(None, None),
                P(None, None, 'tp'), P(None, 'tp', None), act)
    out_specs = (act, act, P('dp', None), P('dp', None, None, 'tp', None), P('dp', 'tp', None, None), P('dp', None),
                 P('dp', None, 'tp'), P('dp', 'tp', None))
    step = jax.shard_map(step, mesh=mesh, in_specs=in_specs, out_specs=out_specs, check_vma=False)
    return step
```

```python
import functools
import math

import jax
import jax.numpy as jnp
from jax import lax
from jax.experimental import pallas as pl
from jax.experimental.pallas import tpu as pltpu
from jax.sharding import PartitionSpec as P


LN_EPS = 1e-5
CORES = 2
CHIPS = 4
BF = jnp.bfloat16
F32 = jnp.float32
MESH = pl.DeviceIdType.MESH
VMEM_BYTES = 67043328
GELU_C = 0.7978845608028654
GELU_K = 0.044715
SLOTS = 3
PAIRS = 2
TILES = 2

ORDER = (
    ('e3', 15), ('b4', 18), ('e1', 7), ('f3', 16), ('MY', 9), ('a4', 17), ('b3', 10), ('WG', 17), ('a3', 9),
    ('WP', 9), ('d1', 5), ('d3', 12), ('MU', 8), ('c5', 21), ('c1', 3), ('b1', 2), ('f4', 27), ('e4', 22),
    ('b5', 20), ('a5', 19), ('B2', 16), ('a1', 1), ('MD', 8), ('YL', 18), ('f1', 7), ('c3', 10), ('F1', 0),
    ('d4', 20), ('c4', 18), ('YS', 18),
)


def dg(a, b, ca, cb):
    return lax.dot_general(a, b, (((ca,), (cb,)), ((), ())), preferred_element_type=F32)


def ln_parts(z):
    mu = jnp.mean(z, axis=-1, keepdims=True)
    c = z - mu
    var = jnp.mean(c * c, axis=-1, keepdims=True)
    r = lax.rsqrt(var + LN_EPS)
    return c * r, r


def ln_bwd(z, gain, d):
    xhat, r = ln_parts(z)
    h = d * gain
    m1 = jnp.mean(h, axis=-1, keepdims=True)
    m2 = jnp.mean(h * xhat, axis=-1, keepdims=True)
    return r * (h - m1 - xhat * m2), jnp.sum(d * xhat, axis=0, keepdims=True)


def gelu_both(z):
    z2 = z * z
    t = jnp.tanh(GELU_C * (z + GELU_K * (z2 * z)))
    cdf = 0.5 * (1.0 + t)
    d = cdf + z * (0.5 * (1.0 - t * t)) * (GELU_C * (1.0 + (3.0 * GELU_K) * z2))
    return z * cdf, d


def tile_of(n, want):
    t = min(n, want)
    while n % t:
        t //= 2
    return t


def body(heads, x, dy, dyf, wqkv_h, wo_h, wu_h, wd_h, ga, gm,
         ya_o, yb_o, dx_o, dwq_o, dwo_o, dwu_o, dwd_o, nm_o, g_o, a_o, o_o, qkv_o, h_o, dp_o, dq_o, py_o, dgain_o,
         wqkv, wo, wu, wd, S, RD, R1, R2, xb, ab, nb, dyb, gb, qb, qb2, dqb, dqt, ob, obt, hb_, dpb, pyb,
         xs, xm, gs, own, dgb, dgs, lsem, wsem, dsem, ysem, qsem, ssem1, rsem1, ssem, rsem):
    nseq, slen, dm = x.shape
    tok = nseq * slen
    half = slen // CORES
    blk = half // CHIPS
    hb = blk // 2
    he = wo.shape[0]
    e = he // heads
    ff = wu.shape[1]
    scale = e ** -0.5
    tpn = CHIPS * CORES
    tp = lax.axis_index('tp')
    chip = tp // CORES
    core = tp % CORES
    sib = chip * CORES + (1 - core)
    rchip = (chip + 1) % CHIPS
    lchip = (chip + CHIPS - 1) % CHIPS
    ochip = (chip + 2) % CHIPS
    right = rchip * CORES + core
    left = lchip * CORES + core

    def seq(c):
        return pl.ds(pl.multiple_of(c * slen, slen), slen)

    def off(ch, co):
        return pl.multiple_of(co * half + ch * blk, blk)

    myoff = off(chip, core)

    def lc(src, dst, k):
        return pltpu.make_async_copy(src, dst, lsem.at[k])

    qt = tile_of(3 * wo.shape[0], 3 * wo.shape[0] // 2)

    def ld_wqkv(t):
        r = pl.ds(pl.multiple_of(t * qt, qt), qt)
        return pltpu.make_async_copy(wqkv_h.at[r], wqkv.at[r], qsem.at[t])

    ld_wo = lc(wo_h, wo, 1)
    w2 = (lc(wu_h, wu, 2), lc(wd_h, wd, 3))

    def ld_x(c):
        return lc(x.at[c], xb, 4)

    def ld_dy(c):
        return lc(dy.at[c], dyb, 5)

    def ld_nm(c):
        return lc(nm_o.at[seq(c)], nb, 6)

    def ld_g(c):
        return lc(g_o.at[seq(c)], gb, 7)

    def ld_q(c):
        return lc(qkv_o.at[c], qb2, 8)

    def st_a(c):
        return lc(ab, a_o.at[seq(c)], 9)

    def st_q(c):
        return lc(qb, qkv_o.at[c], 10)

    def st_o(c):
        return lc(ob, o_o.at[seq(c)], 11)

    def st_h(c):
        return lc(hb_, h_o.at[seq(c)], 12)

    def st_dp(c):
        return lc(dpb, dp_o.at[seq(c)], 13)

    def st_py(c):
        return lc(pyb, py_o.at[seq(c)], 14)

    def st_dq(c):
        return lc(dqb, dq_o.at[seq(c)], 15)

    xs_ld = lc(x.at[:, pl.ds(myoff, blk), :], xs, 16)
    dys_ld = lc(dy.at[:, pl.ds(myoff, blk), :], gs, 17)
    out_ref = {1: nm_o, 3: g_o, 4: dx_o}
    fset = {1: 0, 3: 1, 4: 0, 5: 1}

    def out_rows(fl, c, o, n):
        return out_ref[fl].at[pl.ds(pl.multiple_of(c * slen + o, n), n)]

    def st_own(fl, c):
        return lc(own.at[fset[fl], c % 2], out_rows(fl, c, myoff, blk), 19 + fset[fl] * 2 + c % 2)

    def rc(kind, fl, c, src, dst, dev):
        f = fset[fl]
        if kind < 5:
            send, recv = ssem1.at[f, kind * SLOTS + c], rsem1.at[f, kind * SLOTS + c]
        else:
            send, recv = (m.at[f, (kind - 5) * nseq + c] for m in (ssem, rsem))
        return pltpu.make_async_remote_copy(
            src_ref=src, dst_ref=dst, send_sem=send, recv_sem=recv,
            device_id={'tp': dev}, device_id_type=MESH)

    def c_pair(fl, c):
        f = fset[fl]
        return rc(0, fl, c % PAIRS, S.at[f, SLOTS], RD.at[f, c % PAIRS], sib)

    def c_first(fl, c, d):
        f, s = fset[fl], c % SLOTS
        src = S.at[f, s, pl.ds(blk + hb if d else hb, blk)]
        return rc(1 + d, fl, c % SLOTS, src, R1.at[f, s, d], left if d else right)

    def c_second(fl, c, d):
        f, s = fset[fl], c % SLOTS
        src = S.at[f, s, pl.ds(2 * blk + hb if d else 0, hb)]
        return rc(3 + d, fl, c % SLOTS, src, R2.at[f, s, d], left if d else right)

    def c_own(fl, c, d):
        dev = (right, left, sib)[d]
        return rc(5 + d, fl, c, own.at[fset[fl], c % 2], out_rows(fl, c, myoff, blk), dev)

    def c_fwd(fl, c, d):
        r = out_rows(fl, c, off(rchip if d else lchip, core) + d * hb, hb)
        return rc(8 + d, fl, c, r, r, left if d else right)

    def c_cross(fl, c, d):
        r = out_rows(fl, c, off((lchip, rchip, ochip)[d], core), blk)
        return rc(10 + d, fl, c, r, r, sib)

    def c_gain(k):
        return pltpu.make_async_remote_copy(
            src_ref=dgb, dst_ref=dgs.at[tp], send_sem=dsem.at[0, k], recv_sem=dsem.at[1, k],
            device_id={'tp': (tp + k) % tpn}, device_id_type=MESH)

    def store_part(f, c, col, n, val):
        v = val.astype(BF)
        s = c % SLOTS
        i0 = s * (1 - core) + SLOTS * core
        i1 = s * core + SLOTS * (1 - core)
        for b in range(CHIPS):
            r = pl.ds(pl.multiple_of(((b + CHIPS - 1 - chip) % CHIPS) * blk, blk), blk)
            S[f, i0, r, pl.ds(col, n)] = v[b * blk:(b + 1) * blk]
            S[f, i1, r, pl.ds(col, n)] = v[half + b * blk:half + (b + 1) * blk]

    def stage_a(fl, c):
        f, s = fset[fl], c % SLOTS
        c_pair(fl, c).wait_recv()
        c_pair(fl, c).wait_send()
        for st in {1: (st_a, st_q, st_o), 3: (st_h, st_dp), 4: (st_dq,), 5: ()}[fl]:
            st(c).wait()

        def add(t, _):
            r = pl.ds(pl.multiple_of(t * hb, hb), hb)
            S[f, s, r] = (S[f, s, r].astype(F32) + RD[f, c % PAIRS, r].astype(F32)).astype(BF)
            return 0

        lax.fori_loop(0, half // hb, add, 0, unroll=2)
        for d in (0, 1):
            c_first(fl, c, d).start()

    def stage_b(fl, c):
        f, s = fset[fl], c % SLOTS
        for d in (0, 1):
            c_first(fl, c, d).wait_recv()
        for d in (0, 1):
            o = pl.ds(2 * blk + hb if d else 0, hb)
            S[f, s, o] = (S[f, s, o].astype(F32) + R1[f, s, d, pl.ds(0 if d else hb, hb)].astype(F32)).astype(BF)
            c_second(fl, c, d).start()

    def stage_c(fl, c):
        f, s = fset[fl], c % SLOTS
        for d in (0, 1):
            c_second(fl, c, d).wait_recv()

        for k in (0, 1):
            q = pl.ds(k * hb, hb)
            o = pl.ds(3 * blk + k * hb, hb)
            tot = S[f, s, o].astype(F32) + R1[f, s, 1 - k, pl.ds(0 if k else hb, hb)].astype(F32) + R2[f, s, k].astype(F32)
            if fl == 1:
                if k == 0:
                    @pl.when(c == 0)
                    def _():
                        xs_ld.wait()

                z = (xs[c, q].astype(F32) + tot).astype(BF)
                xm[c, q] = z
                xh, _ = ln_parts(z.astype(F32))
                own[f, c % 2, q] = (xh * gm[...]).astype(BF)
            elif fl == 3:
                dr, dgn = ln_bwd(xm[c, q].astype(F32), gm[...], tot)
                v = (gs[c, q].astype(F32) + dr).astype(BF)
                gs[c, q] = v
                own[f, c % 2, q] = v
                dgb[1:2] += dgn
            elif fl == 5:
                xm[c, q] = (xm[c, q].astype(F32) + tot).astype(BF)
            else:
                dr, dgn = ln_bwd(xs[c, q].astype(F32), ga[...], tot)
                own[f, c % 2, q] = (gs[c, q].astype(F32) + dr).astype(BF)
                dgb[0:1] += dgn
        if fl != 5:
            for d in (0, 1, 2):
                c_own(fl, c, d).start()
            st_own(fl, c).start()
        for d in (0, 1):
            c_first(fl, c, d).wait_send()
            c_second(fl, c, d).wait_send()
        if fl == 4:
            @pl.when(c == nseq - 1)
            def _():
                dgs[tp] = dgb[...]
                for k in range(1, tpn):
                    c_gain(k).start()

    def stage_d(fl, c):
        for d in (1, 0):
            c_own(fl, c, 1 - d).wait_recv()
            c_fwd(fl, c, 1 - d).start()
        for d in (0, 1):
            c_cross(fl, c, d).start()
        for d in (0, 1, 2):
            c_own(fl, c, d).wait_send()
        st_own(fl, c).wait()

    def stage_e(fl, c):
        for d in (0, 1):
            c_fwd(fl, c, d).wait_recv()
        c_cross(fl, c, 2).start()

    def stage_f(fl, c):
        c_own(fl, c, 2).wait_recv()
        for d in (0, 1, 2):
            c_cross(fl, c, d).wait_recv()
        for d in (0, 1):
            c_fwd(fl, c, d).wait_send()
        for d in (0, 1, 2):
            c_cross(fl, c, d).wait_send()
        if fl == 1:
            ld_nm(c).start()
        if fl == 3:
            ld_g(c).start()

    def probs_t(q_ref, hd):
        qt = q_ref[pl.ds(pl.multiple_of(hd * e, e), e)]
        kt = q_ref[pl.ds(pl.multiple_of(he + hd * e, e), e)]
        vt = q_ref[pl.ds(pl.multiple_of(2 * he + hd * e, e), e)]
        s = dg(kt, qt, 0, 0) * scale
        keep = lax.broadcasted_iota(jnp.int32, (slen, slen), 0) <= lax.broadcasted_iota(jnp.int32, (slen, slen), 1)
        s = jnp.where(keep, s, -1e30)
        ex = jnp.exp(s - jnp.max(s, axis=0, keepdims=True))
        return qt, kt, vt, ex * (1.0 / jnp.sum(ex, axis=0, keepdims=True))

    def norm_rows():
        def ln(t, _):
            r = pl.ds(pl.multiple_of(t * hb, hb), hb)
            xh, _ = ln_parts(xb[r].astype(F32))
            ab[r] = (xh * ga[...]).astype(BF)
            return 0

        lax.fori_loop(0, slen // hb, ln, 0, unroll=4)

    def stage_F1(c):
        @pl.when(c > 0)
        def _():
            ld_x(c).wait()
            norm_rows()

        st_a(c).start()

        @pl.when(c + 1 < nseq)
        def _():
            ld_x(c + 1).start()

        def qkv(t, _):
            @pl.when(c == 0)
            def _():
                ld_wqkv(t).wait()

            r = pl.ds(pl.multiple_of(t * qt, qt), qt)
            qb[r] = dg(wqkv[r], ab[...], 1, 1).astype(BF)
            return 0

        lax.fori_loop(0, 3 * he // qt, qkv, 0)
        st_q(c).start()

        def head(hd, _):
            _, _, vt, p = probs_t(qb, hd)
            obt[pl.ds(pl.multiple_of(hd * e, e), e)] = dg(vt, p.astype(BF), 1, 0).astype(BF)
            return 0

        lax.fori_loop(0, heads, head, 0, unroll=True)
        tr = tile_of(he, 128)
        for t in range(he // tr):
            ob[:, t * tr:(t + 1) * tr] = obt[t * tr:(t + 1) * tr].T
        st_o(c).start()
        n = tile_of(dm, 1024)

        @pl.when(c == 0)
        def _():
            ld_wo.wait()
            for w in w2:
                w.start()
            for w in (xs_ld, dys_ld, ld_dy(0)):
                w.start()

        def proj(t, _):
            col = pl.multiple_of(t * n, n)
            store_part(0, c, col, n, dg(ob[...], wo[:, pl.ds(col, n)], 1, 0))
            return 0

        lax.fori_loop(0, dm // n, proj, 0)
        c_pair(1, c).start()

    def stage_MU(c):
        @pl.when(c == 0)
        def _():
            for w in w2:
                w.wait()
            dys_ld.wait()

        ld_nm(c).wait()
        ld_dy(c).wait()
        n = tile_of(ff, 768)

        def up(t, _):
            col = pl.ds(pl.multiple_of(t * n, n), n)
            pre = dg(nb[...], wu[:, col], 1, 0)
            dh = dg(dyb[...], wd[col], 1, 1)
            act, der = gelu_both(pre)
            hb_[:, col] = act.astype(BF)
            dpb[:, col] = (dh.astype(BF).astype(F32) * der).astype(BF)
            return 0

        lax.fori_loop(0, ff // n, up, 0)
        st_h(c).start()
        st_dp(c).start()

        @pl.when(c + 1 < nseq)
        def _():
            ld_dy(c + 1).start()

    m = tile_of(dm, 1024)

    def stage_MD(c):
        def down(t, _):
            col = pl.multiple_of(t * m, m)
            store_part(1, c, col, m, dg(dpb[...], wu[pl.ds(col, m)], 1, 1))
            return 0

        lax.fori_loop(0, dm // m, down, 0)
        c_pair(3, c).start()

    def stage_MY(c):
        @pl.when(c > 0)
        def _():
            st_py(c - 1).wait()

        def outp(t, _):
            col = pl.multiple_of(t * m, m)
            pyb[:, pl.ds(col, m)] = dg(hb_[...], wd[:, pl.ds(col, m)], 1, 0).astype(BF)
            return 0

        lax.fori_loop(0, dm // m, outp, 0)
        st_py(c).start()

    def stage_B2(c):
        ld_q(c).start()
        ld_g(c).wait()
        obt[...] = dg(wo[...], gb[...], 1, 1).astype(BF)
        ld_q(c).wait()

        def head(hd, _):
            qt, kt, vt, p = probs_t(qb2, hd)
            do = obt[pl.ds(pl.multiple_of(hd * e, e), e)]
            dqt[pl.ds(pl.multiple_of(2 * he + hd * e, e), e)] = dg(do, p.astype(BF), 1, 1).astype(BF)
            dpr = dg(vt, do, 0, 0).astype(BF).astype(F32)
            ds = p * (dpr - jnp.sum(dpr * p, axis=0, keepdims=True))
            ds = (ds * scale).astype(BF)
            dqt[pl.ds(pl.multiple_of(hd * e, e), e)] = dg(kt, ds, 1, 0).astype(BF)
            dqt[pl.ds(pl.multiple_of(he + hd * e, e), e)] = dg(qt, ds, 1, 1).astype(BF)
            return 0

        lax.fori_loop(0, heads, head, 0, unroll=2)
        tr = tile_of(3 * he, 128)
        for t in range(3 * he // tr):
            dqb[:, t * tr:(t + 1) * tr] = dqt[t * tr:(t + 1) * tr].T
        st_dq(c).start()
        n = tile_of(dm, 1024)

        def proj(t, _):
            col = pl.multiple_of(t * n, n)
            store_part(0, c, col, n, dg(dqb[...], wqkv[:, pl.ds(col, n)], 1, 0))
            return 0

        lax.fori_loop(0, dm // n, proj, 0)
        c_pair(4, c).start()

    def y_loads(c):
        s = c % SLOTS

        cps = []
        for b in range(CHIPS):
            ch = (chip + 1 + b) % CHIPS
            for k, (co, t) in enumerate(((1 - core, SLOTS), (core, s))):
                src = py_o.at[pl.ds(pl.multiple_of(c * slen + co * half + ch * blk, blk), blk)]
                cps.append(pltpu.make_async_copy(src, S.at[1, t, pl.ds(b * blk, blk)], ysem.at[k, b]))
        return cps

    def stage_YL(c):
        @pl.when(c == nseq - 1)
        def _():
            st_py(c).wait()

        for cp in y_loads(c):
            cp.start()

    def stage_YS(c):
        for cp in y_loads(c):
            cp.wait()
        c_pair(5, c).start()

    kh = tok // 2
    gemms = []
    for lhs, rhs, res in ((nm_o, dp_o, dwu_o), (h_o, dyf, dwd_o), (dq_o, a_o, dwq_o), (o_o, g_o, dwo_o)):
        for cb in range(rhs.shape[1] // ff):
            gemms.append((lhs, rhs, res, lhs.shape[1] // he, cb * ff))
    first = [sum(g[3] for g in gemms[:p]) for p in range(len(gemms) + 1)]
    tiles = first[-1]

    def a_buf(b, k):
        return wd.at[pl.ds(0, kh), pl.ds(pl.multiple_of((2 * b + k) * he, he), he)]

    def b_parts(p):
        if p % 2 == 0:
            return [(0, kh, wu.at[pl.ds(0, kh)]), (kh, kh, wu.at[pl.ds(kh, kh)])]
        q = kh // 2
        return [(0, kh, wd.at[pl.ds(0, kh), pl.ds(ff, ff)]), (kh, q, wd.at[pl.ds(kh, q), pl.ds(0, ff)]),
                (kh + q, q, wd.at[pl.ds(kh, q), pl.ds(ff, ff)])]

    def o_buf(b):
        return wu.at[pl.ds(pl.multiple_of(tok + b * he, math.gcd(tok, he)), he)]

    def a_load(p, w, k):
        col = pl.multiple_of((w - first[p]) * he, he)
        return pltpu.make_async_copy(gemms[p][0].at[pl.ds(k * kh, kh), pl.ds(col, he)], a_buf(w % 2, k), wsem.at[k, w % 2])

    def b_loads(p):
        return [pltpu.make_async_copy(gemms[p][1].at[pl.ds(t, n), pl.ds(gemms[p][4], ff)], m, wsem.at[3 + q, p % 2])
                for q, (t, n, m) in enumerate(b_parts(p))]

    def o_store(p, w):
        row = pl.multiple_of((w - first[p]) * he, he)
        return pltpu.make_async_copy(o_buf(w % 2), gemms[p][2].at[pl.ds(row, he), pl.ds(gemms[p][4], ff)], wsem.at[2, w % 2])

    def in_gemm(p, w):
        return (w >= first[p]) & (w < first[p + 1])

    def start_a(w):
        for p in range(len(gemms)):
            @pl.when(in_gemm(p, w))
            def _():
                for k in (0, 1):
                    a_load(p, w, k).start()

    def tile(w):
        for k in (0, 1):
            a_load(0, w % 2, k).wait()
        start_a(w + 1)
        for p in range(len(gemms)):
            @pl.when(w == first[p])
            def _():
                for cp in b_loads(p):
                    cp.wait()
                if p + 1 < len(gemms):
                    for cp in b_loads(p + 1):
                        cp.start()

        @pl.when(w >= 2)
        def _():
            o_store(0, w % 2).wait()

        n = tile_of(ff, 512)
        for odd in (0, 1):
            sel = functools.reduce(lambda u, v: u | v, [in_gemm(p, w) for p in range(len(gemms)) if p % 2 == odd])

            @pl.when(sel)
            def _():
                for j in range(ff // n):
                    acc = None
                    for t0, nt, m in b_parts(odd):
                        lhs = a_buf(w % 2, t0 // kh)[pl.ds(t0 % kh, nt)]
                        t = dg(lhs, m[:, pl.ds(j * n, n)], 0, 0)
                        acc = t if acc is None else acc + t
                    o_buf(w % 2)[:, pl.ds(j * n, n)] = acc.astype(BF)

        for p in range(len(gemms)):
            @pl.when(in_gemm(p, w))
            def _():
                o_store(p, w).start()

    def stage_WG(c):
        def one(j, _):
            tile(c * TILES + j)
            return 0

        lax.fori_loop(0, TILES, one, 0)

    def stage_WP(c):
        @pl.when(c == nseq - 1)
        def _():
            start_a(0)
            for cp in b_loads(0):
                cp.start()

    ld_x(0).start()
    for t in (0, 1):
        ld_wqkv(t).start()
    ld_wo.start()
    barrier = pltpu.get_barrier_semaphore()
    for k in range(1, tpn):
        pl.semaphore_signal(barrier, inc=1, device_id={'tp': (tp + k) % tpn}, device_id_type=MESH)
    dgb[...] = jnp.zeros_like(dgb)
    ld_x(0).wait()
    norm_rows()
    pl.semaphore_wait(barrier, tpn - 1)

    run = {'F1': stage_F1, 'MU': stage_MU, 'MD': stage_MD, 'MY': stage_MY, 'B2': stage_B2,
           'YL': stage_YL, 'YS': stage_YS, 'WG': stage_WG, 'WP': stage_WP}
    hops = {'a': stage_a, 'b': stage_b, 'c': stage_c, 'd': stage_d, 'e': stage_e, 'f': stage_f}
    order = ORDER

    def count(name):
        return tiles // TILES if name == 'WG' else nseq

    def step(i, _):
        for name, lag in order:
            c = i - lag

            @pl.when((c >= 0) & (c < count(name)))
            def _():
                if name in run:
                    run[name](c)
                else:
                    hops[name[0]](int(name[1]), c)
        return 0

    lax.fori_loop(0, max(count(n) + l for n, l in order), step, 0)

    ys = [lc(xm.at[pl.ds(k * nseq // 2, nseq // 2)], r, (0, 18)[k]) for k, r in enumerate((ya_o, yb_o))]
    for cp in ys:
        cp.start()
    for b in (0, 1):
        o_store(0, b).wait()
    for k in range(1, tpn):
        c_gain(k).wait_recv()
    tot = dgs[0]
    for t in range(1, tpn):
        tot = tot + dgs[t]
    dgain_o[...] = tot
    for k in range(1, tpn):
        c_gain(k).wait_send()
    for cp in ys:
        cp.wait()


def mega(x, dy, wqkv, wo, wu, wd, ga, gm, heads):
    nseq, slen, dm = x.shape
    he, ff = wo.shape[0], wu.shape[1]
    half = slen // CORES
    blk = half // CHIPS
    hb = blk // 2
    tok = nseq * slen

    def arr(*shape):
        return jax.ShapeDtypeStruct(shape, BF)

    act = arr(tok, dm)
    outs = (arr(nseq // 2, blk, dm), arr(nseq // 2, blk, dm), act, arr(3 * he, dm), arr(he, dm), arr(dm, ff), arr(ff, dm), act, act, act, arr(tok, he),
            arr(nseq, 3 * he, slen), arr(tok, ff), arr(tok, ff), arr(tok, 3 * he), act, jax.ShapeDtypeStruct((2, dm), F32))
    hbm = pl.BlockSpec(memory_space=pl.ANY)
    vm = pl.BlockSpec(memory_space=pltpu.VMEM)
    V = pltpu.VMEM
    scratch = [
        V(wqkv.shape, BF), V(wo.shape, BF), V(wu.shape, BF), V(wd.shape, BF),
        V((2, SLOTS + 1, half, dm), BF), V((2, PAIRS, half, dm), BF),
        V((2, SLOTS, 2, blk, dm), BF), V((2, SLOTS, 2, hb, dm), BF),
        V((slen, dm), BF), V((slen, dm), BF), V((slen, dm), BF), V((slen, dm), BF), V((slen, dm), BF),
        V((3 * he, slen), BF), V((3 * he, slen), BF), V((slen, 3 * he), BF), V((3 * he, slen), BF),
        V((slen, he), BF), V((he, slen), BF), V((slen, ff), BF), V((slen, ff), BF), V((slen, dm), BF),
        V((nseq, blk, dm), BF), V((nseq, blk, dm), BF), V((nseq, blk, dm), BF), V((2, 2, blk, dm), BF), V((2, dm), F32),
        V((CHIPS * CORES, 2, dm), F32),
        pltpu.SemaphoreType.DMA((23,)), pltpu.SemaphoreType.DMA((6, 2)), pltpu.SemaphoreType.DMA((2, CHIPS * CORES)),
        pltpu.SemaphoreType.DMA((2, CHIPS)), pltpu.SemaphoreType.DMA((2,)),
        pltpu.SemaphoreType.DMA((2, 5 * SLOTS)), pltpu.SemaphoreType.DMA((2, 5 * SLOTS)),
        pltpu.SemaphoreType.DMA((2, 8 * nseq)), pltpu.SemaphoreType.DMA((2, 8 * nseq)),
    ]
    flops = 2 * nseq * slen * dm * (4 * he * 2 + ff * 4)
    return pl.pallas_call(
        functools.partial(body, heads),
        name='mega',
        out_shape=outs,
        in_specs=[hbm] * 7 + [vm] * 2,
        out_specs=(hbm,) * 16 + (vm,),
        scratch_shapes=scratch,
        compiler_params=pltpu.CompilerParams(collective_id=0, has_side_effects=True, vmem_limit_bytes=VMEM_BYTES),
        cost_estimate=pl.CostEstimate(flops=flops, bytes_accessed=12 * nseq * slen * dm * 2, transcendentals=0),
    )(x, dy, dy.reshape(tok, dm), wqkv, wo, wu, wd, ga, gm)


def copied(arrays):
    n = len(arrays)
    cuts = []
    for a, v in enumerate(arrays):
        rows = tile_of(v.shape[0], 256 * 3072 // v.shape[1])
        cuts += [(a, r, rows) for r in range(0, v.shape[0], rows)]

    def move(*refs):
        src, dst, buf, isem, osem = refs[:n], refs[n:2 * n], refs[2 * n:3 * n], refs[-2], refs[-1]
        into = [pltpu.make_async_copy(src[a].at[pl.ds(r, m)], buf[a].at[pl.ds(r, m)], isem.at[k]) for k, (a, r, m) in enumerate(cuts)]
        out = [pltpu.make_async_copy(buf[a].at[pl.ds(r, m)], dst[a].at[pl.ds(r, m)], osem.at[k]) for k, (a, r, m) in enumerate(cuts)]
        for cp in into:
            cp.start()
        for k in range(len(cuts)):
            into[k].wait()
            out[k].start()
        for cp in out:
            cp.wait()

    hbm = pl.BlockSpec(memory_space=pl.ANY)
    size = sum(v.size for v in arrays)
    return pl.pallas_call(
        move, in_specs=[hbm] * n, out_specs=(hbm,) * n,
        out_shape=tuple(jax.ShapeDtypeStruct(v.shape, v.dtype) for v in arrays),
        scratch_shapes=[pltpu.VMEM(v.shape, v.dtype) for v in arrays] + [pltpu.SemaphoreType.DMA((len(cuts),))] * 2,
        compiler_params=pltpu.CompilerParams(vmem_limit_bytes=VMEM_BYTES),
        cost_estimate=pl.CostEstimate(flops=size * 500, bytes_accessed=4 * size, transcendentals=0))(*arrays)


def placed(out, pieces, shape, at_of):
    n = len(pieces)
    given = [] if out is None else [out]

    def put(*refs):
        src, dst = refs[:n], refs[n + len(given)]
        buf, isem, osem = refs[n + len(given) + 1:-2], refs[-2], refs[-1]
        tp = lax.axis_index('tp')
        at = at_of(tp // CORES, tp % CORES)
        into = [pltpu.make_async_copy(src[k], buf[k], isem.at[k]) for k in range(n)]
        outc = [pltpu.make_async_copy(
            buf[k], dst.at[pl.ds(at[k][0], p.shape[0]), pl.ds(pl.multiple_of(at[k][1], p.shape[1]), p.shape[1])], osem.at[k])
            for k, p in enumerate(pieces)]
        for cp in into:
            cp.start()
        for k in range(n):
            into[k].wait()
            outc[k].start()
        for cp in outc:
            cp.wait()

    hbm = pl.BlockSpec(memory_space=pl.ANY)
    return pl.pallas_call(
        put, in_specs=[hbm] * (n + len(given)), out_specs=hbm, out_shape=jax.ShapeDtypeStruct(shape, BF),
        scratch_shapes=[pltpu.VMEM(p.shape, p.dtype) for p in pieces] + [pltpu.SemaphoreType.DMA((n,))] * 2,
        input_output_aliases={n: 0} if given else {},
        compiler_params=pltpu.CompilerParams(vmem_limit_bytes=VMEM_BYTES),
        cost_estimate=pl.CostEstimate(flops=sum(p.size for p in pieces) * 500, bytes_accessed=0, transcendentals=0),
    )(*pieces, *given)


def solution(mesh):
    tpn = mesh.shape['tp']
    assert tpn == CHIPS * CORES

    def hop(v, chips_by, cores_by):
        perm = []
        for t in range(tpn):
            ch, co = t // CORES, t % CORES
            perm.append((t, ((ch + chips_by) % CHIPS) * CORES + (co + cores_by) % CORES))
        return lax.ppermute(v, 'tp', perm)

    def gather(va, vb):
        ns, blk, dm = va.shape
        half = blk * CHIPS
        la, rb = hop(va, 1, 0), hop(vb, -1, 0)
        lb, ra = hop(vb, 1, 0), hop(va, -1, 0)
        n2 = ns // 2
        opp = [(hop(la[k * n2:(k + 1) * n2], 1, 0), hop(rb[k * n2:(k + 1) * n2], -1, 0))
               for k in (0, 1)]
        near = [va, vb, la, lb, ra, rb]
        near += [hop(p, 0, 1) for p in near]
        far = [p + tuple(hop(v, 0, 1) for v in p) for p in opp]

        def near_at(chip, core):
            chips = (chip, (chip + CHIPS - 1) % CHIPS, (chip + 1) % CHIPS)
            return [(k * ns, co * half + ch * blk) for co in (core, 1 - core) for ch in chips for k in (0, 1)]

        def far_at(part, chip, core):
            o = ((chip + 2) % CHIPS) * blk
            return [(k * ns + part * n2, co * half + o) for co in (core, 1 - core) for k in (0, 1)]

        out = placed(None, near, (2 * ns, half * CORES, dm), near_at)
        for k in (0, 1):
            out = placed(out, far[k], out.shape, functools.partial(far_at, k))
        return out

    def step(x_in, gain_attn, w_qkv, w_out, gain_mlp, w_up, w_down, dy_out):
        heads, e = w_qkv.shape[3:]
        dm = x_in.shape[2]
        he = heads * e
        wqkv = jnp.transpose(w_qkv[0], (1, 2, 3, 0)).reshape(3 * he, dm)
        wo = w_out[0].reshape(he, dm)
        out = mega(x_in, dy_out, wqkv, wo, w_up[0], w_down[0], gain_attn, gain_mlp, heads)
        ya, yb, dx, dwq, dwo, dwu, dwd = out[:7]
        dgain = out[-1]
        dx, dwu, dwo = copied((dx, dwu, dwo))
        dwd, dwq = copied((dwd, dwq))
        y = gather(ya, yb)
        dwq = jnp.transpose(dwq.reshape(3, heads, e, dm), (3, 0, 1, 2))
        return (y, dx.reshape(x_in.shape), dgain[0:1], dwq[None], dwo.reshape(1, heads, e, dm),
                dgain[1:2], dwu[None], dwd[None])

    act = P('dp', None, None)
    in_specs = (act, P(None, None), P(None, None, None, 'tp', None), P(None, 'tp', None, None), P(None, None),
                P(None, None, 'tp'), P(None, 'tp', None), act)
    out_specs = (act, act, P('dp', None), P('dp', None, None, 'tp', None), P('dp', 'tp', None, None), P('dp', None),
                 P('dp', None, 'tp'), P('dp', 'tp', None))
    step = jax.shard_map(step, mesh=mesh, in_specs=in_specs, out_specs=out_specs, check_vma=False)
    return step
```

```python
import functools
import math

import jax
import jax.numpy as jnp
from jax import lax
from jax.experimental import pallas as pl
from jax.experimental.pallas import tpu as pltpu
from jax.sharding import PartitionSpec as P


LN_EPS = 1e-5
CORES = 2
CHIPS = 4
BF = jnp.bfloat16
F32 = jnp.float32
MESH = pl.DeviceIdType.MESH
VMEM_BYTES = 67043328
GELU_C = 0.7978845608028654
GELU_K = 0.044715
SLOTS = 3
PAIRS = 2
TILES = 2

ORDER = (
    ('a3', 9), ('b5', 20), ('a1', 1), ('a5', 19), ('F1', 0), ('d4', 20), ('MU', 8), ('f1', 7), ('c4', 18),
    ('YL', 18), ('d1', 4), ('B2', 16), ('WP', 9), ('b4', 17), ('d3', 11), ('f3', 15), ('YS', 18), ('a4', 16),
    ('c3', 10), ('WG', 16), ('e1', 5), ('MD', 8), ('c1', 2), ('MY', 8), ('e4', 21), ('c5', 20), ('e3', 14),
    ('b3', 9), ('f4', 22), ('b1', 1),
)


def dg(a, b, ca, cb):
    return lax.dot_general(a, b, (((ca,), (cb,)), ((), ())), preferred_element_type=F32)


def ln_parts(z):
    mu = jnp.mean(z, axis=-1, keepdims=True)
    c = z - mu
    var = jnp.mean(c * c, axis=-1, keepdims=True)
    r = lax.rsqrt(var + LN_EPS)
    return c * r, r


def ln_bwd(z, gain, d):
    xhat, r = ln_parts(z)
    h = d * gain
    m1 = jnp.mean(h, axis=-1, keepdims=True)
    m2 = jnp.mean(h * xhat, axis=-1, keepdims=True)
    return r * (h - m1 - xhat * m2), jnp.sum(d * xhat, axis=0, keepdims=True)


def gelu_both(z):
    z2 = z * z
    t = jnp.tanh(GELU_C * (z + GELU_K * (z2 * z)))
    cdf = 0.5 * (1.0 + t)
    d = cdf + z * (0.5 * (1.0 - t * t)) * (GELU_C * (1.0 + (3.0 * GELU_K) * z2))
    return z * cdf, d


def tile_of(n, want):
    t = min(n, want)
    while n % t:
        t //= 2
    return t


def body(heads, x, dy, dyf, wqkv_h, wo_h, wu_h, wd_h, ga, gm,
         ya_o, yb_o, dx_o, dwq_o, dwo_o, dwu_o, dwd_o, nm_o, g_o, a_o, o_o, qkv_o, h_o, dp_o, dq_o, py_o, dgain_o,
         wqkv, wo, wu, wd, S, RD, R1, R2, xb, ab, nb, dyb, gb, qb, qb2, dqb, dqt, ob, obt, hb_, dpb, pyb,
         xs, xm, gs, own, dgb, dgs, lsem, wsem, dsem, ysem, qsem, ssem1, rsem1, ssem, rsem):
    nseq, slen, dm = x.shape
    tok = nseq * slen
    half = slen // CORES
    blk = half // CHIPS
    hb = blk // 2
    he = wo.shape[0]
    e = he // heads
    ff = wu.shape[1]
    scale = e ** -0.5
    tpn = CHIPS * CORES
    tp = lax.axis_index('tp')
    chip = tp // CORES
    core = tp % CORES
    sib = chip * CORES + (1 - core)
    rchip = (chip + 1) % CHIPS
    lchip = (chip + CHIPS - 1) % CHIPS
    ochip = (chip + 2) % CHIPS
    right = rchip * CORES + core
    left = lchip * CORES + core

    def seq(c):
        return pl.ds(pl.multiple_of(c * slen, slen), slen)

    def off(ch, co):
        return pl.multiple_of(co * half + ch * blk, blk)

    myoff = off(chip, core)

    def lc(src, dst, k):
        return pltpu.make_async_copy(src, dst, lsem.at[k])

    qt = tile_of(3 * wo.shape[0], 3 * wo.shape[0] // 2)

    def ld_wqkv(t):
        r = pl.ds(pl.multiple_of(t * qt, qt), qt)
        return pltpu.make_async_copy(wqkv_h.at[r], wqkv.at[r], qsem.at[t])

    ld_wo = lc(wo_h, wo, 1)
    w2 = (lc(wu_h, wu, 2), lc(wd_h, wd, 3))

    def ld_x(c):
        return lc(x.at[c], xb, 4)

    def ld_dy(c):
        return lc(dy.at[c], dyb, 5)

    def ld_nm(c):
        return lc(nm_o.at[seq(c)], nb, 6)

    def ld_g(c):
        return lc(g_o.at[seq(c)], gb, 7)

    def ld_q(c):
        return lc(qkv_o.at[c], qb2, 8)

    def st_a(c):
        return lc(ab, a_o.at[seq(c)], 9)

    def st_q(c):
        return lc(qb, qkv_o.at[c], 10)

    def st_o(c):
        return lc(ob, o_o.at[seq(c)], 11)

    def st_h(c):
        return lc(hb_, h_o.at[seq(c)], 12)

    def st_dp(c):
        return lc(dpb, dp_o.at[seq(c)], 13)

    def st_py(c):
        return lc(pyb, py_o.at[seq(c)], 14)

    def st_dq(c):
        return lc(dqb, dq_o.at[seq(c)], 15)

    xs_ld = lc(x.at[:, pl.ds(myoff, blk), :], xs, 16)
    dys_ld = lc(dy.at[:, pl.ds(myoff, blk), :], gs, 17)
    out_ref = {1: nm_o, 3: g_o, 4: dx_o}
    fset = {1: 0, 3: 1, 4: 0, 5: 1}

    def out_rows(fl, c, o, n):
        return out_ref[fl].at[pl.ds(pl.multiple_of(c * slen + o, n), n)]

    def st_own(fl, c):
        return lc(own.at[fset[fl], c % 2], out_rows(fl, c, myoff, blk), 19 + fset[fl] * 2 + c % 2)

    def rc(kind, fl, c, src, dst, dev):
        f = fset[fl]
        if kind < 5:
            send, recv = ssem1.at[f, kind * SLOTS + c], rsem1.at[f, kind * SLOTS + c]
        else:
            send, recv = (m.at[f, (kind - 5) * nseq + c] for m in (ssem, rsem))
        return pltpu.make_async_remote_copy(
            src_ref=src, dst_ref=dst, send_sem=send, recv_sem=recv,
            device_id={'tp': dev}, device_id_type=MESH)

    def c_pair(fl, c):
        f = fset[fl]
        return rc(0, fl, c % PAIRS, S.at[f, SLOTS], RD.at[f, c % PAIRS], sib)

    def c_first(fl, c, d):
        f, s = fset[fl], c % SLOTS
        src = S.at[f, s, pl.ds(blk + hb if d else hb, blk)]
        return rc(1 + d, fl, c % SLOTS, src, R1.at[f, s, d], left if d else right)

    def c_second(fl, c, d):
        f, s = fset[fl], c % SLOTS
        src = S.at[f, s, pl.ds(2 * blk + hb if d else 0, hb)]
        return rc(3 + d, fl, c % SLOTS, src, R2.at[f, s, d], left if d else right)

    def c_own(fl, c, d):
        dev = (right, left, sib)[d]
        return rc(5 + d, fl, c, own.at[fset[fl], c % 2], out_rows(fl, c, myoff, blk), dev)

    def c_fwd(fl, c, d):
        r = out_rows(fl, c, off(rchip if d else lchip, core) + d * hb, hb)
        return rc(8 + d, fl, c, r, r, left if d else right)

    def c_cross(fl, c, d):
        r = out_rows(fl, c, off((lchip, rchip, ochip)[d], core), blk)
        return rc(10 + d, fl, c, r, r, sib)

    def c_gain(k):
        return pltpu.make_async_remote_copy(
            src_ref=dgb, dst_ref=dgs.at[tp], send_sem=dsem.at[0, k], recv_sem=dsem.at[1, k],
            device_id={'tp': (tp + k) % tpn}, device_id_type=MESH)

    def store_part(f, c, col, n, val):
        v = val.astype(BF)
        s = c % SLOTS
        i0 = s * (1 - core) + SLOTS * core
        i1 = s * core + SLOTS * (1 - core)
        for b in range(CHIPS):
            r = pl.ds(pl.multiple_of(((b + CHIPS - 1 - chip) % CHIPS) * blk, blk), blk)
            S[f, i0, r, pl.ds(col, n)] = v[b * blk:(b + 1) * blk]
            S[f, i1, r, pl.ds(col, n)] = v[half + b * blk:half + (b + 1) * blk]

    def stage_a(fl, c):
        f, s = fset[fl], c % SLOTS
        c_pair(fl, c).wait_recv()
        c_pair(fl, c).wait_send()
        for st in {1: (st_a, st_q, st_o), 3: (st_h, st_dp), 4: (st_dq,), 5: ()}[fl]:
            st(c).wait()

        def add(t, _):
            r = pl.ds(pl.multiple_of(t * hb, hb), hb)
            S[f, s, r] = S[f, s, r] + RD[f, c % PAIRS, r]
            return 0

        lax.fori_loop(0, half // hb, add, 0, unroll=8)
        for d in (0, 1):
            c_first(fl, c, d).start()

    def stage_b(fl, c):
        f, s = fset[fl], c % SLOTS
        for d in (0, 1):
            c_first(fl, c, d).wait_recv()
        for d in (0, 1):
            o = pl.ds(2 * blk + hb if d else 0, hb)
            S[f, s, o] = (S[f, s, o].astype(F32) + R1[f, s, d, pl.ds(0 if d else hb, hb)].astype(F32)).astype(BF)
            c_second(fl, c, d).start()

    def stage_c(fl, c):
        f, s = fset[fl], c % SLOTS
        for d in (0, 1):
            c_second(fl, c, d).wait_recv()

        for k in (0, 1):
            q = pl.ds(k * hb, hb)
            o = pl.ds(3 * blk + k * hb, hb)
            tot = S[f, s, o].astype(F32) + R1[f, s, 1 - k, pl.ds(0 if k else hb, hb)].astype(F32) + R2[f, s, k].astype(F32)
            if fl == 1:
                if k == 0:
                    @pl.when(c == 0)
                    def _():
                        xs_ld.wait()

                z = (xs[c, q].astype(F32) + tot).astype(BF)
                xm[c, q] = z
                xh, _ = ln_parts(z.astype(F32))
                own[f, c % 2, q] = (xh * gm[...]).astype(BF)
            elif fl == 3:
                dr, dgn = ln_bwd(xm[c, q].astype(F32), gm[...], tot)
                v = (gs[c, q].astype(F32) + dr).astype(BF)
                gs[c, q] = v
                own[f, c % 2, q] = v
                dgb[1:2] += dgn
            elif fl == 5:
                xm[c, q] = (xm[c, q].astype(F32) + tot).astype(BF)
            else:
                dr, dgn = ln_bwd(xs[c, q].astype(F32), ga[...], tot)
                own[f, c % 2, q] = (gs[c, q].astype(F32) + dr).astype(BF)
                dgb[0:1] += dgn
        if fl != 5:
            for d in (0, 1, 2):
                c_own(fl, c, d).start()
            st_own(fl, c).start()
        for d in (0, 1):
            c_first(fl, c, d).wait_send()
            c_second(fl, c, d).wait_send()
        if fl == 4:
            @pl.when(c == nseq - 1)
            def _():
                dgs[tp] = dgb[...]
                for k in range(1, tpn):
                    c_gain(k).start()

    def stage_d(fl, c):
        for d in (1, 0):
            c_own(fl, c, 1 - d).wait_recv()
            c_fwd(fl, c, 1 - d).start()
        for d in (0, 1):
            c_cross(fl, c, d).start()
        for d in (0, 1, 2):
            c_own(fl, c, d).wait_send()
        st_own(fl, c).wait()

    def stage_e(fl, c):
        for d in (0, 1):
            c_fwd(fl, c, d).wait_recv()
        c_cross(fl, c, 2).start()

    def stage_f(fl, c):
        c_own(fl, c, 2).wait_recv()
        for d in (0, 1, 2):
            c_cross(fl, c, d).wait_recv()
        for d in (0, 1):
            c_fwd(fl, c, d).wait_send()
        for d in (0, 1, 2):
            c_cross(fl, c, d).wait_send()
        if fl == 1:
            ld_nm(c).start()
        if fl == 3:
            ld_g(c).start()

    def probs_t(q_ref, hd):
        qt = q_ref[pl.ds(pl.multiple_of(hd * e, e), e)]
        kt = q_ref[pl.ds(pl.multiple_of(he + hd * e, e), e)]
        vt = q_ref[pl.ds(pl.multiple_of(2 * he + hd * e, e), e)]
        s = dg(kt, qt, 0, 0) * scale
        keep = lax.broadcasted_iota(jnp.int32, (slen, slen), 0) <= lax.broadcasted_iota(jnp.int32, (slen, slen), 1)
        s = jnp.where(keep, s, -1e30)
        ex = jnp.exp(s - jnp.max(s, axis=0, keepdims=True))
        return qt, kt, vt, ex * (1.0 / jnp.sum(ex, axis=0, keepdims=True))

    def norm_rows():
        def ln(t, _):
            r = pl.ds(pl.multiple_of(t * hb, hb), hb)
            xh, _ = ln_parts(xb[r].astype(F32))
            ab[r] = (xh * ga[...]).astype(BF)
            return 0

        lax.fori_loop(0, slen // hb, ln, 0, unroll=8)

    def stage_F1(c):
        @pl.when(c > 0)
        def _():
            ld_x(c).wait()
            norm_rows()

        st_a(c).start()

        @pl.when(c + 1 < nseq)
        def _():
            ld_x(c + 1).start()

        def qkv(t, _):
            @pl.when(c == 0)
            def _():
                ld_wqkv(t).wait()

            r = pl.ds(pl.multiple_of(t * qt, qt), qt)
            qb[r] = dg(wqkv[r], ab[...], 1, 1).astype(BF)
            return 0

        lax.fori_loop(0, 3 * he // qt, qkv, 0)
        st_q(c).start()

        def head(hd, _):
            _, _, vt, p = probs_t(qb, hd)
            obt[pl.ds(pl.multiple_of(hd * e, e), e)] = dg(vt, p.astype(BF), 1, 0).astype(BF)
            return 0

        lax.fori_loop(0, heads, head, 0, unroll=True)
        tr = tile_of(he, 128)
        for t in range(he // tr):
            ob[:, t * tr:(t + 1) * tr] = obt[t * tr:(t + 1) * tr].T
        st_o(c).start()
        n = tile_of(dm, 3072)

        @pl.when(c == 0)
        def _():
            ld_wo.wait()
            for w in w2:
                w.start()
            for w in (xs_ld, dys_ld, ld_dy(0)):
                w.start()

        def proj(t, _):
            col = pl.multiple_of(t * n, n)
            store_part(0, c, col, n, dg(ob[...], wo[:, pl.ds(col, n)], 1, 0))
            return 0

        lax.fori_loop(0, dm // n, proj, 0)
        c_pair(1, c).start()

    def stage_MU(c):
        @pl.when(c == 0)
        def _():
            for w in w2:
                w.wait()
            dys_ld.wait()

        ld_nm(c).wait()
        ld_dy(c).wait()
        n = tile_of(ff, 1536)

        def up(t, _):
            col = pl.ds(pl.multiple_of(t * n, n), n)
            pre = dg(nb[...], wu[:, col], 1, 0)
            dh = dg(dyb[...], wd[col], 1, 1)
            act, der = gelu_both(pre)
            hb_[:, col] = act.astype(BF)
            dpb[:, col] = (dh.astype(BF).astype(F32) * der).astype(BF)
            return 0

        lax.fori_loop(0, ff // n, up, 0)
        st_h(c).start()
        st_dp(c).start()

        @pl.when(c + 1 < nseq)
        def _():
            ld_dy(c + 1).start()

    m = tile_of(dm, 3072)

    def stage_MD(c):
        def down(t, _):
            col = pl.multiple_of(t * m, m)
            store_part(1, c, col, m, dg(dpb[...], wu[pl.ds(col, m)], 1, 1))
            return 0

        lax.fori_loop(0, dm // m, down, 0)
        c_pair(3, c).start()

    def stage_MY(c):
        @pl.when(c > 0)
        def _():
            st_py(c - 1).wait()

        def outp(t, _):
            col = pl.multiple_of(t * m, m)
            pyb[:, pl.ds(col, m)] = dg(hb_[...], wd[:, pl.ds(col, m)], 1, 0).astype(BF)
            return 0

        lax.fori_loop(0, dm // m, outp, 0)
        st_py(c).start()

    def stage_B2(c):
        ld_q(c).start()
        ld_g(c).wait()
        obt[...] = dg(wo[...], gb[...], 1, 1).astype(BF)
        ld_q(c).wait()

        def head(hd, _):
            qt, kt, vt, p = probs_t(qb2, hd)
            do = obt[pl.ds(pl.multiple_of(hd * e, e), e)]
            dqt[pl.ds(pl.multiple_of(2 * he + hd * e, e), e)] = dg(do, p.astype(BF), 1, 1).astype(BF)
            dpr = dg(vt, do, 0, 0).astype(BF).astype(F32)
            ds = p * (dpr - jnp.sum(dpr * p, axis=0, keepdims=True))
            ds = (ds * scale).astype(BF)
            dqt[pl.ds(pl.multiple_of(hd * e, e), e)] = dg(kt, ds, 1, 0).astype(BF)
            dqt[pl.ds(pl.multiple_of(he + hd * e, e), e)] = dg(qt, ds, 1, 1).astype(BF)
            return 0

        lax.fori_loop(0, heads, head, 0, unroll=2)
        tr = tile_of(3 * he, 128)
        for t in range(3 * he // tr):
            dqb[:, t * tr:(t + 1) * tr] = dqt[t * tr:(t + 1) * tr].T
        st_dq(c).start()
        n = tile_of(dm, 3072)

        def proj(t, _):
            col = pl.multiple_of(t * n, n)
            store_part(0, c, col, n, dg(dqb[...], wqkv[:, pl.ds(col, n)], 1, 0))
            return 0

        lax.fori_loop(0, dm // n, proj, 0)
        c_pair(4, c).start()

    def y_loads(c):
        s = c % SLOTS

        cps = []
        for b in range(CHIPS):
            ch = (chip + 1 + b) % CHIPS
            for k, (co, t) in enumerate(((1 - core, SLOTS), (core, s))):
                src = py_o.at[pl.ds(pl.multiple_of(c * slen + co * half + ch * blk, blk), blk)]
                cps.append(pltpu.make_async_copy(src, S.at[1, t, pl.ds(b * blk, blk)], ysem.at[k, b]))
        return cps

    def stage_YL(c):
        @pl.when(c == nseq - 1)
        def _():
            st_py(c).wait()

        for cp in y_loads(c):
            cp.start()

    def stage_YS(c):
        for cp in y_loads(c):
            cp.wait()
        c_pair(5, c).start()

    kh = tok // 2
    gemms = []
    for lhs, rhs, res in ((nm_o, dp_o, dwu_o), (h_o, dyf, dwd_o), (dq_o, a_o, dwq_o), (o_o, g_o, dwo_o)):
        for cb in range(rhs.shape[1] // ff):
            gemms.append((lhs, rhs, res, lhs.shape[1] // he, cb * ff))
    first = [sum(g[3] for g in gemms[:p]) for p in range(len(gemms) + 1)]
    tiles = first[-1]

    def a_buf(b, k):
        return wd.at[pl.ds(0, kh), pl.ds(pl.multiple_of((2 * b + k) * he, he), he)]

    def b_parts(p):
        if p % 2 == 0:
            return [(0, kh, wu.at[pl.ds(0, kh)]), (kh, kh, wu.at[pl.ds(kh, kh)])]
        q = kh // 2
        return [(0, kh, wd.at[pl.ds(0, kh), pl.ds(ff, ff)]), (kh, q, wd.at[pl.ds(kh, q), pl.ds(0, ff)]),
                (kh + q, q, wd.at[pl.ds(kh, q), pl.ds(ff, ff)])]

    def o_buf(b):
        return wu.at[pl.ds(pl.multiple_of(tok + b * he, math.gcd(tok, he)), he)]

    def a_load(p, w, k):
        col = pl.multiple_of((w - first[p]) * he, he)
        return pltpu.make_async_copy(gemms[p][0].at[pl.ds(k * kh, kh), pl.ds(col, he)], a_buf(w % 2, k), wsem.at[k, w % 2])

    def b_loads(p):
        return [pltpu.make_async_copy(gemms[p][1].at[pl.ds(t, n), pl.ds(gemms[p][4], ff)], m, wsem.at[3 + q, p % 2])
                for q, (t, n, m) in enumerate(b_parts(p))]

    def o_store(p, w):
        row = pl.multiple_of((w - first[p]) * he, he)
        return pltpu.make_async_copy(o_buf(w % 2), gemms[p][2].at[pl.ds(row, he), pl.ds(gemms[p][4], ff)], wsem.at[2, w % 2])

    def in_gemm(p, w):
        return (w >= first[p]) & (w < first[p + 1])

    def start_a(w):
        for p in range(len(gemms)):
            @pl.when(in_gemm(p, w))
            def _():
                for k in (0, 1):
                    a_load(p, w, k).start()

    def tile(w):
        for k in (0, 1):
            a_load(0, w % 2, k).wait()
        start_a(w + 1)
        for p in range(len(gemms)):
            @pl.when(w == first[p])
            def _():
                for cp in b_loads(p):
                    cp.wait()
                if p + 1 < len(gemms):
                    for cp in b_loads(p + 1):
                        cp.start()

        @pl.when(w >= 2)
        def _():
            o_store(0, w % 2).wait()

        n = tile_of(ff, 512)
        for odd in (0, 1):
            sel = functools.reduce(lambda u, v: u | v, [in_gemm(p, w) for p in range(len(gemms)) if p % 2 == odd])

            @pl.when(sel)
            def _():
                for j in range(ff // n):
                    acc = None
                    for t0, nt, m in b_parts(odd):
                        lhs = a_buf(w % 2, t0 // kh)[pl.ds(t0 % kh, nt)]
                        t = dg(lhs, m[:, pl.ds(j * n, n)], 0, 0)
                        acc = t if acc is None else acc + t
                    o_buf(w % 2)[:, pl.ds(j * n, n)] = acc.astype(BF)

        for p in range(len(gemms)):
            @pl.when(in_gemm(p, w))
            def _():
                o_store(p, w).start()

    def stage_WG(c):
        def one(j, _):
            tile(c * TILES + j)
            return 0

        lax.fori_loop(0, TILES, one, 0)

    def stage_WP(c):
        @pl.when(c == nseq - 1)
        def _():
            start_a(0)
            for cp in b_loads(0):
                cp.start()

    ld_x(0).start()
    for t in (0, 1):
        ld_wqkv(t).start()
    ld_wo.start()
    barrier = pltpu.get_barrier_semaphore()
    for k in range(1, tpn):
        pl.semaphore_signal(barrier, inc=1, device_id={'tp': (tp + k) % tpn}, device_id_type=MESH)
    dgb[...] = jnp.zeros_like(dgb)
    ld_x(0).wait()
    norm_rows()
    pl.semaphore_wait(barrier, tpn - 1)

    run = {'F1': stage_F1, 'MU': stage_MU, 'MD': stage_MD, 'MY': stage_MY, 'B2': stage_B2,
           'YL': stage_YL, 'YS': stage_YS, 'WG': stage_WG, 'WP': stage_WP}
    hops = {'a': stage_a, 'b': stage_b, 'c': stage_c, 'd': stage_d, 'e': stage_e, 'f': stage_f}
    order = ORDER

    def count(name):
        return tiles // TILES if name == 'WG' else nseq

    def step(i, _):
        for name, lag in order:
            c = i - lag

            @pl.when((c >= 0) & (c < count(name)))
            def _():
                if name in run:
                    run[name](c)
                else:
                    hops[name[0]](int(name[1]), c)
        return 0

    lax.fori_loop(0, max(count(n) + l for n, l in order), step, 0)

    ys = [lc(xm.at[pl.ds(k * nseq // 2, nseq // 2)], r, (0, 18)[k]) for k, r in enumerate((ya_o, yb_o))]
    for cp in ys:
        cp.start()
    for b in (0, 1):
        o_store(0, b).wait()
    for k in range(1, tpn):
        c_gain(k).wait_recv()
    tot = dgs[0]
    for t in range(1, tpn):
        tot = tot + dgs[t]
    dgain_o[...] = tot
    for k in range(1, tpn):
        c_gain(k).wait_send()
    for cp in ys:
        cp.wait()


def mega(x, dy, wqkv, wo, wu, wd, ga, gm, heads):
    nseq, slen, dm = x.shape
    he, ff = wo.shape[0], wu.shape[1]
    half = slen // CORES
    blk = half // CHIPS
    hb = blk // 2
    tok = nseq * slen

    def arr(*shape):
        return jax.ShapeDtypeStruct(shape, BF)

    act = arr(tok, dm)
    outs = (arr(nseq // 2, blk, dm), arr(nseq // 2, blk, dm), act, arr(3 * he, dm), arr(he, dm), arr(dm, ff), arr(ff, dm), act, act, act, arr(tok, he),
            arr(nseq, 3 * he, slen), arr(tok, ff), arr(tok, ff), arr(tok, 3 * he), act, jax.ShapeDtypeStruct((2, dm), F32))
    hbm = pl.BlockSpec(memory_space=pl.ANY)
    vm = pl.BlockSpec(memory_space=pltpu.VMEM)
    V = pltpu.VMEM
    scratch = [
        V(wqkv.shape, BF), V(wo.shape, BF), V(wu.shape, BF), V(wd.shape, BF),
        V((2, SLOTS + 1, half, dm), BF), V((2, PAIRS, half, dm), BF),
        V((2, SLOTS, 2, blk, dm), BF), V((2, SLOTS, 2, hb, dm), BF),
        V((slen, dm), BF), V((slen, dm), BF), V((slen, dm), BF), V((slen, dm), BF), V((slen, dm), BF),
        V((3 * he, slen), BF), V((3 * he, slen), BF), V((slen, 3 * he), BF), V((3 * he, slen), BF),
        V((slen, he), BF), V((he, slen), BF), V((slen, ff), BF), V((slen, ff), BF), V((slen, dm), BF),
        V((nseq, blk, dm), BF), V((nseq, blk, dm), BF), V((nseq, blk, dm), BF), V((2, 2, blk, dm), BF), V((2, dm), F32),
        V((CHIPS * CORES, 2, dm), F32),
        pltpu.SemaphoreType.DMA((23,)), pltpu.SemaphoreType.DMA((6, 2)), pltpu.SemaphoreType.DMA((2, CHIPS * CORES)),
        pltpu.SemaphoreType.DMA((2, CHIPS)), pltpu.SemaphoreType.DMA((2,)),
        pltpu.SemaphoreType.DMA((2, 5 * SLOTS)), pltpu.SemaphoreType.DMA((2, 5 * SLOTS)),
        pltpu.SemaphoreType.DMA((2, 8 * nseq)), pltpu.SemaphoreType.DMA((2, 8 * nseq)),
    ]
    flops = 2 * nseq * slen * dm * (4 * he * 2 + ff * 4)
    return pl.pallas_call(
        functools.partial(body, heads),
        name='mega',
        out_shape=outs,
        in_specs=[hbm] * 7 + [vm] * 2,
        out_specs=(hbm,) * 16 + (vm,),
        scratch_shapes=scratch,
        compiler_params=pltpu.CompilerParams(collective_id=0, has_side_effects=True, vmem_limit_bytes=VMEM_BYTES),
        cost_estimate=pl.CostEstimate(flops=flops, bytes_accessed=12 * nseq * slen * dm * 2, transcendentals=0),
    )(x, dy, dy.reshape(tok, dm), wqkv, wo, wu, wd, ga, gm)


def copied(arrays):
    n = len(arrays)
    cuts = []
    for a, v in enumerate(arrays):
        rows = tile_of(v.shape[0], 256 * 3072 // v.shape[1])
        cuts += [(a, r, rows) for r in range(0, v.shape[0], rows)]

    def move(*refs):
        src, dst, buf, isem, osem = refs[:n], refs[n:2 * n], refs[2 * n:3 * n], refs[-2], refs[-1]
        into = [pltpu.make_async_copy(src[a].at[pl.ds(r, m)], buf[a].at[pl.ds(r, m)], isem.at[k]) for k, (a, r, m) in enumerate(cuts)]
        out = [pltpu.make_async_copy(buf[a].at[pl.ds(r, m)], dst[a].at[pl.ds(r, m)], osem.at[k]) for k, (a, r, m) in enumerate(cuts)]
        for cp in into:
            cp.start()
        for k in range(len(cuts)):
            into[k].wait()
            out[k].start()
        for cp in out:
            cp.wait()

    hbm = pl.BlockSpec(memory_space=pl.ANY)
    size = sum(v.size for v in arrays)
    return pl.pallas_call(
        move, in_specs=[hbm] * n, out_specs=(hbm,) * n,
        out_shape=tuple(jax.ShapeDtypeStruct(v.shape, v.dtype) for v in arrays),
        scratch_shapes=[pltpu.VMEM(v.shape, v.dtype) for v in arrays] + [pltpu.SemaphoreType.DMA((len(cuts),))] * 2,
        compiler_params=pltpu.CompilerParams(vmem_limit_bytes=VMEM_BYTES),
        cost_estimate=pl.CostEstimate(flops=size * 500, bytes_accessed=4 * size, transcendentals=0))(*arrays)


def placed(out, pieces, shape, at_of):
    n = len(pieces)
    given = [] if out is None else [out]

    def put(*refs):
        src, dst = refs[:n], refs[n + len(given)]
        buf, isem, osem = refs[n + len(given) + 1:-2], refs[-2], refs[-1]
        tp = lax.axis_index('tp')
        at = at_of(tp // CORES, tp % CORES)
        into = [pltpu.make_async_copy(src[k], buf[k], isem.at[k]) for k in range(n)]
        outc = [pltpu.make_async_copy(
            buf[k], dst.at[pl.ds(at[k][0], p.shape[0]), pl.ds(pl.multiple_of(at[k][1], p.shape[1]), p.shape[1])], osem.at[k])
            for k, p in enumerate(pieces)]
        for cp in into:
            cp.start()
        for k in range(n):
            into[k].wait()
            outc[k].start()
        for cp in outc:
            cp.wait()

    hbm = pl.BlockSpec(memory_space=pl.ANY)
    return pl.pallas_call(
        put, in_specs=[hbm] * (n + len(given)), out_specs=hbm, out_shape=jax.ShapeDtypeStruct(shape, BF),
        scratch_shapes=[pltpu.VMEM(p.shape, p.dtype) for p in pieces] + [pltpu.SemaphoreType.DMA((n,))] * 2,
        input_output_aliases={n: 0} if given else {},
        compiler_params=pltpu.CompilerParams(vmem_limit_bytes=VMEM_BYTES),
        cost_estimate=pl.CostEstimate(flops=sum(p.size for p in pieces) * 500, bytes_accessed=0, transcendentals=0),
    )(*pieces, *given)


def solution(mesh):
    tpn = mesh.shape['tp']
    assert tpn == CHIPS * CORES

    def hop(v, chips_by, cores_by):
        perm = []
        for t in range(tpn):
            ch, co = t // CORES, t % CORES
            perm.append((t, ((ch + chips_by) % CHIPS) * CORES + (co + cores_by) % CORES))
        return lax.ppermute(v, 'tp', perm)

    def gather(va, vb):
        ns, blk, dm = va.shape
        half = blk * CHIPS
        la, rb = hop(va, 1, 0), hop(vb, -1, 0)
        lb, ra = hop(vb, 1, 0), hop(va, -1, 0)
        oa, ob = hop(la, 1, 0), hop(rb, -1, 0)
        near = [va, vb, la, lb, ra, rb]
        near += [hop(p, 0, 1) for p in near]
        far = [oa, ob, hop(oa, 0, 1), hop(ob, 0, 1)]

        def near_at(chip, core):
            chips = (chip, (chip + CHIPS - 1) % CHIPS, (chip + 1) % CHIPS)
            return [(k * ns, co * half + ch * blk) for co in (core, 1 - core) for ch in chips for k in (0, 1)]

        def far_at(chip, core):
            o = ((chip + 2) % CHIPS) * blk
            return [(k * ns, co * half + o) for co in (core, 1 - core) for k in (0, 1)]

        out = placed(None, near, (2 * ns, half * CORES, dm), near_at)
        return placed(out, far, out.shape, far_at)

    def step(x_in, gain_attn, w_qkv, w_out, gain_mlp, w_up, w_down, dy_out):
        heads, e = w_qkv.shape[3:]
        dm = x_in.shape[2]
        he = heads * e
        wqkv = jnp.transpose(w_qkv[0], (1, 2, 3, 0)).reshape(3 * he, dm)
        wo = w_out[0].reshape(he, dm)
        out = mega(x_in, dy_out, wqkv, wo, w_up[0], w_down[0], gain_attn, gain_mlp, heads)
        ya, yb, dx, dwq, dwo, dwu, dwd = out[:7]
        dgain = out[-1]
        dx, dwu, dwo = copied((dx, dwu, dwo))
        dwd, dwq = copied((dwd, dwq))
        y = gather(ya, yb)
        dwq = jnp.transpose(dwq.reshape(3, heads, e, dm), (3, 0, 1, 2))
        return (y, dx.reshape(x_in.shape), dgain[0:1], dwq[None], dwo.reshape(1, heads, e, dm),
                dgain[1:2], dwu[None], dwd[None])

    act = P('dp', None, None)
    in_specs = (act, P(None, None), P(None, None, None, 'tp', None), P(None, 'tp', None, None), P(None, None),
                P(None, None, 'tp'), P(None, 'tp', None), act)
    out_specs = (act, act, P('dp', None), P('dp', None, None, 'tp', None), P('dp', 'tp', None, None), P('dp', None),
                 P('dp', None, 'tp'), P('dp', 'tp', None))
    step = jax.shard_map(step, mesh=mesh, in_specs=in_specs, out_specs=out_specs, check_vma=False)
    return step
```

```python
import functools
import math

import jax
import jax.numpy as jnp
from jax import lax
from jax.experimental import pallas as pl
from jax.experimental.pallas import tpu as pltpu
from jax.sharding import PartitionSpec as P


LN_EPS = 1e-5
CORES = 2
CHIPS = 4
BF = jnp.bfloat16
F32 = jnp.float32
MESH = pl.DeviceIdType.MESH
VMEM_BYTES = 67043328
GELU_C = 0.7978845608028654
GELU_K = 0.044715
SLOTS = 3
PAIRS = 2
TILES = 2

ORDER = (
    ('a3', 9), ('b5', 20), ('a1', 1), ('a5', 19), ('F1', 0), ('d4', 20), ('MU', 8), ('f1', 7), ('c4', 18),
    ('YL', 18), ('d1', 4), ('B2', 16), ('WP', 9), ('b4', 17), ('d3', 11), ('f3', 15), ('YS', 18), ('a4', 16),
    ('c3', 10), ('WG', 16), ('e1', 5), ('MD', 8), ('c1', 2), ('MY', 8), ('e4', 21), ('c5', 20), ('e3', 14),
    ('b3', 9), ('f4', 22), ('b1', 1),
)


def dg(a, b, ca, cb):
    return lax.dot_general(a, b, (((ca,), (cb,)), ((), ())), preferred_element_type=F32)


def ln_parts(z):
    mu = jnp.mean(z, axis=-1, keepdims=True)
    c = z - mu
    var = jnp.mean(c * c, axis=-1, keepdims=True)
    r = lax.rsqrt(var + LN_EPS)
    return c * r, r


def ln_bwd(z, gain, d):
    xhat, r = ln_parts(z)
    h = d * gain
    m1 = jnp.mean(h, axis=-1, keepdims=True)
    m2 = jnp.mean(h * xhat, axis=-1, keepdims=True)
    return r * (h - m1 - xhat * m2), jnp.sum(d * xhat, axis=0, keepdims=True)


def gelu_both(z):
    z2 = z * z
    t = jnp.tanh(GELU_C * (z + GELU_K * (z2 * z)))
    cdf = 0.5 * (1.0 + t)
    d = cdf + z * (0.5 * (1.0 - t * t)) * (GELU_C * (1.0 + (3.0 * GELU_K) * z2))
    return z * cdf, d


def tile_of(n, want):
    t = min(n, want)
    while n % t:
        t //= 2
    return t


def body(heads, x, dy, dyf, wqkv_h, wo_h, wu_h, wd_h, ga, gm,
         ya_o, yb_o, dx_o, dwq_o, dwo_o, dwu_o, dwd_o, nm_o, g_o, a_o, o_o, qkv_o, h_o, dp_o, dq_o, py_o, dgain_o,
         wqkv, wo, wu, wd, S, RD, R1, R2, xb, ab, nb, dyb, gb, qb, qb2, dqb, dqt, ob, obt, hb_, dpb, pyb,
         xs, xm, gs, own, dgb, dgs, lsem, wsem, dsem, ysem, qsem, ssem1, rsem1, ssem, rsem):
    nseq, slen, dm = x.shape
    tok = nseq * slen
    half = slen // CORES
    blk = half // CHIPS
    hb = blk // 2
    he = wo.shape[0]
    e = he // heads
    ff = wu.shape[1]
    scale = e ** -0.5
    tpn = CHIPS * CORES
    tp = lax.axis_index('tp')
    chip = tp // CORES
    core = tp % CORES
    sib = chip * CORES + (1 - core)
    rchip = (chip + 1) % CHIPS
    lchip = (chip + CHIPS - 1) % CHIPS
    ochip = (chip + 2) % CHIPS
    right = rchip * CORES + core
    left = lchip * CORES + core

    def seq(c):
        return pl.ds(pl.multiple_of(c * slen, slen), slen)

    def off(ch, co):
        return pl.multiple_of(co * half + ch * blk, blk)

    myoff = off(chip, core)

    def lc(src, dst, k):
        return pltpu.make_async_copy(src, dst, lsem.at[k])

    qt = tile_of(3 * wo.shape[0], 3 * wo.shape[0] // 2)

    def ld_wqkv(t):
        r = pl.ds(pl.multiple_of(t * qt, qt), qt)
        return pltpu.make_async_copy(wqkv_h.at[r], wqkv.at[r], qsem.at[t])

    ld_wo = lc(wo_h, wo, 1)
    w2 = (lc(wu_h, wu, 2), lc(wd_h, wd, 3))

    def ld_x(c):
        return lc(x.at[c], xb, 4)

    def ld_dy(c):
        return lc(dy.at[c], dyb, 5)

    def ld_nm(c):
        return lc(nm_o.at[seq(c)], nb, 6)

    def ld_g(c):
        return lc(g_o.at[seq(c)], gb, 7)

    def ld_q(c):
        return lc(qkv_o.at[c], qb2, 8)

    def st_a(c):
        return lc(ab, a_o.at[seq(c)], 9)

    def st_q(c):
        return lc(qb, qkv_o.at[c], 10)

    def st_o(c):
        return lc(ob, o_o.at[seq(c)], 11)

    def st_h(c):
        return lc(hb_, h_o.at[seq(c)], 12)

    def st_dp(c):
        return lc(dpb, dp_o.at[seq(c)], 13)

    def st_py(c):
        return lc(pyb, py_o.at[seq(c)], 14)

    def st_dq(c):
        return lc(dqb, dq_o.at[seq(c)], 15)

    xs_ld = lc(x.at[:, pl.ds(myoff, blk), :], xs, 16)
    dys_ld = lc(dy.at[:, pl.ds(myoff, blk), :], gs, 17)
    out_ref = {1: nm_o, 3: g_o, 4: dx_o}
    fset = {1: 0, 3: 1, 4: 0, 5: 1}

    def out_rows(fl, c, o, n):
        return out_ref[fl].at[pl.ds(pl.multiple_of(c * slen + o, n), n)]

    def st_own(fl, c):
        return lc(own.at[fset[fl], c % 2], out_rows(fl, c, myoff, blk), 19 + fset[fl] * 2 + c % 2)

    def rc(kind, fl, c, src, dst, dev):
        f = fset[fl]
        if kind < 5:
            send, recv = ssem1.at[f, kind * SLOTS + c], rsem1.at[f, kind * SLOTS + c]
        else:
            send, recv = (m.at[f, (kind - 5) * nseq + c] for m in (ssem, rsem))
        return pltpu.make_async_remote_copy(
            src_ref=src, dst_ref=dst, send_sem=send, recv_sem=recv,
            device_id={'tp': dev}, device_id_type=MESH)

    def c_pair(fl, c):
        f = fset[fl]
        return rc(0, fl, c % PAIRS, S.at[f, SLOTS], RD.at[f, c % PAIRS], sib)

    def c_first(fl, c, d):
        f, s = fset[fl], c % SLOTS
        src = S.at[f, s, pl.ds(blk + hb if d else hb, blk)]
        return rc(1 + d, fl, c % SLOTS, src, R1.at[f, s, d], left if d else right)

    def c_second(fl, c, d):
        f, s = fset[fl], c % SLOTS
        src = S.at[f, s, pl.ds(2 * blk + hb if d else 0, hb)]
        return rc(3 + d, fl, c % SLOTS, src, R2.at[f, s, d], left if d else right)

    def c_own(fl, c, d):
        dev = (right, left, sib)[d]
        return rc(5 + d, fl, c, own.at[fset[fl], c % 2], out_rows(fl, c, myoff, blk), dev)

    def c_fwd(fl, c, d):
        r = out_rows(fl, c, off(rchip if d else lchip, core) + d * hb, hb)
        return rc(8 + d, fl, c, r, r, left if d else right)

    def c_cross(fl, c, d):
        r = out_rows(fl, c, off((lchip, rchip, ochip)[d], core), blk)
        return rc(10 + d, fl, c, r, r, sib)

    def c_gain(k):
        return pltpu.make_async_remote_copy(
            src_ref=dgb, dst_ref=dgs.at[tp], send_sem=dsem.at[0, k], recv_sem=dsem.at[1, k],
            device_id={'tp': (tp + k) % tpn}, device_id_type=MESH)

    def store_part(f, c, col, n, val):
        v = val.astype(BF)
        s = c % SLOTS
        i0 = s * (1 - core) + SLOTS * core
        i1 = s * core + SLOTS * (1 - core)
        for b in range(CHIPS):
            r = pl.ds(pl.multiple_of(((b + CHIPS - 1 - chip) % CHIPS) * blk, blk), blk)
            S[f, i0, r, pl.ds(col, n)] = v[b * blk:(b + 1) * blk]
            S[f, i1, r, pl.ds(col, n)] = v[half + b * blk:half + (b + 1) * blk]

    def stage_a(fl, c):
        f, s = fset[fl], c % SLOTS
        c_pair(fl, c).wait_recv()
        c_pair(fl, c).wait_send()
        for st in {1: (st_a, st_q, st_o), 3: (st_h, st_dp), 4: (st_dq,), 5: ()}[fl]:
            st(c).wait()

        def add(t, _):
            r = pl.ds(pl.multiple_of(t * hb, hb), hb)
            S[f, s, r] = S[f, s, r] + RD[f, c % PAIRS, r]
            return 0

        lax.fori_loop(0, half // hb, add, 0, unroll=8)
        for d in (0, 1):
            c_first(fl, c, d).start()

    def stage_b(fl, c):
        f, s = fset[fl], c % SLOTS
        for d in (0, 1):
            c_first(fl, c, d).wait_recv()
        for d in (0, 1):
            o = pl.ds(2 * blk + hb if d else 0, hb)
            S[f, s, o] = (S[f, s, o].astype(F32) + R1[f, s, d, pl.ds(0 if d else hb, hb)].astype(F32)).astype(BF)
            c_second(fl, c, d).start()

    def stage_c(fl, c):
        f, s = fset[fl], c % SLOTS
        for d in (0, 1):
            c_second(fl, c, d).wait_recv()

        for k in (0, 1):
            q = pl.ds(k * hb, hb)
            o = pl.ds(3 * blk + k * hb, hb)
            tot = S[f, s, o].astype(F32) + R1[f, s, 1 - k, pl.ds(0 if k else hb, hb)].astype(F32) + R2[f, s, k].astype(F32)
            if fl == 1:
                if k == 0:
                    @pl.when(c == 0)
                    def _():
                        xs_ld.wait()

                z = (xs[c, q].astype(F32) + tot).astype(BF)
                xm[c, q] = z
                xh, _ = ln_parts(z.astype(F32))
                own[f, c % 2, q] = (xh * gm[...]).astype(BF)
            elif fl == 3:
                dr, dgn = ln_bwd(xm[c, q].astype(F32), gm[...], tot)
                v = (gs[c, q].astype(F32) + dr).astype(BF)
                gs[c, q] = v
                own[f, c % 2, q] = v
                dgb[1:2] += dgn
            elif fl == 5:
                xm[c, q] = (xm[c, q].astype(F32) + tot).astype(BF)
            else:
                dr, dgn = ln_bwd(xs[c, q].astype(F32), ga[...], tot)
                own[f, c % 2, q] = (gs[c, q].astype(F32) + dr).astype(BF)
                dgb[0:1] += dgn
        if fl != 5:
            for d in (0, 1, 2):
                c_own(fl, c, d).start()
            st_own(fl, c).start()
        for d in (0, 1):
            c_first(fl, c, d).wait_send()
            c_second(fl, c, d).wait_send()
        if fl == 4:
            @pl.when(c == nseq - 1)
            def _():
                dgs[tp] = dgb[...]
                for k in range(1, tpn):
                    c_gain(k).start()

    def stage_d(fl, c):
        for d in (1, 0):
            c_own(fl, c, 1 - d).wait_recv()
            c_fwd(fl, c, 1 - d).start()
        for d in (0, 1):
            c_cross(fl, c, d).start()
        for d in (0, 1, 2):
            c_own(fl, c, d).wait_send()
        st_own(fl, c).wait()

    def stage_e(fl, c):
        for d in (0, 1):
            c_fwd(fl, c, d).wait_recv()
        c_cross(fl, c, 2).start()

    def stage_f(fl, c):
        c_own(fl, c, 2).wait_recv()
        for d in (0, 1, 2):
            c_cross(fl, c, d).wait_recv()
        for d in (0, 1):
            c_fwd(fl, c, d).wait_send()
        for d in (0, 1, 2):
            c_cross(fl, c, d).wait_send()
        if fl == 1:
            ld_nm(c).start()
        if fl == 3:
            ld_g(c).start()

    def probs_t(q_ref, hd):
        qt = q_ref[pl.ds(pl.multiple_of(hd * e, e), e)]
        kt = q_ref[pl.ds(pl.multiple_of(he + hd * e, e), e)]
        vt = q_ref[pl.ds(pl.multiple_of(2 * he + hd * e, e), e)]
        s = dg(kt, qt, 0, 0) * scale
        keep = lax.broadcasted_iota(jnp.int32, (slen, slen), 0) <= lax.broadcasted_iota(jnp.int32, (slen, slen), 1)
        s = jnp.where(keep, s, -1e30)
        ex = jnp.exp(s - jnp.max(s, axis=0, keepdims=True))
        return qt, kt, vt, ex * (1.0 / jnp.sum(ex, axis=0, keepdims=True))

    def norm_rows():
        def ln(t, _):
            r = pl.ds(pl.multiple_of(t * hb, hb), hb)
            xh, _ = ln_parts(xb[r].astype(F32))
            ab[r] = (xh * ga[...]).astype(BF)
            return 0

        lax.fori_loop(0, slen // hb, ln, 0, unroll=8)

    def stage_F1(c):
        @pl.when(c > 0)
        def _():
            ld_x(c).wait()
            norm_rows()

        st_a(c).start()

        @pl.when(c + 1 < nseq)
        def _():
            ld_x(c + 1).start()

        def qkv(t, _):
            @pl.when(c == 0)
            def _():
                ld_wqkv(t).wait()

            r = pl.ds(pl.multiple_of(t * qt, qt), qt)
            qb[r] = dg(wqkv[r], ab[...], 1, 1).astype(BF)
            return 0

        lax.fori_loop(0, 3 * he // qt, qkv, 0)
        st_q(c).start()

        def head(hd, _):
            _, _, vt, p = probs_t(qb, hd)
            obt[pl.ds(pl.multiple_of(hd * e, e), e)] = dg(vt, p.astype(BF), 1, 0).astype(BF)
            return 0

        lax.fori_loop(0, heads, head, 0, unroll=True)
        tr = tile_of(he, 128)
        for t in range(he // tr):
            ob[:, t * tr:(t + 1) * tr] = obt[t * tr:(t + 1) * tr].T
        st_o(c).start()
        n = tile_of(dm, 3072)

        @pl.when(c == 0)
        def _():
            ld_wo.wait()
            for w in w2:
                w.start()
            for w in (xs_ld, dys_ld, ld_dy(0)):
                w.start()

        def proj(t, _):
            col = pl.multiple_of(t * n, n)
            store_part(0, c, col, n, dg(ob[...], wo[:, pl.ds(col, n)], 1, 0))
            return 0

        lax.fori_loop(0, dm // n, proj, 0)
        c_pair(1, c).start()

    def stage_MU(c):
        @pl.when(c == 0)
        def _():
            for w in w2:
                w.wait()
            dys_ld.wait()

        ld_nm(c).wait()
        ld_dy(c).wait()
        n = tile_of(ff, 1536)

        def up(t, _):
            col = pl.ds(pl.multiple_of(t * n, n), n)
            pre = dg(nb[...], wu[:, col], 1, 0)
            dh = dg(dyb[...], wd[col], 1, 1)
            act, der = gelu_both(pre)
            hb_[:, col] = act.astype(BF)
            dpb[:, col] = (dh.astype(BF).astype(F32) * der).astype(BF)
            return 0

        lax.fori_loop(0, ff // n, up, 0)
        st_h(c).start()
        st_dp(c).start()

        @pl.when(c + 1 < nseq)
        def _():
            ld_dy(c + 1).start()

    m = tile_of(dm, 3072)

    def stage_MD(c):
        def down(t, _):
            col = pl.multiple_of(t * m, m)
            store_part(1, c, col, m, dg(dpb[...], wu[pl.ds(col, m)], 1, 1))
            return 0

        lax.fori_loop(0, dm // m, down, 0)
        c_pair(3, c).start()

    def stage_MY(c):
        @pl.when(c > 0)
        def _():
            st_py(c - 1).wait()

        def outp(t, _):
            col = pl.multiple_of(t * m, m)
            pyb[:, pl.ds(col, m)] = dg(hb_[...], wd[:, pl.ds(col, m)], 1, 0).astype(BF)
            return 0

        lax.fori_loop(0, dm // m, outp, 0)
        st_py(c).start()

    def stage_B2(c):
        ld_q(c).start()
        ld_g(c).wait()
        obt[...] = dg(wo[...], gb[...], 1, 1).astype(BF)
        ld_q(c).wait()

        def head(hd, _):
            qt, kt, vt, p = probs_t(qb2, hd)
            do = obt[pl.ds(pl.multiple_of(hd * e, e), e)]
            dqt[pl.ds(pl.multiple_of(2 * he + hd * e, e), e)] = dg(do, p.astype(BF), 1, 1).astype(BF)
            dpr = dg(vt, do, 0, 0).astype(BF).astype(F32)
            ds = p * (dpr - jnp.sum(dpr * p, axis=0, keepdims=True))
            ds = (ds * scale).astype(BF)
            dqt[pl.ds(pl.multiple_of(hd * e, e), e)] = dg(kt, ds, 1, 0).astype(BF)
            dqt[pl.ds(pl.multiple_of(he + hd * e, e), e)] = dg(qt, ds, 1, 1).astype(BF)
            return 0

        lax.fori_loop(0, heads, head, 0, unroll=2)
        tr = tile_of(3 * he, 128)
        for t in range(3 * he // tr):
            dqb[:, t * tr:(t + 1) * tr] = dqt[t * tr:(t + 1) * tr].T
        st_dq(c).start()
        n = tile_of(dm, 3072)

        def proj(t, _):
            col = pl.multiple_of(t * n, n)
            store_part(0, c, col, n, dg(dqb[...], wqkv[:, pl.ds(col, n)], 1, 0))
            return 0

        lax.fori_loop(0, dm // n, proj, 0)
        c_pair(4, c).start()

    def y_loads(c):
        s = c % SLOTS

        cps = []
        for b in range(CHIPS):
            ch = (chip + 1 + b) % CHIPS
            for k, (co, t) in enumerate(((1 - core, SLOTS), (core, s))):
                src = py_o.at[pl.ds(pl.multiple_of(c * slen + co * half + ch * blk, blk), blk)]
                cps.append(pltpu.make_async_copy(src, S.at[1, t, pl.ds(b * blk, blk)], ysem.at[k, b]))
        return cps

    def stage_YL(c):
        @pl.when(c == nseq - 1)
        def _():
            st_py(c).wait()

        for cp in y_loads(c):
            cp.start()

    def stage_YS(c):
        for cp in y_loads(c):
            cp.wait()
        c_pair(5, c).start()

    kh = tok // 2
    gemms = []
    for lhs, rhs, res in ((nm_o, dp_o, dwu_o), (h_o, dyf, dwd_o), (dq_o, a_o, dwq_o), (o_o, g_o, dwo_o)):
        for cb in range(rhs.shape[1] // ff):
            gemms.append((lhs, rhs, res, lhs.shape[1] // he, cb * ff))
    first = [sum(g[3] for g in gemms[:p]) for p in range(len(gemms) + 1)]
    tiles = first[-1]

    def a_buf(b, k):
        return wd.at[pl.ds(0, kh), pl.ds(pl.multiple_of((2 * b + k) * he, he), he)]

    def b_parts(p):
        if p % 2 == 0:
            return [(0, kh, wu.at[pl.ds(0, kh)]), (kh, kh, wu.at[pl.ds(kh, kh)])]
        q = kh // 2
        return [(0, kh, wd.at[pl.ds(0, kh), pl.ds(ff, ff)]), (kh, q, wd.at[pl.ds(kh, q), pl.ds(0, ff)]),
                (kh + q, q, wd.at[pl.ds(kh, q), pl.ds(ff, ff)])]

    def o_buf(b):
        return wu.at[pl.ds(pl.multiple_of(tok + b * he, math.gcd(tok, he)), he)]

    def a_load(p, w, k):
        col = pl.multiple_of((w - first[p]) * he, he)
        return pltpu.make_async_copy(gemms[p][0].at[pl.ds(k * kh, kh), pl.ds(col, he)], a_buf(w % 2, k), wsem.at[k, w % 2])

    def b_loads(p):
        return [pltpu.make_async_copy(gemms[p][1].at[pl.ds(t, n), pl.ds(gemms[p][4], ff)], m, wsem.at[3 + q, p % 2])
                for q, (t, n, m) in enumerate(b_parts(p))]

    def o_store(p, w):
        row = pl.multiple_of((w - first[p]) * he, he)
        return pltpu.make_async_copy(o_buf(w % 2), gemms[p][2].at[pl.ds(row, he), pl.ds(gemms[p][4], ff)], wsem.at[2, w % 2])

    def in_gemm(p, w):
        return (w >= first[p]) & (w < first[p + 1])

    def start_a(w):
        for p in range(len(gemms)):
            @pl.when(in_gemm(p, w))
            def _():
                for k in (0, 1):
                    a_load(p, w, k).start()

    def tile(w):
        for k in (0, 1):
            a_load(0, w % 2, k).wait()
        start_a(w + 1)
        for p in range(len(gemms)):
            @pl.when(w == first[p])
            def _():
                for cp in b_loads(p):
                    cp.wait()
                if p + 1 < len(gemms):
                    for cp in b_loads(p + 1):
                        cp.start()

        @pl.when(w >= 2)
        def _():
            o_store(0, w % 2).wait()

        n = tile_of(ff, 512)
        for odd in (0, 1):
            sel = functools.reduce(lambda u, v: u | v, [in_gemm(p, w) for p in range(len(gemms)) if p % 2 == odd])

            @pl.when(sel)
            def _():
                for j in range(ff // n):
                    acc = None
                    for t0, nt, m in b_parts(odd):
                        lhs = a_buf(w % 2, t0 // kh)[pl.ds(t0 % kh, nt)]
                        t = dg(lhs, m[:, pl.ds(j * n, n)], 0, 0)
                        acc = t if acc is None else acc + t
                    o_buf(w % 2)[:, pl.ds(j * n, n)] = acc.astype(BF)

        for p in range(len(gemms)):
            @pl.when(in_gemm(p, w))
            def _():
                o_store(p, w).start()

    def stage_WG(c):
        def one(j, _):
            tile(c * TILES + j)
            return 0

        lax.fori_loop(0, TILES, one, 0)

    def stage_WP(c):
        @pl.when(c == nseq - 1)
        def _():
            start_a(0)
            for cp in b_loads(0):
                cp.start()

    ld_x(0).start()
    for t in (0, 1):
        ld_wqkv(t).start()
    ld_wo.start()
    barrier = pltpu.get_barrier_semaphore()
    for k in range(1, tpn):
        pl.semaphore_signal(barrier, inc=1, device_id={'tp': (tp + k) % tpn}, device_id_type=MESH)
    dgb[...] = jnp.zeros_like(dgb)
    ld_x(0).wait()
    norm_rows()
    pl.semaphore_wait(barrier, tpn - 1)

    run = {'F1': stage_F1, 'MU': stage_MU, 'MD': stage_MD, 'MY': stage_MY, 'B2': stage_B2,
           'YL': stage_YL, 'YS': stage_YS, 'WG': stage_WG, 'WP': stage_WP}
    hops = {'a': stage_a, 'b': stage_b, 'c': stage_c, 'd': stage_d, 'e': stage_e, 'f': stage_f}
    order = ORDER

    def count(name):
        return tiles // TILES if name == 'WG' else nseq

    def step(i, _):
        for name, lag in order:
            c = i - lag

            @pl.when((c >= 0) & (c < count(name)))
            def _():
                if name in run:
                    run[name](c)
                else:
                    hops[name[0]](int(name[1]), c)
        return 0

    lax.fori_loop(0, max(count(n) + l for n, l in order), step, 0)

    ys = [lc(xm.at[pl.ds(k * nseq // 2, nseq // 2)], r, (0, 18)[k]) for k, r in enumerate((ya_o, yb_o))]
    for cp in ys:
        cp.start()
    for b in (0, 1):
        o_store(0, b).wait()
    for k in range(1, tpn):
        c_gain(k).wait_recv()
    tot = dgs[0]
    for t in range(1, tpn):
        tot = tot + dgs[t]
    dgain_o[...] = tot
    for k in range(1, tpn):
        c_gain(k).wait_send()
    for cp in ys:
        cp.wait()


def mega(x, dy, wqkv, wo, wu, wd, ga, gm, heads):
    nseq, slen, dm = x.shape
    he, ff = wo.shape[0], wu.shape[1]
    half = slen // CORES
    blk = half // CHIPS
    hb = blk // 2
    tok = nseq * slen

    def arr(*shape):
        return jax.ShapeDtypeStruct(shape, BF)

    act = arr(tok, dm)
    outs = (arr(nseq // 2, blk, dm), arr(nseq // 2, blk, dm), act, arr(3 * he, dm), arr(he, dm), arr(dm, ff), arr(ff, dm), act, act, act, arr(tok, he),
            arr(nseq, 3 * he, slen), arr(tok, ff), arr(tok, ff), arr(tok, 3 * he), act, jax.ShapeDtypeStruct((2, dm), F32))
    hbm = pl.BlockSpec(memory_space=pl.ANY)
    vm = pl.BlockSpec(memory_space=pltpu.VMEM)
    V = pltpu.VMEM
    scratch = [
        V(wqkv.shape, BF), V(wo.shape, BF), V(wu.shape, BF), V(wd.shape, BF),
        V((2, SLOTS + 1, half, dm), BF), V((2, PAIRS, half, dm), BF),
        V((2, SLOTS, 2, blk, dm), BF), V((2, SLOTS, 2, hb, dm), BF),
        V((slen, dm), BF), V((slen, dm), BF), V((slen, dm), BF), V((slen, dm), BF), V((slen, dm), BF),
        V((3 * he, slen), BF), V((3 * he, slen), BF), V((slen, 3 * he), BF), V((3 * he, slen), BF),
        V((slen, he), BF), V((he, slen), BF), V((slen, ff), BF), V((slen, ff), BF), V((slen, dm), BF),
        V((nseq, blk, dm), BF), V((nseq, blk, dm), BF), V((nseq, blk, dm), BF), V((2, 2, blk, dm), BF), V((2, dm), F32),
        V((CHIPS * CORES, 2, dm), F32),
        pltpu.SemaphoreType.DMA((23,)), pltpu.SemaphoreType.DMA((6, 2)), pltpu.SemaphoreType.DMA((2, CHIPS * CORES)),
        pltpu.SemaphoreType.DMA((2, CHIPS)), pltpu.SemaphoreType.DMA((2,)),
        pltpu.SemaphoreType.DMA((2, 5 * SLOTS)), pltpu.SemaphoreType.DMA((2, 5 * SLOTS)),
        pltpu.SemaphoreType.DMA((2, 8 * nseq)), pltpu.SemaphoreType.DMA((2, 8 * nseq)),
    ]
    flops = 2 * nseq * slen * dm * (4 * he * 2 + ff * 4)
    return pl.pallas_call(
        functools.partial(body, heads),
        name='mega',
        out_shape=outs,
        in_specs=[hbm] * 7 + [vm] * 2,
        out_specs=(hbm,) * 16 + (vm,),
        scratch_shapes=scratch,
        compiler_params=pltpu.CompilerParams(collective_id=0, has_side_effects=True, vmem_limit_bytes=VMEM_BYTES),
        cost_estimate=pl.CostEstimate(flops=flops, bytes_accessed=12 * nseq * slen * dm * 2, transcendentals=0),
    )(x, dy, dy.reshape(tok, dm), wqkv, wo, wu, wd, ga, gm)


def copied(arrays):
    n = len(arrays)
    cuts = []
    for a, v in enumerate(arrays):
        rows = tile_of(v.shape[0], 256 * 3072 // v.shape[1])
        cuts += [(a, r, rows) for r in range(0, v.shape[0], rows)]

    def move(*refs):
        src, dst, buf, isem, osem = refs[:n], refs[n:2 * n], refs[2 * n:3 * n], refs[-2], refs[-1]
        into = [pltpu.make_async_copy(src[a].at[pl.ds(r, m)], buf[a].at[pl.ds(r, m)], isem.at[k]) for k, (a, r, m) in enumerate(cuts)]
        out = [pltpu.make_async_copy(buf[a].at[pl.ds(r, m)], dst[a].at[pl.ds(r, m)], osem.at[k]) for k, (a, r, m) in enumerate(cuts)]
        for cp in into:
            cp.start()
        for k in range(len(cuts)):
            into[k].wait()
            out[k].start()
        for cp in out:
            cp.wait()

    hbm = pl.BlockSpec(memory_space=pl.ANY)
    size = sum(v.size for v in arrays)
    return pl.pallas_call(
        move, in_specs=[hbm] * n, out_specs=(hbm,) * n,
        out_shape=tuple(jax.ShapeDtypeStruct(v.shape, v.dtype) for v in arrays),
        scratch_shapes=[pltpu.VMEM(v.shape, v.dtype) for v in arrays] + [pltpu.SemaphoreType.DMA((len(cuts),))] * 2,
        compiler_params=pltpu.CompilerParams(vmem_limit_bytes=VMEM_BYTES),
        cost_estimate=pl.CostEstimate(flops=size * 500, bytes_accessed=4 * size, transcendentals=0))(*arrays)


def placed(out, pieces, shape, at_of):
    n = len(pieces)
    given = [] if out is None else [out]

    def put(*refs):
        src, dst = refs[:n], refs[n + len(given)]
        buf, isem, osem = refs[n + len(given) + 1:-2], refs[-2], refs[-1]
        tp = lax.axis_index('tp')
        at = at_of(tp // CORES, tp % CORES)
        into = [pltpu.make_async_copy(src[k], buf[k], isem.at[k]) for k in range(n)]
        outc = [pltpu.make_async_copy(
            buf[k], dst.at[pl.ds(at[k][0], p.shape[0]), pl.ds(pl.multiple_of(at[k][1], p.shape[1]), p.shape[1])], osem.at[k])
            for k, p in enumerate(pieces)]
        for cp in into:
            cp.start()
        for k in range(n):
            into[k].wait()
            outc[k].start()
        for cp in outc:
            cp.wait()

    hbm = pl.BlockSpec(memory_space=pl.ANY)
    return pl.pallas_call(
        put, in_specs=[hbm] * (n + len(given)), out_specs=hbm, out_shape=jax.ShapeDtypeStruct(shape, BF),
        scratch_shapes=[pltpu.VMEM(p.shape, p.dtype) for p in pieces] + [pltpu.SemaphoreType.DMA((n,))] * 2,
        input_output_aliases={n: 0} if given else {},
        compiler_params=pltpu.CompilerParams(vmem_limit_bytes=VMEM_BYTES),
        cost_estimate=pl.CostEstimate(flops=sum(p.size for p in pieces) * 500, bytes_accessed=0, transcendentals=0),
    )(*pieces, *given)


def solution(mesh):
    tpn = mesh.shape['tp']
    assert tpn == CHIPS * CORES

    def hop(v, chips_by, cores_by):
        perm = []
        for t in range(tpn):
            ch, co = t // CORES, t % CORES
            perm.append((t, ((ch + chips_by) % CHIPS) * CORES + (co + cores_by) % CORES))
        return lax.ppermute(v, 'tp', perm)

    def gather(va, vb):
        ns, blk, dm = va.shape
        half = blk * CHIPS
        la, rb = hop(va, 1, 0), hop(vb, -1, 0)
        lb, ra = hop(vb, 1, 0), hop(va, -1, 0)
        oa, ob = hop(la, 1, 0), hop(rb, -1, 0)
        near = [va, vb, la, lb, ra, rb]
        near += [hop(p, 0, 1) for p in near]
        far = [(oa, ob), (hop(oa, 0, 1), hop(ob, 0, 1))]

        def near_at(chip, core):
            chips = (chip, (chip + CHIPS - 1) % CHIPS, (chip + 1) % CHIPS)
            return [(k * ns, co * half + ch * blk) for co in (core, 1 - core) for ch in chips for k in (0, 1)]

        def far_at(other, chip, core):
            o = ((chip + 2) % CHIPS) * blk
            return [(k * ns, (1 - core if other else core) * half + o) for k in (0, 1)]

        out = placed(None, near, (2 * ns, half * CORES, dm), near_at)
        for k in (0, 1):
            out = placed(out, far[k], out.shape, functools.partial(far_at, k))
        return out

    def step(x_in, gain_attn, w_qkv, w_out, gain_mlp, w_up, w_down, dy_out):
        heads, e = w_qkv.shape[3:]
        dm = x_in.shape[2]
        he = heads * e
        wqkv = jnp.transpose(w_qkv[0], (1, 2, 3, 0)).reshape(3 * he, dm)
        wo = w_out[0].reshape(he, dm)
        out = mega(x_in, dy_out, wqkv, wo, w_up[0], w_down[0], gain_attn, gain_mlp, heads)
        ya, yb, dx, dwq, dwo, dwu, dwd = out[:7]
        dgain = out[-1]
        dx, dwu, dwo = copied((dx, dwu, dwo))
        dwd, dwq = copied((dwd, dwq))
        y = gather(ya, yb)
        dwq = jnp.transpose(dwq.reshape(3, heads, e, dm), (3, 0, 1, 2))
        return (y, dx.reshape(x_in.shape), dgain[0:1], dwq[None], dwo.reshape(1, heads, e, dm),
                dgain[1:2], dwu[None], dwd[None])

    act = P('dp', None, None)
    in_specs = (act, P(None, None), P(None, None, None, 'tp', None), P(None, 'tp', None, None), P(None, None),
                P(None, None, 'tp'), P(None, 'tp', None), act)
    out_specs = (act, act, P('dp', None), P('dp', None, None, 'tp', None), P('dp', 'tp', None, None), P('dp', None),
                 P('dp', None, 'tp'), P('dp', 'tp', None))
    step = jax.shard_map(step, mesh=mesh, in_specs=in_specs, out_specs=out_specs, check_vma=False)
    return step
```
